32 devices in a mesh: emb: 32 (over z, y, x, core).
Axes of the slice: x: 2, y: 2, z: 4, core: 2. Of those that a mesh axis runs over, the one named last changes fastest.
Arguments:
- tok_ids: int32 [32768], P('emb')
- x_in: bfloat16 [32768, 1024], P('emb')
- d_out: bfloat16 [32768, 1024], P('emb')
- ple_tables: bfloat16 [3, 151936, 256], P(None, 'emb')
- w_up: bfloat16 [3, 1024, 3072], replicated
- w_down: bfloat16 [3, 3072, 1024], replicated
- w_gate: bfloat16 [3, 1024, 256], replicated
- w_proj: bfloat16 [3, 256, 1024], replicated
Outputs:
- output 1: bfloat16 [32768, 1024], P('emb')
- output 2: float32 [3, 151936, 256], P(None, 'emb')
- output 3: float32 [3, 1024, 3072], replicated
- output 4: float32 [3, 3072, 1024], replicated
- output 5: float32 [3, 1024, 256], replicated
- output 6: float32 [3, 256, 1024], replicated
All inputs are finite; a program needn't handle non-finite values.
Results may differ from the reference program's by a relative error of at most 0.0144084.
Values are sent between devices in bfloat16 or wider.
A program may use at most 1 GiB of HBM per device.

```python
import math
import jax
import jax.numpy as jnp
from jax import lax

VOCAB_SIZE = 151936
MODEL_DIM = 1024
HIDDEN_DIM = 3072
EMBED_DIM = 256
LAYERS = 3
TOKENS = 32768
SHARDS = 32

ROWS_DEV = VOCAB_SIZE // SHARDS
TOKENS_PER = TOKENS // SHARDS
CAP_ROWS = TOKENS_PER // 4
ROW_BITS = int(math.log2(ROWS_DEV)) + 1
EPS = 1e-6


def draw_ids(key):
    k_hot, k_off, k_row, k_shift, k_perm = jax.random.split(key, 5)
    hot_owner = jax.random.randint(k_hot, (SHARDS, 1), 0, SHARDS)
    start_off = jax.random.randint(k_off, (SHARDS, 1), 0, SHARDS - 1)
    slot_idx = jnp.arange(TOKENS_PER)[None, :]
    spread_owner = (hot_owner + 1 + (start_off + slot_idx - CAP_ROWS) % (SHARDS - 1)) % SHARDS
    owner_dev = jnp.where(slot_idx < CAP_ROWS, hot_owner, spread_owner)
    raw_rows = jax.random.randint(k_row, (SHARDS, TOKENS_PER), 0, ROWS_DEV)
    shift_bits = jax.random.randint(k_shift, (SHARDS, TOKENS_PER), 0, ROW_BITS + 1)
    local_row = jnp.right_shift(raw_rows, shift_bits)
    id_grid = owner_dev * ROWS_DEV + local_row
    id_grid = jax.random.permutation(k_perm, id_grid, axis=1, independent=True)
    return id_grid.reshape(TOKENS).astype(jnp.int32)


def draw_normal(key, shape, scale):
    return (jax.random.normal(key, shape, jnp.float32) * scale).astype(jnp.bfloat16)


def setup_inputs(seed: int = 0) -> dict:
    key_list = jax.random.split(jax.random.key(seed), 8)
    return {
        "tok_ids": draw_ids(key_list[0]),
        "x_in": draw_normal(key_list[1], (TOKENS, MODEL_DIM), 1.0),
        "d_out": draw_normal(key_list[2], (TOKENS, MODEL_DIM), 1.0),
        "ple_tables": draw_normal(key_list[3], (LAYERS, VOCAB_SIZE, EMBED_DIM), 1.0),
        "w_up": draw_normal(key_list[4], (LAYERS, MODEL_DIM, HIDDEN_DIM), MODEL_DIM ** -0.5),
        "w_down": draw_normal(key_list[5], (LAYERS, HIDDEN_DIM, MODEL_DIM), 0.5 * HIDDEN_DIM ** -0.5),
        "w_gate": draw_normal(key_list[6], (LAYERS, MODEL_DIM, EMBED_DIM), MODEL_DIM ** -0.5),
        "w_proj": draw_normal(key_list[7], (LAYERS, EMBED_DIM, MODEL_DIM), 0.35 * EMBED_DIM ** -0.5),
    }


def gelu_tanh(pre_act):
    return jax.nn.gelu(pre_act, approximate=True)


def gelu_back(pre_act, grad_out):
    _, pull_back = jax.vjp(gelu_tanh, pre_act.astype(jnp.float32))
    return pull_back(grad_out.astype(jnp.float32))[0]


def layer_fwd(x_cur, up_mat, down_mat, gate_mat, proj_mat, emb_rows):
    x_wide = x_cur.astype(jnp.float32)
    inv_rms = lax.rsqrt(jnp.mean(x_wide * x_wide, axis=-1, keepdims=True) + EPS)
    normed = (x_wide * inv_rms).astype(jnp.bfloat16)
    hidden = jnp.dot(normed, up_mat, preferred_element_type=jnp.float32).astype(jnp.bfloat16)
    act_out = gelu_tanh(hidden.astype(jnp.float32)).astype(jnp.bfloat16)
    mlp_out = jnp.dot(act_out, down_mat, preferred_element_type=jnp.float32).astype(jnp.bfloat16)
    gate_pre = jnp.dot(normed, gate_mat, preferred_element_type=jnp.float32).astype(jnp.bfloat16)
    gate_act = gelu_tanh(gate_pre.astype(jnp.float32)).astype(jnp.bfloat16)
    mix_rows = (gate_act.astype(jnp.float32) * emb_rows.astype(jnp.float32)).astype(jnp.bfloat16)
    ple_out = jnp.dot(mix_rows, proj_mat, preferred_element_type=jnp.float32).astype(jnp.bfloat16)
    x_next = (x_wide + mlp_out.astype(jnp.float32) + ple_out.astype(jnp.float32)).astype(jnp.bfloat16)
    return x_next, (x_wide, inv_rms, normed, hidden, act_out, gate_pre, gate_act, mix_rows)


def layer_bwd(d_x, saved, emb_rows, up_mat, down_mat, gate_mat, proj_mat):
    x_wide, inv_rms, normed, hidden, act_out, gate_pre, gate_act, mix_rows = saved
    g_out = d_x.astype(jnp.bfloat16)
    d_act = jnp.dot(g_out, down_mat.T, preferred_element_type=jnp.float32).astype(jnp.bfloat16)
    d_hidden = gelu_back(hidden, d_act).astype(jnp.bfloat16)
    d_mix = jnp.dot(g_out, proj_mat.T, preferred_element_type=jnp.float32).astype(jnp.bfloat16)
    d_rows = gate_act.astype(jnp.float32) * d_mix.astype(jnp.float32)
    d_gate_act = (emb_rows.astype(jnp.float32) * d_mix.astype(jnp.float32)).astype(jnp.bfloat16)
    d_gate_pre = gelu_back(gate_pre, d_gate_act).astype(jnp.bfloat16)
    d_norm = jnp.dot(d_hidden, up_mat.T, preferred_element_type=jnp.float32) + jnp.dot(d_gate_pre, gate_mat.T, preferred_element_type=jnp.float32)
    d_x_new = d_x + inv_rms * d_norm - inv_rms ** 3 * x_wide * jnp.mean(d_norm * x_wide, axis=-1, keepdims=True)
    g_up = jnp.dot(normed.T, d_hidden, preferred_element_type=jnp.float32)
    g_down = jnp.dot(act_out.T, g_out, preferred_element_type=jnp.float32)
    g_gate = jnp.dot(normed.T, d_gate_pre, preferred_element_type=jnp.float32)
    g_proj = jnp.dot(mix_rows.T, g_out, preferred_element_type=jnp.float32)
    return d_x_new, (g_up, g_down, g_gate, g_proj), d_rows


def reference(tok_ids, x_in, d_out, ple_tables, w_up, w_down, w_gate, w_proj):
    weights = (w_up, w_down, w_gate, w_proj)
    ids_blocks = tok_ids.reshape(SHARDS, TOKENS_PER)
    x_blocks = x_in.reshape(SHARDS, TOKENS_PER, MODEL_DIM)
    dy_blocks = d_out.reshape(SHARDS, TOKENS_PER, MODEL_DIM)

    def fwd_step(x_cur, layer_in):
        up_mat, down_mat, gate_mat, proj_mat, emb_rows = layer_in
        return layer_fwd(x_cur, up_mat, down_mat, gate_mat, proj_mat, emb_rows)

    def bwd_step(d_x, layer_in):
        saved, up_mat, down_mat, gate_mat, proj_mat, emb_rows = layer_in
        d_x_new, grads, d_rows = layer_bwd(d_x, saved, emb_rows, up_mat, down_mat, gate_mat, proj_mat)
        return d_x_new, (grads, d_rows)

    def block_step(carry, block_in):
        grad_acc, table_acc = carry
        blk_ids, blk_x, blk_dy = block_in
        rows_all = ple_tables[:, blk_ids, :]
        x_last, saved_all = lax.scan(fwd_step, blk_x, weights + (rows_all,))
        _, (grads, d_rows) = lax.scan(bwd_step, blk_dy.astype(jnp.float32), (saved_all,) + weights + (rows_all,), reverse=True)
        grad_acc = tuple(acc_part + new_part for acc_part, new_part in zip(grad_acc, grads))
        table_acc = table_acc.at[:, blk_ids, :].add(d_rows)
        return (grad_acc, table_acc), x_last

    grad_init = tuple(jnp.zeros(weight_mat.shape, jnp.float32) for weight_mat in weights)
    table_init = jnp.zeros(ple_tables.shape, jnp.float32)
    (grad_acc, table_acc), x_done = lax.scan(block_step, (grad_init, table_init), (ids_blocks, x_blocks, dy_blocks))
    x_out = x_done.reshape(TOKENS, MODEL_DIM)
    return (x_out, table_acc, grad_acc[0], grad_acc[1], grad_acc[2], grad_acc[3])
```

```python
import functools

import jax
import jax.numpy as jnp
from jax import lax
from jax.experimental import pallas as pl
from jax.experimental.pallas import tpu as pltpu
from jax.sharding import PartitionSpec as P

EPS = 1e-6
CAP_DIV = 4


def gelu_tanh(pre_act):
    return jax.nn.gelu(pre_act, approximate=True)


def gelu_back(pre_act, grad_out):
    _, pull_back = jax.vjp(gelu_tanh, pre_act.astype(jnp.float32))
    return pull_back(grad_out.astype(jnp.float32))[0]


def dot32(a, b, dims):
    return lax.dot_general(a, b, (dims, ((), ())), preferred_element_type=jnp.float32)


def layer_fwd(x_cur, up_mat, down_mat, gate_mat, proj_mat, emb_rows):
    x_wide = x_cur.astype(jnp.float32)
    inv_rms = lax.rsqrt(jnp.mean(x_wide * x_wide, axis=-1, keepdims=True) + EPS)
    normed = (x_wide * inv_rms).astype(jnp.bfloat16)
    hidden = jnp.dot(normed, up_mat, preferred_element_type=jnp.float32).astype(jnp.bfloat16)
    act_out = gelu_tanh(hidden.astype(jnp.float32)).astype(jnp.bfloat16)
    mlp_out = jnp.dot(act_out, down_mat, preferred_element_type=jnp.float32).astype(jnp.bfloat16)
    gate_pre = jnp.dot(normed, gate_mat, preferred_element_type=jnp.float32).astype(jnp.bfloat16)
    gate_act = gelu_tanh(gate_pre.astype(jnp.float32)).astype(jnp.bfloat16)
    mix_rows = (gate_act.astype(jnp.float32) * emb_rows.astype(jnp.float32)).astype(jnp.bfloat16)
    ple_out = jnp.dot(mix_rows, proj_mat, preferred_element_type=jnp.float32).astype(jnp.bfloat16)
    x_next = (x_wide + mlp_out.astype(jnp.float32) + ple_out.astype(jnp.float32)).astype(jnp.bfloat16)
    return x_next, (x_cur, inv_rms, normed, hidden, act_out, gate_pre, gate_act, mix_rows)


def layer_bwd(d_x, saved, emb_rows, up_mat, down_mat, gate_mat, proj_mat, last):
    x_cur, inv_rms, normed, hidden, act_out, gate_pre, gate_act, mix_rows = saved
    x_wide = x_cur.astype(jnp.float32)
    g_out = d_x.astype(jnp.bfloat16)
    d_act = dot32(g_out, down_mat, ((1,), (1,))).astype(jnp.bfloat16)
    d_hidden = gelu_back(hidden, d_act).astype(jnp.bfloat16)
    d_mix = dot32(g_out, proj_mat, ((1,), (1,))).astype(jnp.bfloat16)
    d_gate_act = (emb_rows.astype(jnp.float32) * d_mix.astype(jnp.float32)).astype(jnp.bfloat16)
    d_gate_pre = gelu_back(gate_pre, d_gate_act).astype(jnp.bfloat16)
    d_x_new = None
    if not last:
        d_norm = dot32(d_hidden, up_mat, ((1,), (1,))) + dot32(d_gate_pre, gate_mat, ((1,), (1,)))
        d_x_new = d_x + inv_rms * d_norm - inv_rms ** 3 * x_wide * jnp.mean(d_norm * x_wide, axis=-1, keepdims=True)
    return d_x_new, (normed, act_out, mix_rows, g_out, d_hidden, d_gate_pre), (gate_act, d_mix)


MESH = pl.DeviceIdType.MESH
BLK = 256
NB = 16
NS = 8


def reduce_kernel(sizes, *refs):
    n_layers, per, n = sizes
    ops = refs[:6 * n_layers]
    out = refs[6 * n_layers]
    (v_as, v_o, v_u, v_d, blk1, blk2, blk3, rc1, rc2, rc3, rf1, rf2, rs1, rs2, ri1, ri2, rm1, rm2, fin1, fin2,
     ri3, rm3, rf3, rs3, fin3, ssem, rsem, lsem, osem) = refs[6 * n_layers + 1:]
    me = lax.axis_index("emb")
    core, x, y, z = lax.rem(me, 2), lax.rem(me // 2, 2), lax.rem(me // 4, 2), me // 8
    mid = (z == 1) | (z == 2)
    end = (z == 0) | (z == 3)
    zb = z // 2
    p_core = me + 1 - 2 * core
    p_x = me + 2 - 4 * x
    p_y = me + 4 - 8 * y
    step_in = jnp.where((z == 0) | (z == 1), 8, -8)
    p_side = jnp.where((z == 0) | (z == 2), me + 8, me - 8)
    p_mid = jnp.where(z == 1, me + 8, jnp.where(z == 2, me - 8, me))

    barrier = pltpu.get_barrier_semaphore()
    for dev in (p_core, p_x, p_y, p_side):
        pl.semaphore_signal(barrier, inc=1, device_id=(dev,), device_id_type=MESH)

    @pl.when(mid)
    def _():
        pl.semaphore_signal(barrier, inc=1, device_id=(p_mid,), device_id_type=MESH)
        pl.semaphore_wait(barrier, 5)

    @pl.when(end)
    def _():
        pl.semaphore_wait(barrier, 4)

    def loads(ell):
        u, a, s, o, dh, dz = ops[6 * ell:6 * ell + 6]
        slot = ell % 2
        hid = a.shape[1]
        return [
            pltpu.make_async_copy(a, v_as.at[slot, :, pl.ds(0, hid)], osem.at[slot, 0]),
            pltpu.make_async_copy(s, v_as.at[slot, :, pl.ds(hid, BLK)], osem.at[slot, 1]),
            pltpu.make_async_copy(o, v_o.at[slot], osem.at[slot, 2]),
            pltpu.make_async_copy(u, v_u.at[slot], osem.at[slot, 3]),
            pltpu.make_async_copy(dh, v_d.at[slot, :, pl.ds(0, hid)], osem.at[slot, 4]),
            pltpu.make_async_copy(dz, v_d.at[slot, :, pl.ds(hid, BLK)], osem.at[slot, 5]),
        ]

    for ell in (0, 1):
        for c in loads(ell):
            c.start()
    for c in loads(0):
        c.wait()

    def seq(k, c3):
        return 3 * (k // 2) + (2 if c3 else lax.rem(k, 2))

    def where_out(k, kind):
        j = seq(k, kind == 2)
        ell, w = j // per, lax.rem(j, per)
        base = {0: 0, 1: per, 2: per * lax.rem(k, 2)}[kind]
        return (n_layers - 1 - ell) * 2 * per + base + w

    def block(slot, j, wide):
        w = lax.rem(j, per)
        if wide:
            rb, cb = w // 13, lax.rem(w, 13)
            lhs, rhs = v_u, v_d
        else:
            rb, cb = w // 4, lax.rem(w, 4)
            lhs, rhs = v_as, v_o
        lv = lhs[slot, :, pl.ds(pl.multiple_of(rb * BLK, BLK), BLK)]
        rv = rhs[slot, :, pl.ds(pl.multiple_of(cb * BLK, BLK), BLK)]
        return lax.dot_general(lv, rv, (((0,), (0,)), ((), ())), preferred_element_type=jnp.float32)

    h0 = core * 128
    flows = []

    def add_flow(off, src, dst, dev, send_if=None, recv_if=None):
        flows.append((len(flows), off, src, dst, dev, send_if, recv_if))
        return flows[-1]

    def rows(start, size):
        return pl.ds(pl.multiple_of(start, 32), size)

    def desc(f, k):
        idx, off, src, dst, dev, _, _ = f
        d = dev(k) if callable(dev) else dev
        return pltpu.make_async_remote_copy(
            src_ref=src(k), dst_ref=dst(k), send_sem=ssem.at[idx, lax.rem(k, NB)], recv_sem=rsem.at[idx, lax.rem(k, NB)],
            device_id=(d,), device_id_type=MESH)

    def ok(k, cond):
        v = (k >= 0) & (k < n)
        return v if cond is None else v & cond

    acts = []

    def xyz(kind, blk, rc, rf, rs, ri, rm, fin, f, s, p_f, p_s):
        q0, q1 = h0 + f * 64, h0 + (1 - f) * 64
        e0, e1 = q0 + s * 32, q0 + (1 - s) * 32
        b = lambda k: lax.rem(k, NB)
        m = lambda k: lax.rem(k, NS)
        o = lambda k: where_out(k, kind)
        f_core = add_flow(1, lambda k: blk.at[b(k), rows(128 - h0, 128)], lambda k: rc.at[m(k)], p_core)
        f_first = add_flow(3, lambda k: blk.at[b(k), rows(q1, 64)], lambda k: rf.at[m(k)], p_f)
        f_second = add_flow(5, lambda k: blk.at[b(k), rows(e1, 32)], lambda k: rs.at[m(k)], p_s)
        f_in = add_flow(7, lambda k: blk.at[b(k), rows(e0, 32)], lambda k: ri.at[m(k)], p_side, end, mid)
        f_mid = add_flow(9, lambda k: blk.at[b(k), rows(e0, 32)], lambda k: rm.at[m(k)], p_mid, mid, mid)
        f_out = add_flow(11, lambda k: fin.at[b(k)], lambda k: fin.at[b(k)], p_side, mid, end)
        g_s = add_flow(13, lambda k: fin.at[b(k)], lambda k: out.at[o(k), rows(e0, 32)], p_s)
        g_f = add_flow(15, lambda k: out.at[o(k), rows(q0, 64)], lambda k: out.at[o(k), rows(q0, 64)], p_f)
        g_c = add_flow(17, lambda k: out.at[o(k), rows(h0, 128)], lambda k: out.at[o(k), rows(h0, 128)], p_core)

        def plus(dst0, size, src):
            def go(k):
                r = rows(dst0, size)
                blk[b(k), r] = blk[b(k), r] + src[m(k)]
            return go

        def final(k):
            fin[b(k)] = blk[b(k), rows(e0, 32)] + rm[m(k)]

        acts.append((f_core, plus(h0, 128, rc)))
        acts.append((f_first, plus(q0, 64, rf)))
        acts.append((f_second, plus(e0, 32, rs)))
        acts.append((f_in, plus(e0, 32, ri)))
        acts.append((f_mid, final))
        acts.append((f_out, None))
        acts.append((g_s, None))
        acts.append((g_f, None))
        acts.append((g_c, None))
        locals_.append((13, lambda k: pltpu.make_async_copy(fin.at[b(k)], out.at[o(k), rows(e0, 32)], lsem.at[kind, m(k)]), None))

    def zfirst(kind, blk, rc, ri, rm, rf, rs, fin):
        def fs(k):
            odd = lax.rem(k, 2) == 1
            return jnp.where(odd, y, x), jnp.where(odd, p_y, p_x), jnp.where(odd, p_x, p_y)

        q0, q1 = h0 + zb * 64, h0 + (1 - zb) * 64
        b = lambda k: lax.rem(k, NB)
        m = lambda k: lax.rem(k, NS)
        o = lambda k: where_out(k, kind)
        e0 = lambda k: q0 + fs(k)[0] * 32
        e1 = lambda k: q0 + (1 - fs(k)[0]) * 32
        p_f = lambda k: fs(k)[1]
        p_s = lambda k: fs(k)[2]
        f_core = add_flow(1, lambda k: blk.at[b(k), rows(128 - h0, 128)], lambda k: rc.at[m(k)], p_core)
        f_in = add_flow(3, lambda k: blk.at[b(k), rows(h0, 128)], lambda k: ri.at[b(k)], p_side, end, mid)
        f_mid = add_flow(5, lambda k: blk.at[b(k), rows(q1, 64)], lambda k: rm.at[m(k)], p_mid, mid, mid)
        f_first = add_flow(7, lambda k: blk.at[b(k), rows(e1(k), 32)], lambda k: rf.at[m(k)], p_f, mid, mid)
        f_second = add_flow(9, lambda k: blk.at[b(k), rows(e0(k), 32)], lambda k: rs.at[m(k)], p_s, mid, mid)
        g_f = add_flow(11, lambda k: fin.at[m(k)], lambda k: out.at[o(k), rows(e0(k), 32)], p_f, mid, mid)
        g_m = add_flow(13, lambda k: out.at[o(k), rows(q0, 64)], lambda k: out.at[o(k), rows(q0, 64)], p_mid, mid, mid)
        g_o = add_flow(15, lambda k: out.at[o(k), rows(h0, 128)], lambda k: out.at[o(k), rows(h0, 128)], p_side, mid, end)
        g_c = add_flow(17, lambda k: out.at[o(k), rows(h0, 128)], lambda k: out.at[o(k), rows(h0, 128)], p_core)

        def plus(start, size, src, idx):
            def go(k):
                r = rows(start(k), size)
                blk[b(k), r] = blk[b(k), r] + src[idx(k)]
            return go

        def final(k):
            fin[m(k)] = blk[b(k), rows(e0(k), 32)] + rs[m(k)]

        acts.append((f_core, plus(lambda k: h0, 128, rc, m)))
        acts.append((f_in, plus(lambda k: h0, 128, ri, b)))
        acts.append((f_mid, plus(lambda k: q0, 64, rm, m)))
        acts.append((f_first, plus(e0, 32, rf, m)))
        acts.append((f_second, final))
        acts.append((g_f, None))
        acts.append((g_m, None))
        acts.append((g_o, None))
        acts.append((g_c, None))
        locals_.append((11, lambda k: pltpu.make_async_copy(fin.at[m(k)], out.at[o(k), rows(e0(k), 32)], lsem.at[kind, m(k)]), mid))

    locals_ = []
    xyz(0, blk1, rc1, rf1, rs1, ri1, rm1, fin1, x, y, p_x, p_y)
    xyz(1, blk2, rc2, rf2, rs2, ri2, rm2, fin2, y, x, p_y, p_x)
    zfirst(2, blk3, rc3, ri3, rm3, rf3, rs3, fin3)

    first_of = [(2 * ((per * ell) // 3)) for ell in range(n_layers)]
    last_of = [(2 * ((per * (ell + 1) - 1) // 3) + 1) for ell in range(n_layers)]

    def round_(r, _):
        for f in flows:
            k = r - f[1] - 4

            @pl.when(ok(k, f[5]))
            def _(f=f, k=k):
                desc(f, k).wait_send()
        for off, mk, cond in locals_:
            k = r - off - 2

            @pl.when(ok(k, cond))
            def _(mk=mk, k=k):
                mk(k).wait()
        for f, fn in acts:
            k = r - f[1] - 2

            @pl.when(ok(k, f[6]))
            def _(f=f, fn=fn, k=k):
                desc(f, k).wait_recv()
                if fn is not None:
                    fn(k)
        for ell in range(1, n_layers):
            @pl.when(r == first_of[ell])
            def _(ell=ell):
                for c in loads(ell):
                    c.wait()
        for f in flows:
            k = r - f[1]

            @pl.when(ok(k, f[5]))
            def _(f=f, k=k):
                desc(f, k).start()
        for off, mk, cond in locals_:
            k = r - off

            @pl.when(ok(k, cond))
            def _(mk=mk, k=k):
                mk(k).start()

        @pl.when(r < n)
        def _():
            s = lax.rem(r, NB)
            j = seq(r, False)
            slot = lax.rem(j // per, 2)
            blk1[s] = block(slot, j, False)
            blk2[s] = block(slot, j, True)
            j3 = seq(r, True)
            slot3 = lax.rem(j3 // per, 2)
            odd = lax.rem(r, 2) == 1

            @pl.when(odd)
            def _():
                blk3[s] = block(slot3, j3, True)

            @pl.when(jnp.logical_not(odd))
            def _():
                blk3[s] = block(slot3, j3, False)
        for ell in range(2, n_layers):
            @pl.when(r == last_of[ell - 2])
            def _(ell=ell):
                for c in loads(ell):
                    c.start()
        return 0

    lax.fori_loop(0, n + 22, round_, 0)


def reduce_grads(layer_ops):
    n_layers = len(layer_ops)
    u, a, s, o, dh, dz = layer_ops[0]
    toks, dim = u.shape
    wide = a.shape[1] + s.shape[1]
    per = (wide // BLK) * (dim // BLK)
    n = 2 * per * n_layers // 3
    f32, bf = jnp.float32, jnp.bfloat16
    V = pltpu.VMEM
    scratch = [
        V((2, toks, wide), bf), V((2, toks, dim), bf), V((2, toks, dim), bf), V((2, toks, wide), bf),
        V((NB, BLK, BLK), f32), V((NB, BLK, BLK), f32), V((NB, BLK, BLK), f32),
        V((NS, 128, BLK), f32), V((NS, 128, BLK), f32), V((NS, 128, BLK), f32),
        V((NS, 64, BLK), f32), V((NS, 64, BLK), f32),
        V((NS, 32, BLK), f32), V((NS, 32, BLK), f32),
        V((NS, 32, BLK), f32), V((NS, 32, BLK), f32),
        V((NS, 32, BLK), f32), V((NS, 32, BLK), f32),
        V((NB, 32, BLK), f32), V((NB, 32, BLK), f32),
        V((NB, 128, BLK), f32), V((NS, 64, BLK), f32), V((NS, 32, BLK), f32), V((NS, 32, BLK), f32), V((NS, 32, BLK), f32),
        pltpu.SemaphoreType.DMA((27, NB)), pltpu.SemaphoreType.DMA((27, NB)), pltpu.SemaphoreType.DMA((3, NS)),
        pltpu.SemaphoreType.DMA((2, 6)),
    ]
    flat = [t for ops in layer_ops for t in ops]
    return pl.pallas_call(
        functools.partial(reduce_kernel, (n_layers, per, n)),
        out_shape=jax.ShapeDtypeStruct((2 * per * n_layers, BLK, BLK), f32),
        in_specs=[pl.BlockSpec(memory_space=pl.ANY)] * len(flat),
        out_specs=pl.BlockSpec(memory_space=pl.ANY),
        scratch_shapes=scratch,
        compiler_params=pltpu.CompilerParams(collective_id=0, has_side_effects=True, vmem_limit_bytes=66_000_000),
        cost_estimate=pl.CostEstimate(flops=600 * 10**9, bytes_accessed=10**8, transcendentals=0),
        name="reduce_grads",
    )(*flat)


def unpack_kernel_rows(src, rows_out, tail_out):
    cols = src.shape[0]
    step = pl.program_id(1)
    last = pl.num_programs(1) - 1

    @pl.when(step < last)
    def _():
        for c in range(cols):
            rows_out[0, :, c * BLK:(c + 1) * BLK] = src[c]

    @pl.when(step == last)
    def _():
        for c in range(cols):
            tail_out[0, :, c * BLK:(c + 1) * BLK] = src[c]


def unpack_kernel_cols(src, wide_out, tail_out):
    cols = src.shape[0] - 1
    for c in range(cols):
        wide_out[0, :, c * BLK:(c + 1) * BLK] = src[c]
    tail_out[0] = src[cols]


def unpack(total, layers, dim, hid, emb):
    f32 = jnp.float32
    nr, nc = (hid + emb) // BLK, dim // BLK
    per = nr * nc
    lim = pltpu.CompilerParams(vmem_limit_bytes=40_000_000)
    down, proj = pl.pallas_call(
        unpack_kernel_rows,
        grid=(layers, nr),
        in_specs=[pl.BlockSpec((nc, BLK, BLK), lambda i, j: ((i * 2 * per + j * nc) // nc, 0, 0))],
        out_specs=[pl.BlockSpec((1, BLK, dim), lambda i, j: (i, jnp.minimum(j, nr - 2), 0)),
                   pl.BlockSpec((1, BLK, dim), lambda i, j: (i, 0, 0))],
        out_shape=[jax.ShapeDtypeStruct((layers, hid, dim), f32), jax.ShapeDtypeStruct((layers, emb, dim), f32)],
        compiler_params=lim, name="unpack_rows",
    )(total)
    up, gate = pl.pallas_call(
        unpack_kernel_cols,
        grid=(layers, nc),
        in_specs=[pl.BlockSpec((nr, BLK, BLK), lambda i, j: (i * 2 * nc + nc + j, 0, 0))],
        out_specs=[pl.BlockSpec((1, BLK, hid), lambda i, j: (i, j, 0)),
                   pl.BlockSpec((1, BLK, emb), lambda i, j: (i, j, 0))],
        out_shape=[jax.ShapeDtypeStruct((layers, dim, hid), f32), jax.ShapeDtypeStruct((layers, dim, emb), f32)],
        compiler_params=lim, name="unpack_cols",
    )(total)
    return up, down, gate, proj


BASE = 32


def spread(tok_ids, shards, rows_dev, cap, over):
    toks = tok_ids.shape[0]
    i32, f32, bf = jnp.int32, jnp.float32, jnp.bfloat16
    owner = tok_ids // rows_dev
    local = tok_ids - owner * rows_dev
    hot = (owner[:, None] == jnp.arange(shards, dtype=i32)[None, :]).astype(bf)
    before = lax.broadcasted_iota(i32, (toks, toks), 0) > lax.broadcasted_iota(i32, (toks, toks), 1)
    ahead = jnp.dot(before.astype(bf), hot, preferred_element_type=f32)
    hot32 = hot.astype(f32)
    rank = jnp.sum(ahead * hot32, axis=1).astype(i32)
    count = jnp.sum(hot32, axis=0).astype(i32)
    extra = jnp.maximum(count - BASE, 0)
    lower = lax.broadcasted_iota(i32, (shards, shards), 0) > lax.broadcasted_iota(i32, (shards, shards), 1)
    start = jnp.sum(jnp.where(lower, extra[None, :], 0), axis=1)
    total = jnp.sum(extra)
    tail = jnp.sum(jnp.where(owner[:, None] == jnp.arange(shards, dtype=i32)[None, :], start[None, :], 0), axis=1)
    slot = jnp.where(rank < BASE, owner * BASE + rank, shards * BASE + tail + rank - BASE)
    pick = (slot[:, None] == lax.broadcasted_iota(i32, (toks, shards * BASE + over), 1)).astype(bf)
    parts = jnp.stack([local // 64, local % 64], axis=1).astype(bf)
    want = dot32(pick, parts, ((0,), (0,)))
    want = (want[:, 0] * 64.0 + want[:, 1]).astype(i32)
    base = want[:shards * BASE].reshape(shards, BASE)
    rest = jnp.broadcast_to(want[shards * BASE:][None, :], (shards, over))
    info = jnp.stack([count, start, extra, jnp.broadcast_to(total, (shards,))], axis=1)
    pad = jnp.zeros((shards, 128 - 4), i32)
    sent = jnp.concatenate([info, pad, base, rest], axis=1)
    got = lax.all_to_all(sent, "emb", 0, 0, tiled=True)
    return pick, got


INFO = 128


def serve_kernel(n_layers, over, got, tables, *refs):
    outs, (tab, wide, stage, sem) = refs[:2 * n_layers], refs[2 * n_layers:]
    shards = got.shape[0]
    loads = [pltpu.make_async_copy(tables.at[k], tab.at[k], sem.at[k]) for k in range(n_layers)]
    for c in loads:
        c.start()
    for k in range(n_layers):
        loads[k].wait()
        wide[...] = tab[k].astype(jnp.float32)
        base_out, over_out = outs[2 * k], outs[2 * k + 1]

        def one(j, _, base_out=base_out, over_out=over_out):
            count = jnp.minimum(got[j, 0], BASE)
            start, extra = got[j, 1], got[j, 2]

            def row(i, _):
                stage[pl.ds(i, 1)] = wide[pl.ds(got[j, INFO + i], 1)]
                return 0

            lax.fori_loop(0, count, row, 0)
            base_out[j] = stage[:BASE].astype(jnp.bfloat16)

            @pl.when(extra == 0)
            def _():
                over_out[j] = jnp.zeros(over_out.shape[1:], jnp.bfloat16)

            @pl.when(extra > 0)
            def _():
                stage[...] = jnp.zeros_like(stage)

                def row2(i, _):
                    stage[pl.ds(start + i, 1)] = wide[pl.ds(got[j, INFO + BASE + start + i], 1)]
                    return 0

                lax.fori_loop(0, extra, row2, 0)
                over_out[j] = stage[:over].astype(jnp.bfloat16)
            return 0

        lax.fori_loop(0, shards, one, 0)


def serve(got, tables, over):
    n_layers, rows_dev, emb = tables.shape
    shards = got.shape[0]
    bf = jnp.bfloat16
    shapes = []
    for _ in range(n_layers):
        shapes += [jax.ShapeDtypeStruct((shards, BASE, emb), bf), jax.ShapeDtypeStruct((shards, over, emb), bf)]
    return pl.pallas_call(
        functools.partial(serve_kernel, n_layers, over),
        in_specs=[pl.BlockSpec(memory_space=pltpu.SMEM), pl.BlockSpec(memory_space=pl.ANY)],
        out_specs=[pl.BlockSpec(memory_space=pltpu.VMEM)] * (2 * n_layers),
        out_shape=shapes,
        scratch_shapes=[pltpu.VMEM((n_layers, rows_dev, emb), bf), pltpu.VMEM((rows_dev, emb), jnp.float32),
                        pltpu.VMEM((over, emb), jnp.float32), pltpu.SemaphoreType.DMA((n_layers,))],
        compiler_params=pltpu.CompilerParams(vmem_limit_bytes=60_000_000),
        name="serve_rows",
    )(got, tables)


def collect_kernel(n_layers, over, got, *refs):
    ins = refs[:2 * n_layers]
    out, base_v, over_v, sem = refs[2 * n_layers:]
    shards = got.shape[0]
    layer = pl.program_id(0)

    def loads(k):
        return (pltpu.make_async_copy(ins[2 * k], base_v.at[k % 2], sem.at[k % 2, 0]),
                pltpu.make_async_copy(ins[2 * k + 1], over_v.at[k % 2], sem.at[k % 2, 1]))

    for k in range(n_layers):
        @pl.when(layer == k)
        def _(k=k):
            if k == 0:
                for c in loads(0):
                    c.start()
            if k + 1 < n_layers:
                for c in loads(k + 1):
                    c.start()
    out[...] = jnp.zeros_like(out)
    for k in range(n_layers):
        @pl.when(layer == k)
        def _(k=k):
            for c in loads(k):
                c.wait()
    slot = lax.rem(layer, 2)

    def one(j, _):
        count = jnp.minimum(got[j, 0], BASE)
        start, extra = got[j, 1], got[j, 2]

        def row(i, _):
            r = pl.ds(got[j, INFO + i], 1)
            out[0, r] = out[0, r] + base_v[slot, j, pl.ds(i, 1)]
            return 0

        lax.fori_loop(0, count, row, 0)

        def row2(i, _):
            r = pl.ds(got[j, INFO + BASE + start + i], 1)
            out[0, r] = out[0, r] + over_v[slot, j, pl.ds(start + i, 1)]
            return 0

        lax.fori_loop(0, extra, row2, 0)
        return 0

    lax.fori_loop(0, shards, one, 0)


def collect(got, parts, rows_dev, over):
    n_layers = len(parts)
    shards = got.shape[0]
    emb = parts[0][0].shape[-1]
    f32 = jnp.float32
    flat = []
    for b, o in parts:
        flat += [b.reshape(shards, BASE, emb), o.reshape(shards, over, emb)]
    return pl.pallas_call(
        functools.partial(collect_kernel, n_layers, over),
        grid=(n_layers,),
        in_specs=[pl.BlockSpec(memory_space=pltpu.SMEM)] + [pl.BlockSpec(memory_space=pl.ANY)] * (2 * n_layers),
        out_specs=pl.BlockSpec((1, rows_dev, emb), lambda i: (i, 0, 0)),
        out_shape=jax.ShapeDtypeStruct((n_layers, rows_dev, emb), f32),
        scratch_shapes=[pltpu.VMEM((2, shards, BASE, emb), f32), pltpu.VMEM((2, shards, over, emb), f32),
                        pltpu.SemaphoreType.DMA((2, 2))],
        compiler_params=pltpu.CompilerParams(vmem_limit_bytes=60_000_000),
        name="collect_rows",
    )(got, *flat)


def tail_sum(block, n, order):
    me = lax.axis_index("emb")
    bits = {"core": 1, "x": 2, "y": 4, "zfar": 16, "znear": 8}
    cur = block.reshape((2, 2, 2, 2, 2) + block.shape[1:])
    axes = ["zfar", "znear", "y", "x", "core"]
    for way in order:
        bit = bits[way]
        ax = axes.index(way)
        mine = (me // bit) % 2
        perm = [(i, i ^ bit) for i in range(n)]
        sent = lax.dynamic_slice_in_dim(cur, 1 - mine, 1, ax)
        kept = lax.dynamic_slice_in_dim(cur, mine, 1, ax)
        cur = kept + lax.ppermute(sent, "emb", perm)
    return cur.reshape(block.shape[1:])


def fast_step(cap, over, got, pick, x_in, d_out, ple_tables, w_up, w_down, w_gate, w_proj):
    layers, rows_dev, emb = ple_tables.shape
    shards = got.shape[0]
    served = serve(got, ple_tables, over)
    returned = []
    for k in range(layers):
        base = lax.all_to_all(served[2 * k].reshape(shards * BASE, emb), "emb", 0, 0, tiled=True)
        order = ("core", "x", "y", "zfar", "znear") if k % 2 == 0 else ("core", "y", "x", "zfar", "znear")
        rest = tail_sum(served[2 * k + 1], shards, order)
        returned.append((base, rest))
    x_cur = x_in
    saved_list, rows_list = [], []
    for k in range(layers):
        emb_rows = dot32(pick, jnp.concatenate(returned[k], axis=0), ((1,), (0,))).astype(jnp.bfloat16)
        x_cur, saved = layer_fwd(x_cur, w_up[k], w_down[k], w_gate[k], w_proj[k], emb_rows)
        saved_list.append(saved)
        rows_list.append(emb_rows)
    d_x = d_out.astype(jnp.float32)
    layer_ops = []
    parts = [None] * layers
    for k in reversed(range(layers)):
        d_x, ops, (g, ds) = layer_bwd(d_x, saved_list[k], rows_list[k], w_up[k], w_down[k], w_gate[k], w_proj[k], k == 0)
        send = dot32(pick, g, ((0,), (0,))) * dot32(pick, ds, ((0,), (0,)))
        base = lax.all_to_all(send[:shards * BASE], "emb", 0, 0, tiled=True)
        rest = lax.all_gather(send[shards * BASE:], "emb", axis=0, tiled=True)
        parts[k] = (base, rest)
        layer_ops.append(ops)
    total = reduce_grads(layer_ops)
    grads = unpack(total, layers, w_up.shape[1], w_up.shape[2], w_gate.shape[2])
    return (x_cur, collect(got, parts, rows_dev, over)) + tuple(grads)


def padded_step(shards, tok_ids, x_in, d_out, ple_tables, w_up, w_down, w_gate, w_proj):
    layers = ple_tables.shape[0]
    rows_dev = ple_tables.shape[1]
    cap_rows = tok_ids.shape[0] // CAP_DIV
    owner_dev = tok_ids // rows_dev
    local_row = tok_ids - owner_dev * rows_dev
    owner_hot = (owner_dev[:, None] == jnp.arange(shards, dtype=jnp.int32)[None, :]).astype(jnp.int32)
    slot_rank = jnp.sum((jnp.cumsum(owner_hot, axis=0) - owner_hot) * owner_hot, axis=1)
    dest_slot = owner_dev * cap_rows + slot_rank
    req_send = jnp.zeros((shards * cap_rows,), jnp.int32).at[dest_slot].set(local_row)
    req_recv = lax.all_to_all(req_send, "emb", 0, 0, tiled=True)
    x_cur = x_in
    saved_list = []
    rows_list = []
    for layer_idx in range(layers):
        served = jnp.take(ple_tables[layer_idx], req_recv, axis=0)
        returned = lax.all_to_all(served, "emb", 0, 0, tiled=True)
        emb_rows = jnp.take(returned, dest_slot, axis=0)
        x_cur, saved = layer_fwd(x_cur, w_up[layer_idx], w_down[layer_idx], w_gate[layer_idx], w_proj[layer_idx], emb_rows)
        saved_list.append(saved)
        rows_list.append(emb_rows)
    d_x = d_out.astype(jnp.float32)
    grads_by_layer = [None] * layers
    tables_by_layer = [None] * layers
    for layer_idx in reversed(range(layers)):
        d_x, ops, (g, ds) = layer_bwd(d_x, saved_list[layer_idx], rows_list[layer_idx], w_up[layer_idx], w_down[layer_idx], w_gate[layer_idx], w_proj[layer_idx], layer_idx == 0)
        d_rows = g.astype(jnp.float32) * ds.astype(jnp.float32)
        u, a, s, o, dh, dz = ops
        grads = tuple(dot32(p, q, ((0,), (0,))) for p, q in ((u, dh), (a, o), (u, dz), (s, o)))
        grad_send = jnp.zeros((shards * cap_rows, d_rows.shape[1]), jnp.float32).at[dest_slot].set(d_rows)
        grad_recv = lax.all_to_all(grad_send, "emb", 0, 0, tiled=True)
        tables_by_layer[layer_idx] = jax.ops.segment_sum(grad_recv, req_recv, num_segments=rows_dev)
        grads_by_layer[layer_idx] = lax.psum(grads, "emb")
    grad_stacks = [jnp.stack([entry[grad_pos] for entry in grads_by_layer]) for grad_pos in range(4)]
    return (x_cur, jnp.stack(tables_by_layer), grad_stacks[0], grad_stacks[1], grad_stacks[2], grad_stacks[3])


def solution(mesh):
    shards = mesh.shape["emb"]

    def device_step(tok_ids, *rest):
        cap = tok_ids.shape[0] // CAP_DIV
        over = cap - BASE
        rows_dev = rest[2].shape[1]
        pick, got = spread(tok_ids, shards, rows_dev, cap, over)
        fits = jnp.max(got[:, 3]) <= over
        return lax.cond(fits, lambda: fast_step(cap, over, got, pick, *rest), lambda: tuple(padded_step(shards, tok_ids, *rest)))

    return jax.shard_map(
        device_step,
        mesh=mesh,
        in_specs=(P("emb"), P("emb", None), P("emb", None), P(None, "emb", None), P(), P(), P(), P()),
        out_specs=(P("emb", None), P(None, "emb", None), P(), P(), P(), P()),
        check_vma=False,
    )
```

```python
import functools

import jax
import jax.numpy as jnp
from jax import lax
from jax.experimental import pallas as pl
from jax.experimental.layout import Layout, with_layout_constraint
from jax.experimental.pallas import tpu as pltpu
from jax.sharding import PartitionSpec as P


EPS = 1e-6
CAP_DIV = 4


def gelu_tanh(pre_act):
    return jax.nn.gelu(pre_act, approximate=True)


def gelu_back(pre_act, grad_out):
    _, pull_back = jax.vjp(gelu_tanh, pre_act.astype(jnp.float32))
    return pull_back(grad_out.astype(jnp.float32))[0]


def dot32(a, b, dims):
    return lax.dot_general(a, b, (dims, ((), ())), preferred_element_type=jnp.float32)


def layer_fwd(x_cur, up_mat, down_mat, gate_mat, proj_mat, emb_rows):
    x_wide = x_cur.astype(jnp.float32)
    inv_rms = lax.rsqrt(jnp.mean(x_wide * x_wide, **ROW) + EPS)
    normed = (x_wide * inv_rms).astype(jnp.bfloat16)
    hidden = jnp.dot(normed, up_mat, preferred_element_type=jnp.float32).astype(jnp.bfloat16)
    act_out = gelu_tanh(hidden.astype(jnp.float32)).astype(jnp.bfloat16)
    mlp_out = jnp.dot(act_out, down_mat, preferred_element_type=jnp.float32).astype(jnp.bfloat16)
    gate_pre = jnp.dot(normed, gate_mat, preferred_element_type=jnp.float32).astype(jnp.bfloat16)
    gate_act = gelu_tanh(gate_pre.astype(jnp.float32)).astype(jnp.bfloat16)
    mix_rows = (gate_act.astype(jnp.float32) * emb_rows.astype(jnp.float32)).astype(jnp.bfloat16)
    ple_out = jnp.dot(mix_rows, proj_mat, preferred_element_type=jnp.float32).astype(jnp.bfloat16)
    x_next = (x_wide + mlp_out.astype(jnp.float32) + ple_out.astype(jnp.float32)).astype(jnp.bfloat16)
    return x_next, (x_cur, inv_rms, normed, hidden, act_out, gate_pre, gate_act, mix_rows)


def layer_bwd(d_x, saved, emb_rows, up_mat, down_mat, gate_mat, proj_mat, last):
    x_cur, inv_rms, normed, hidden, act_out, gate_pre, gate_act, mix_rows = saved
    x_wide = x_cur.astype(jnp.float32)
    g_out = d_x.astype(jnp.bfloat16)
    d_act = dot32(g_out, down_mat, NT).astype(jnp.bfloat16)
    d_hidden = gelu_back(hidden, d_act).astype(jnp.bfloat16)
    d_mix = dot32(g_out, proj_mat, NT).astype(jnp.bfloat16)
    d_gate_act = (emb_rows.astype(jnp.float32) * d_mix.astype(jnp.float32)).astype(jnp.bfloat16)
    d_gate_pre = gelu_back(gate_pre, d_gate_act).astype(jnp.bfloat16)
    d_x_new = None
    if not last:
        d_norm = dot32(d_hidden, up_mat, NT) + dot32(d_gate_pre, gate_mat, NT)
        d_x_new = d_x + inv_rms * d_norm - inv_rms ** 3 * x_wide * jnp.mean(d_norm * x_wide, **ROW)
    return d_x_new, (normed, act_out, mix_rows, g_out, d_hidden, d_gate_pre), (gate_act, d_mix)


AXES = ("far", "near", "y", "x", "core")
WEIGHT = {name: 1 << i for i, name in enumerate(reversed(AXES))}
ORDERS = (("core", "x", "y", "near", "far"), ("core", "y", "near", "x", "far"), ("core", "near", "x", "y", "far"))
MESH = pl.DeviceIdType.MESH
DEPTH = 2
FIRST = range(DEPTH)
LAG = 2
NN, NT, TN = ((1,), (0,)), ((1,), (1,)), ((0,), (0,))
ROW = {"axis": -1, "keepdims": True}
HALF, QUART, EIGHTH = 128, 64, 32


def bit(v):
    return lax.rem(v, 2)


def loop(first, last, body):
    def step(i, carry):
        body(i)
        return carry

    lax.fori_loop(first, last, step, 0)


def swap(a):
    return lax.all_to_all(a, "emb", 0, 0, tiled=True)


def line(i):
    return pl.ds(i, 1)


def col(v):
    return v[:, None]


def row(v):
    return v[None, :]


def numbers(n):
    return jnp.arange(n, dtype=jnp.int32)


BLK = 256
NB = 16
NS = 8


def reduce_kernel(sizes, *refs):
    n_layers, per, n = sizes
    u_0, a_0, us, as_, ss, os_, dhs, dzs, send_t, out, tails = refs[:11]
    (v_as, v_o, v_u, v_d, blk1, blk2, blk3, rc1, rc2, rc3, rf1, rf2, rs1, rs2, ri1, ri2, rm1, rm2, fin1, fin2,
     ri3, rm3, rx3, rf3, rs3, fin3, ssem, rsem, lsem, osem, tv, tsem, trsem, tlsem) = refs[11:]
    me = lax.axis_index("emb")
    core, x, y, z = bit(me), bit(me // 2), bit(me // 4), me // 8
    mid = (z == 1) | (z == 2)
    end = (z == 0) | (z == 3)
    zb = z // 2
    p_core = me + 1 - 2 * core
    p_x = me + 2 - 4 * x
    p_y = me + 4 - 8 * y
    step_in = jnp.where((z == 0) | (z == 1), 8, -8)
    p_side = jnp.where((z == 0) | (z == 2), me + 8, me - 8)
    p_mid = jnp.where(z == 1, me + 8, jnp.where(z == 2, me - 8, me))

    barrier = pltpu.get_barrier_semaphore()
    p_far = me + 16 - EIGHTH * zb
    for dev in (p_core, p_x, p_y, p_side, p_far):
        pl.semaphore_signal(barrier, inc=1, device_id=(dev,), device_id_type=MESH)

    @pl.when(mid)
    def _():
        pl.semaphore_signal(barrier, inc=1, device_id=(p_mid,), device_id_type=MESH)
        pl.semaphore_wait(barrier, 6)

    @pl.when(end)
    def _():
        pl.semaphore_wait(barrier, 5)

    def loads(ell):
        layer = n_layers - 1 - ell
        u, a = (us.at[layer - 1], as_.at[layer - 1]) if layer else (u_0, a_0)
        s, o, dh, dz = (t.at[layer] for t in (ss, os_, dhs, dzs))
        slot = ell % 2
        hid = a_0.shape[1]
        left, right = pl.ds(0, hid), pl.ds(hid, BLK)
        ways = ((a, v_as.at[slot, :, left]), (s, v_as.at[slot, :, right]), (o, v_o.at[slot]), (u, v_u.at[slot]),
                (dh, v_d.at[slot, :, left]), (dz, v_d.at[slot, :, right]))
        return [pltpu.make_async_copy(src, dst, osem.at[slot, i]) for i, (src, dst) in enumerate(ways)]

    emb = tv.shape[2]
    spot = {"far": z // 2, "near": bit(z), "y": y, "x": x, "core": core}
    other = {"far": p_far, "near": p_side, "y": p_y, "x": p_x, "core": p_core}
    t_half = tv.shape[1] // 2

    def tail_copy(layer, s, p):
        order = tuple(reversed(ORDERS[layer]))
        block = p // 2
        at = {name: bit(block // (1 << t)) for t, name in enumerate(order[:s])}
        where = tuple(at.get(name, spot[name]) for name in AXES)
        ref = tails.at[(layer,) + where + (pl.ds(pl.multiple_of(bit(p) * t_half, t_half), t_half),)]
        i = lax.rem(p, 4)
        return pltpu.make_async_remote_copy(src_ref=ref, dst_ref=ref, send_sem=tsem.at[layer, s, i], recv_sem=trsem.at[layer, s, i],
                                            device_id=(other[order[s]],), device_id_type=MESH)

    t_first = [4]
    for s in range(len(AXES)):
        t_first.append(t_first[-1] + (2 << s) + 2)
    t_in = [pltpu.make_async_copy(send_t.at[:, pl.ds(k * emb, emb)], tv.at[k], tlsem.at[k]) for k in range(n_layers)]
    t_own = [pltpu.make_async_copy(tv.at[k], tails.at[(k,) + tuple(spot[name] for name in AXES)], tlsem.at[k]) for k in range(n_layers)]
    for c in t_in:
        c.start()
    for c, d in zip(t_in, t_own):
        c.wait()
        d.start()
    for c in t_own:
        c.wait()
    for ell in (0, 1):
        for c in loads(ell):
            c.start()
    for c in loads(0):
        c.wait()

    span = n // n_layers
    rest = {0: 2, 1: 4}

    def active(k, kind):
        return True if kind == 2 else lax.rem(k, 5) != rest[kind]

    def unit(k, kind):
        t = lax.rem(k, span)
        if kind == 2:
            return span * 4 // 5 + t // 2
        p = lax.rem(t, 5)
        return 4 * (t // 5) + p - (p > rest[kind]).astype(jnp.int32)

    def where_out(k, kind):
        base = {0: 0, 1: per, 2: per * bit(k)}[kind]
        return (n_layers - 1 - k // span) * 2 * per + base + unit(k, kind)

    def block(slot, w, wide):
        if wide:
            rb, cb = w // 13, lax.rem(w, 13)
            lhs, rhs = v_u, v_d
        else:
            rb, cb = lax.rem(w, 13), w // 13
            lhs, rhs = v_as, v_o
        lv = lhs[slot, :, pl.ds(pl.multiple_of(rb * BLK, BLK), BLK)]
        rv = rhs[slot, :, pl.ds(pl.multiple_of(cb * BLK, BLK), BLK)]
        return dot32(lv, rv, TN)

    h0 = core * HALF
    flows = []

    def add_flow(off, src, dst, dev, send_if=None, recv_if=None):
        flows.append((len(flows), off, src, dst, dev, send_if, recv_if))
        return flows[-1]

    def rows(start, size):
        return pl.ds(pl.multiple_of(start, EIGHTH), size)

    def desc(f, k):
        idx, _, src, dst, dev, _, _ = f
        d = dev(k) if callable(dev) else dev
        return pltpu.make_async_remote_copy(
            src_ref=src(k), dst_ref=dst(k), send_sem=ssem.at[idx, lax.rem(k, NB)], recv_sem=rsem.at[idx, lax.rem(k, NB)],
            device_id=(d,), device_id_type=MESH)

    def ok(k, cond):
        v = (k >= 0) & (k < n)
        return v if cond is None else v & (cond(k) if callable(cond) else cond)

    acts = []

    def clock():
        now = [-1]

        def at(more=LAG):
            now[0] += more
            return now[0]

        return at

    def xyz(kind, blk, rc, rf, rs, ri, rm, fin, f, s, p_f, p_s):
        at = clock()
        q0, q1 = h0 + f * QUART, h0 + (1 - f) * QUART
        e0, e1 = q0 + s * EIGHTH, q0 + (1 - s) * EIGHTH
        b = lambda k: lax.rem(k, NB)
        m = lambda k: lax.rem(k, NS)
        o = lambda k: where_out(k, kind)
        go = lambda k: active(k, kind)
        on = lambda side: (lambda k: side & active(k, kind))
        f_core = add_flow(at(), lambda k: blk.at[b(k), rows(HALF - h0, HALF)], lambda k: rc.at[m(k)], p_core, go, go)
        f_first = add_flow(at(), lambda k: blk.at[b(k), rows(q1, QUART)], lambda k: rf.at[m(k)], p_f, go, go)
        f_second = add_flow(at(), lambda k: blk.at[b(k), rows(e1, EIGHTH)], lambda k: rs.at[m(k)], p_s, go, go)
        f_in = add_flow(at(), lambda k: blk.at[b(k), rows(e0, EIGHTH)], lambda k: ri.at[m(k)], p_side, on(end), on(mid))
        f_mid = add_flow(at(), lambda k: blk.at[b(k), rows(e0, EIGHTH)], lambda k: rm.at[m(k)], p_mid, on(mid), on(mid))
        f_out = add_flow(at(), lambda k: fin.at[b(k)], lambda k: fin.at[b(k)], p_side, on(mid), on(end))
        g_s = add_flow(at(), lambda k: fin.at[b(k)], lambda k: out.at[o(k), rows(e0, EIGHTH)], p_s, go, go)
        g_f = add_flow(at(), lambda k: out.at[o(k), rows(q0, QUART)], lambda k: out.at[o(k), rows(q0, QUART)], p_f, go, go)
        g_c = add_flow(at(), lambda k: out.at[o(k), rows(h0, HALF)], lambda k: out.at[o(k), rows(h0, HALF)], p_core, go, go)

        def plus(dst0, size, src):
            def add(k):
                r = rows(dst0, size)
                blk[b(k), r] = blk[b(k), r] + src[m(k)]

            return add

        def final(k):
            fin[b(k)] = blk[b(k), rows(e0, EIGHTH)] + rm[m(k)]

        acts.append((f_core, plus(h0, HALF, rc)))
        acts.append((f_first, plus(q0, QUART, rf)))
        acts.append((f_second, plus(e0, EIGHTH, rs)))
        acts.append((f_in, plus(e0, EIGHTH, ri)))
        acts.append((f_mid, final))
        acts.extend((g, None) for g in (f_out, g_s, g_f, g_c))
        locals_.append((g_s[1], lambda k: pltpu.make_async_copy(fin.at[b(k)], out.at[o(k), rows(e0, EIGHTH)], lsem.at[kind, m(k)]), go))

    def zfirst(kind, blk, rc, ri, rm, rx, rf, rs, fin):
        at = clock()
        odd = lambda k: bit(k) == 1
        at_end = lambda k: bit(k // 2) == 1
        here = lambda k: jnp.where(at_end(k), end, mid)
        q0, q1 = h0 + zb * QUART, h0 + (1 - zb) * QUART
        b = lambda k: lax.rem(k, NB)
        m = lambda k: lax.rem(k, NS)
        o = lambda k: where_out(k, kind)
        f = lambda k: jnp.where(odd(k), y, x)
        e0 = lambda k: q0 + f(k) * EIGHTH
        e1 = lambda k: q0 + (1 - f(k)) * EIGHTH
        p_f = lambda k: jnp.where(odd(k), p_y, p_x)
        p_s = lambda k: jnp.where(odd(k), p_x, p_y)
        e_root = lambda side: (lambda k: side & at_end(k))
        m_root = lambda side: (lambda k: side & jnp.logical_not(at_end(k)))
        f_core = add_flow(at(), lambda k: blk.at[b(k), rows(HALF - h0, HALF)], lambda k: rc.at[m(k)], p_core)
        f_in = add_flow(at(), lambda k: blk.at[b(k), rows(h0, HALF)], lambda k: ri.at[b(k)], p_side, m_root(end), m_root(mid))
        f_in2 = add_flow(at(0), lambda k: blk.at[b(k), rows(q1, QUART)], lambda k: ri.at[b(k), pl.ds(0, QUART)], p_side, e_root(end), e_root(mid))
        f_mid = add_flow(at(), lambda k: blk.at[b(k), rows(q1, QUART)], lambda k: rm.at[m(k)], p_mid, mid, mid)
        f_x = add_flow(at(), lambda k: blk.at[b(k), rows(q0, QUART)], lambda k: rx.at[m(k)], p_side, e_root(mid), e_root(end))
        f_first = add_flow(at(), lambda k: blk.at[b(k), rows(e1(k), EIGHTH)], lambda k: rf.at[m(k)], p_f, here, here)
        f_second = add_flow(at(), lambda k: blk.at[b(k), rows(e0(k), EIGHTH)], lambda k: rs.at[m(k)], p_s, here, here)
        g_f = add_flow(at(), lambda k: fin.at[m(k)], lambda k: out.at[o(k), rows(e0(k), EIGHTH)], p_f, here, here)
        g_x = add_flow(at(), lambda k: out.at[o(k), rows(q0, QUART)], lambda k: out.at[o(k), rows(q0, QUART)], p_side, e_root(end), e_root(mid))
        g_m = add_flow(at(), lambda k: out.at[o(k), rows(q0, QUART)], lambda k: out.at[o(k), rows(q0, QUART)], p_mid, mid, mid)
        g_o = add_flow(at(), lambda k: out.at[o(k), rows(h0, HALF)], lambda k: out.at[o(k), rows(h0, HALF)], p_side, m_root(mid), m_root(end))
        g_o2 = add_flow(at(0), lambda k: out.at[o(k), rows(q1, QUART)], lambda k: out.at[o(k), rows(q1, QUART)], p_side, e_root(mid), e_root(end))
        g_c = add_flow(at(), lambda k: out.at[o(k), rows(h0, HALF)], lambda k: out.at[o(k), rows(h0, HALF)], p_core)

        def plus(start, size, src):
            def go(k):
                r = rows(start(k), size)
                blk[b(k), r] = blk[b(k), r] + src(k)

            return go

        def final(k):
            fin[m(k)] = blk[b(k), rows(e0(k), EIGHTH)] + rs[m(k)]

        acts.append((f_core, plus(lambda k: h0, HALF, lambda k: rc[m(k)])))
        acts.append((f_in, plus(lambda k: h0, HALF, lambda k: ri[b(k)])))
        acts.append((f_in2, plus(lambda k: q1, QUART, lambda k: ri[b(k), :QUART])))
        acts.append((f_mid, plus(lambda k: q0, QUART, lambda k: rm[m(k)])))
        acts.append((f_x, plus(lambda k: q0, QUART, lambda k: rx[m(k)])))
        acts.append((f_first, plus(e0, EIGHTH, lambda k: rf[m(k)])))
        acts.append((f_second, final))
        acts.extend((g, None) for g in (g_f, g_x, g_m, g_o, g_o2, g_c))
        locals_.append((g_f[1], lambda k: pltpu.make_async_copy(fin.at[m(k)], out.at[o(k), rows(e0(k), EIGHTH)], lsem.at[kind, m(k)]), here))

    locals_ = []
    xyz(0, blk1, rc1, rf1, rs1, ri1, rm1, fin1, x, y, p_x, p_y)
    xyz(1, blk2, rc2, rf2, rs2, ri2, rm2, fin2, y, x, p_y, p_x)
    zfirst(2, blk3, rc3, ri3, rm3, rx3, rf3, rs3, fin3)

    def round_(r):
        for f in flows:
            _, off, _, _, _, give, _ = f
            k = r - off - LAG - LAG

            @pl.when(ok(k, give))
            def _(f=f, k=k):
                desc(f, k).wait_send()
        for off, mk, cond in locals_:
            k = r - off - LAG

            @pl.when(ok(k, cond))
            def _(mk=mk, k=k):
                mk(k).wait()
        for f, fn in acts:
            _, off, _, _, _, _, take = f
            k = r - off - LAG

            @pl.when(ok(k, take))
            def _(f=f, fn=fn, k=k):
                desc(f, k).wait_recv()
                if fn is not None:
                    fn(k)
        for s in range(len(AXES)):
            p = r - t_first[s]

            @pl.when((p >= 2) & (p < (2 << s) + 2))
            def _(s=s, p=p):
                for k in range(n_layers):
                    tail_copy(k, s, p - 2).wait()

            @pl.when((p >= 0) & (p < (2 << s)))
            def _(s=s, p=p):
                for k in range(n_layers):
                    tail_copy(k, s, p).start()
        for ell in range(1, n_layers):
            @pl.when(r == span * ell)
            def _(ell=ell):
                for c in loads(ell):
                    c.wait()
        for f in flows:
            _, off, _, _, _, give, _ = f
            k = r - off

            @pl.when(ok(k, give))
            def _(f=f, k=k):
                desc(f, k).start()
        for off, mk, cond in locals_:
            k = r - off

            @pl.when(ok(k, cond))
            def _(mk=mk, k=k):
                mk(k).start()

        slot = bit(r // span)
        s = lax.rem(r, NB)
        odd = bit(r) == 1

        @pl.when((r < n) & active(r, 0))
        def _():
            blk1[s] = block(slot, unit(r, 0), False)

        @pl.when((r < n) & active(r, 1))
        def _():
            blk2[s] = block(slot, unit(r, 1), True)

        @pl.when((r < n) & odd)
        def _():
            blk3[s] = block(slot, unit(r, 2), True)

        @pl.when((r < n) & jnp.logical_not(odd))
        def _():
            blk3[s] = block(slot, unit(r, 2), False)

        for ell in range(2, n_layers):
            @pl.when(r == span * (ell - 1) - 1)
            def _(ell=ell):
                for c in loads(ell):
                    c.start()

    loop(0, n + 25, round_)


def reduce_grads(u_0, a_0, us, as_, ss, os_, dhs, dzs, send_t):
    n_layers, toks, wide = ss.shape[0], u_0.shape[0], a_0.shape[1] + ss.shape[2]
    dim = u_0.shape[1]
    over, emb = send_t.shape[0], ss.shape[2]
    per = (wide // BLK) * (dim // BLK)
    n = per * 10 // 13 * n_layers
    f32, bf = jnp.float32, jnp.bfloat16
    V = pltpu.VMEM

    def many(count, slots, rows):
        return [V((slots, rows, BLK), f32)] * count

    big, small = (DEPTH, toks, wide), (DEPTH, toks, dim)
    scratch = [V(big, bf), V(small, bf), V(small, bf), V(big, bf)]
    scratch += many(3, NB, BLK) + many(3, NS, HALF) + many(DEPTH, NS, QUART) + many(6, NS, EIGHTH) + many(DEPTH, NB, EIGHTH)
    scratch += many(1, NB, HALF) + many(DEPTH, NS, QUART) + many(3, NS, EIGHTH)
    D = pltpu.SemaphoreType.DMA
    scratch += [D((31, NB)), D((31, NB)), D((3, NS)), D((DEPTH, 6))]
    scratch += [V((n_layers, over, emb), f32)] + [D((n_layers, len(AXES), LAG + LAG))] * DEPTH + [D((n_layers,))]
    flat = (u_0, a_0, us, as_, ss, os_, dhs, dzs, send_t)
    return pl.pallas_call(
        functools.partial(reduce_kernel, (n_layers, per, n)),
        out_shape=[jax.ShapeDtypeStruct((2 * per * n_layers, BLK, BLK), f32),
                   jax.ShapeDtypeStruct((n_layers,) + (2,) * len(AXES) + (over, emb), f32)],
        in_specs=[pl.BlockSpec(memory_space=pl.ANY)] * len(flat),
        out_specs=[pl.BlockSpec(memory_space=pl.ANY)] * 2,
        scratch_shapes=scratch,
        compiler_params=pltpu.CompilerParams(collective_id=0, has_side_effects=True, vmem_limit_bytes=66_000_000),
        cost_estimate=pl.CostEstimate(flops=600 * 10**9, bytes_accessed=10**8, transcendentals=0),
        name="reduce_grads",
    )(*flat)


TILE = 256
FCH = 512
GK = 0.7978845608028654
GC = 0.044715


def gelu_f(h):
    return (0.5 * h) * (1.0 + jnp.tanh(h * (GK + (GK * GC) * (h * h))))


def gelu_g(h, g):
    h2 = h * h
    t = jnp.tanh(h * (GK + (GK * GC) * h2))
    return g * (0.5 * (1.0 + t) + (0.5 * h) * (1.0 - t * t) * (GK + (3.0 * GK * GC) * h2))


def model_kernel(*refs):
    (x0, m0, h0, z0, g0, base, t0, t1, t2, pick, pick_t, d_out, w_up, w_down, w_gate, w_proj,
     x_out, us, as_, ss, os_, dhs, dzs, hs, send_b, send_t,
     wug, wd, wp, wp0, xs, cs, hbuf, abuf, ubuf, obuf, pbuf, sbuf, zs, es, gs, invs, dus, dsv, sb, st,
     wsem, usem, hsem, asem, osem, isem, jsem, psem, ssem, zsem, vsem) = refs
    f32, bf = jnp.float32, jnp.bfloat16
    slots = base.shape[0]
    n_tiles = xs.shape[1] // TILE
    top = es.shape[0] - 1
    ends = range(n_tiles - DEPTH, n_tiles)
    hid = hbuf.shape[2]
    emb = wp0.shape[0]
    dim = wp0.shape[1]

    def rows(i):
        return pl.ds(pl.multiple_of(i * TILE, TILE), TILE)

    def mm(a, b):
        return dot32(a, b, NN)

    def mt(a, b):
        return dot32(a, b, NT)

    cp = pltpu.make_async_copy

    def weights(layer, slot):
        ways = ((w_up, wug.at[slot, :, pl.ds(0, hid)]), (w_down, wd.at[slot]), (w_gate, wug.at[slot, :, pl.ds(hid, emb)]), (w_proj, wp.at[slot]))
        return [cp(src.at[layer], dst, wsem.at[slot, i]) for i, (src, dst) in enumerate(ways)]

    first = cp(w_proj.at[0], wp0, wsem.at[0, 4])
    first.start()
    w1, w2 = weights(1, 0), weights(2, 1)
    for c in w1 + w2:
        c.start()

    def slot_of(i):
        return bit(i)

    def in_x(i):
        return cp(x0.at[rows(i)], ubuf.at[slot_of(i)], isem.at[slot_of(i)])

    def in_p(i):
        return cp(pick.at[rows(i)], pbuf.at[slot_of(i)], psem.at[slot_of(i)])

    def in_m(i):
        return cp(m0.at[rows(i)], obuf.at[slot_of(i)], jsem.at[slot_of(i)])

    def put(src, dst, layer, sem):
        return lambda i: cp(src.at[slot_of(i)], dst.at[layer, rows(i)] if layer is not None else dst.at[rows(i)], sem.at[slot_of(i)])

    tails = (t0, t1, t2)

    def rows_of(layer, i):
        in_p(i).wait()
        p = pbuf[slot_of(i)]
        return (mm(p[:, :slots], base[:, layer * emb:(layer + 1) * emb]) + mm(p[:, slots:], tails[layer][...])).astype(bf)

    for i in FIRST:
        in_x(i).start()
        in_m(i).start()
        in_p(i).start()
    first.wait()
    put_s = lambda layer: (lambda i: cp(sbuf.at[slot_of(i)], ss.at[layer, rows(i)], ssem.at[slot_of(i)]))

    def finish0(i):
        r, k = rows(i), slot_of(i)

        @pl.when(i >= DEPTH)
        def _():
            put_s(0)(i - DEPTH).wait()

        e = rows_of(0, i)
        es[0, r] = e
        s = (g0[r].astype(f32) * e.astype(f32)).astype(bf)
        sbuf[k] = s
        put_s(0)(i).start()
        q = mm(s, wp0[...]).astype(bf)
        in_x(i).wait()
        in_m(i).wait()
        xs[0, r] = (ubuf[k].astype(f32) + obuf[k].astype(f32) + q.astype(f32)).astype(bf)

        @pl.when(i + DEPTH < n_tiles)
        def _():
            in_x(i + DEPTH).start()
            in_m(i + DEPTH).start()
            in_p(i + DEPTH).start()

    loop(0, n_tiles, finish0)
    for i in ends:
        put_s(0)(i).wait()

    def fwd(layer, slot, loaded):
        below = layer - 1
        outs = [put(ubuf, us, below, usem), put(hbuf, hs, below, hsem), put_s(layer),
                lambda i: cp(abuf.at[slot_of(i), :, pl.ds(0, hid)], as_.at[below, rows(i)], asem.at[slot_of(i)])]
        if layer == top:
            outs.append(put(obuf, x_out, None, osem))
        for c in loaded:
            c.wait()
        for i in FIRST:
            in_p(i).start()

        def tile(i):
            r, k = rows(i), slot_of(i)

            @pl.when(i >= DEPTH)
            def _():
                for o in outs:
                    o(i - DEPTH).wait()

            x = xs[below, r].astype(f32)
            inv = lax.rsqrt(jnp.mean(x * x, **ROW) + EPS)
            invs[below, r] = jnp.broadcast_to(inv, (TILE, invs.shape[2]))
            u = (x * inv).astype(bf)
            ubuf[k] = u
            for c0 in range(0, hid, FCH):
                h = mm(u, wug[slot, :, c0:c0 + FCH]).astype(bf)
                hbuf[k, :, c0:c0 + FCH] = h
                abuf[k, :, c0:c0 + FCH] = gelu_f(h.astype(f32)).astype(bf)
            z = mm(u, wug[slot, :, hid:]).astype(bf)
            g = gelu_f(z.astype(f32)).astype(bf)
            zs[below, r] = z
            gs[below, r] = g
            e = rows_of(layer, i)
            es[layer, r] = e
            s = (g.astype(f32) * e.astype(f32)).astype(bf)
            sbuf[k] = s
            for c0 in range(0, dim, FCH):
                c1 = c0 + FCH
                q = mm(s, wp[slot, :, c0:c1]).astype(bf)
                m = mm(abuf[k, :, :hid], wd[slot, :, c0:c1]).astype(bf)
                new = (xs[below, r, c0:c1].astype(f32) + m.astype(f32) + q.astype(f32)).astype(bf)
                if layer == top:
                    obuf[k, :, c0:c1] = new
                else:
                    xs[layer, r, c0:c1] = new
            for o in outs:
                o(i).start()

            @pl.when(i + DEPTH < n_tiles)
            def _():
                in_p(i + DEPTH).start()

        loop(0, n_tiles, tile)
        for i in ends:
            for o in outs:
                o(i).wait()

    def in_h(layer, i):
        below = layer - 1
        return cp(h0.at[rows(i)] if layer == 0 else hs.at[below, rows(i)], hbuf.at[slot_of(i)], hsem.at[slot_of(i)])

    def bwd(layer, slot):
        below = layer - 1
        outs = [lambda i: cp(abuf.at[slot_of(i), :, pl.ds(0, hid)], dhs.at[layer, rows(i)], asem.at[slot_of(i)]),
                lambda i: cp(abuf.at[slot_of(i), :, pl.ds(hid, emb)], dzs.at[layer, rows(i)], zsem.at[slot_of(i)]),
                put(obuf, os_, layer, osem)]
        proj = wp0 if layer == 0 else wp.at[slot]

        def in_d(i):
            return cp(d_out.at[rows(i)], ubuf.at[slot_of(i)], isem.at[slot_of(i)])

        if layer == top:
            for i in FIRST:
                in_h(layer, i).start()
                in_d(i).start()

        def tile(i):
            r, k = rows(i), slot_of(i)

            @pl.when(i >= DEPTH)
            def _():
                for o in outs:
                    o(i - DEPTH).wait()

            if layer == top:
                in_d(i).wait()
                cs[r] = ubuf[k].astype(f32)
            o = cs[r].astype(bf)
            obuf[k] = o
            ds = mt(o, proj[...]).astype(bf)
            dsv[r] = ds
            z = (z0[r] if layer == 0 else zs[below, r]).astype(f32)
            dg = (es[layer, r].astype(f32) * ds.astype(f32)).astype(bf)
            abuf[k, :, hid:] = gelu_g(z, dg.astype(f32)).astype(bf)
            in_h(layer, i).wait()
            for c0 in range(0, hid, FCH):
                da = mt(o, wd[slot, c0:c0 + FCH]).astype(bf)
                abuf[k, :, c0:c0 + FCH] = gelu_g(hbuf[k, :, c0:c0 + FCH].astype(f32), da.astype(f32)).astype(bf)
            if layer > 0:
                dot = jnp.zeros((TILE, 1), f32)
                for c0 in range(0, dim, FCH):
                    du = mt(abuf[k], wug[slot, c0:c0 + FCH])
                    dus[:, c0:c0 + FCH] = du
                    dot = dot + jnp.sum(du * xs[below, r, c0:c0 + FCH].astype(f32), **ROW)
                inv = invs[below, r][:, :1]
                back = (inv * inv * inv) * (dot * (1.0 / dim))
                for c0 in range(0, dim, FCH):
                    c1 = c0 + FCH
                    cs[r, c0:c1] = cs[r, c0:c1] + inv * dus[:, c0:c1] - back * xs[below, r, c0:c1].astype(f32)
            for ot in outs:
                ot(i).start()

            @pl.when(i + DEPTH < n_tiles)
            def _():
                in_h(layer, i + DEPTH).start()
                if layer == top:
                    in_d(i + DEPTH).start()

        loop(0, n_tiles, tile)
        if layer > 0:
            for i in FIRST:
                in_h(below, i).start()
        g = g0 if layer == 0 else gs.at[below]
        d = g[...].astype(f32) * dsv[...].astype(f32)
        high = d.astype(bf)
        low = (d - high.astype(f32)).astype(bf)
        for c0 in range(0, slots, 256):
            p = pick_t[c0:c0 + 256]
            sb[c0:c0 + 256] = mm(p, high) + mm(p, low)
        p = pick_t[slots:]
        st[...] = mm(p, high) + mm(p, low)
        lanes = slice(layer * emb, (layer + 1) * emb)
        both = [cp(sb, send_b.at[:, lanes], vsem.at[0]), cp(st, send_t.at[:, lanes], vsem.at[1])]
        for c in both:
            c.start()
        for i in ends:
            for o in outs:
                o(i).wait()
        for c in both:
            c.wait()

    fwd(1, 0, w1)
    fwd(2, 1, w2)
    bwd(2, 1)
    last = cp(w_down.at[0], wd.at[1], wsem.at[1, 1])
    last.start()
    bwd(1, 0)
    last.wait()
    bwd(0, 1)


def run_model(pre, base, tails, pick, pick_t, d_out, w_up, w_down, w_gate, w_proj):
    x0, m0, h0, z0, g0 = pre
    layers, dim, hid = w_up.shape
    emb = w_gate.shape[2]
    toks = x0.shape[0]
    slots, over = base.shape[0], tails[0].shape[0]
    below = layers - 1
    f32, bf = jnp.float32, jnp.bfloat16
    hbm, vm = pl.BlockSpec(memory_space=pl.ANY), pl.BlockSpec(memory_space=pltpu.VMEM)
    S = jax.ShapeDtypeStruct
    V = pltpu.VMEM
    D = pltpu.SemaphoreType.DMA
    return pl.pallas_call(
        model_kernel,
        in_specs=[hbm] * 3 + [vm] * 6 + [hbm] + [vm] + [hbm] * 5,
        out_specs=[hbm] * 10,
        out_shape=[S((toks, dim), bf), S((below, toks, dim), bf), S((below, toks, hid), bf), S((layers, toks, emb), bf),
                   S((layers, toks, dim), bf), S((layers, toks, hid), bf), S((layers, toks, emb), bf), S((below, toks, hid), bf),
                   S((slots, layers * emb), f32), S((over, layers * emb), f32)],
        scratch_shapes=[
            V((DEPTH, dim, hid + emb), bf), V((DEPTH, hid, dim), bf), V((DEPTH, emb, dim), bf), V((emb, dim), bf),
            V((DEPTH, toks, dim), bf), V((toks, dim), f32), V((DEPTH, TILE, hid), bf), V((DEPTH, TILE, hid + emb), bf),
            V((DEPTH, TILE, dim), bf), V((DEPTH, TILE, dim), bf), V((DEPTH, TILE, slots + over), bf), V((DEPTH, TILE, emb), bf),
            V((DEPTH, toks, emb), bf), V((layers, toks, emb), bf), V((DEPTH, toks, emb), bf), V((DEPTH, toks, 128), f32), V((TILE, dim), f32),
            V((toks, emb), bf), V((slots, emb), f32), V((over, emb), f32),
            D((DEPTH, 5))] + [D((DEPTH,))] * 10,
        compiler_params=pltpu.CompilerParams(vmem_limit_bytes=67_000_000),
        name="model",
    )(x0, m0, h0, z0, g0, base, *tails, pick, pick_t, d_out, w_up, w_down, w_gate, w_proj)


BASE = 32
TAIL = 128


def spread(tok_ids, shards, rows_dev):
    toks = tok_ids.shape[0]
    i32, f32, bf = jnp.int32, jnp.float32, jnp.bfloat16
    owner = tok_ids // rows_dev
    local = tok_ids - owner * rows_dev
    row_no = lax.broadcasted_iota(i32, (toks, toks), 0)
    col_no = lax.broadcasted_iota(i32, (toks, toks), 1)
    same = col(tok_ids) == row(tok_ids)
    seen = jnp.max(jnp.where(same & (col_no < row_no), 1.0, 0.0), axis=1)
    new = 1.0 - seen
    hot32 = (col(owner) == row(numbers(shards))).astype(f32)
    fresh = hot32 * col(new)
    before = (row_no > col_no).astype(bf)
    ahead = jnp.dot(before, fresh.astype(bf), preferred_element_type=f32)
    rank = jnp.sum(ahead * hot32, axis=1)
    count = jnp.sum(fresh, axis=0)
    extra = jnp.maximum(count - BASE, 0.0)
    lower = lax.broadcasted_iota(i32, (shards, shards), 0) > lax.broadcasted_iota(i32, (shards, shards), 1)
    start = jnp.sum(jnp.where(lower, row(extra), 0.0), axis=1)
    tail = jnp.sum(hot32 * row(start), axis=1)
    place = jnp.where(rank < BASE, owner.astype(f32) * BASE + rank, shards * BASE + tail + rank - BASE)
    row_new = jnp.max(jnp.where(same & (row_no < col_no), 1.0, 0.0), axis=0) == 0.0
    slot = jnp.sum(jnp.where(same & row(row_new), row(place), 0.0), axis=1).astype(i32)
    n_slots = shards * BASE + TAIL
    pick = (col(slot) == lax.broadcasted_iota(i32, (toks, n_slots), 1)).astype(bf)
    pick_t = (row(slot) == lax.broadcasted_iota(i32, (n_slots, toks), 0)).astype(bf)
    parts = (jnp.stack([local // 64, local % 64], axis=1).astype(f32) * col(new)).astype(bf)
    want = jnp.dot(pick_t, parts, preferred_element_type=f32)
    want = (want[:, 0] * 64.0 + want[:, 1]).astype(i32)
    base = want[:shards * BASE].reshape(shards, BASE)
    rest = jnp.broadcast_to(want[shards * BASE:][None, :], (shards, TAIL))
    info = jnp.stack([count, start, extra, jnp.broadcast_to(jnp.sum(extra), (shards,))], axis=1).astype(i32)
    pad = jnp.zeros((shards, INFO - 4), i32)
    sent = jnp.concatenate([info, pad, base, rest], axis=1)
    got = swap(sent)
    return pick, pick_t, got


INFO = 128


def serve_kernel(n_layers, over, got, tables, *refs):
    base_out, outs, (tab, wide, stage, sem) = refs[0], refs[1:1 + n_layers], refs[1 + n_layers:]
    shards = got.shape[0]
    emb = wide.shape[2]
    loads = [pltpu.make_async_copy(tables.at[k], tab.at[k], sem.at[k]) for k in range(n_layers)]
    for c in loads:
        c.start()
    for k in range(n_layers):
        loads[k].wait()
        whole = wide.shape[1] // BLK * BLK

        def widen(i, k=k):
            r = pl.ds(pl.multiple_of(i * BLK, BLK), BLK)
            wide[k, r] = tab[k, r].astype(jnp.float32)

        loop(0, whole // BLK, widen)
        wide[k, whole:] = tab[k, whole:].astype(jnp.float32)

    def one(j):
        start, extra = got[j, 1], got[j, 2]

        def rows8(g):
            at = [got[j, INFO + g * 8 + i] for i in range(8)]
            for i in range(8):
                for k in range(n_layers):
                    stage[k, line(g * 8 + i)] = wide[k, line(at[i])]

        loop(0, BASE // 8, rows8)
        for k in range(n_layers):
            base_out[j, :, k * emb:(k + 1) * emb] = stage[k, :BASE].astype(jnp.bfloat16)

        @pl.when(extra == 0)
        def _():
            for k in range(n_layers):
                outs[k][j] = jnp.zeros((over, emb), jnp.bfloat16)

        @pl.when(extra > 0)
        def _():
            stage[...] = jnp.zeros_like(stage)

            def four(g):
                at = [got[j, INFO + BASE + start + g * 4 + i] for i in range(4)]
                for i in range(4):
                    for k in range(n_layers):
                        stage[k, line(start + g * 4 + i)] = wide[k, line(at[i])]

            def single(i):
                at = got[j, INFO + BASE + start + i]
                for k in range(n_layers):
                    stage[k, line(start + i)] = wide[k, line(at)]

            loop(0, extra // 4, four)
            loop(extra // 4 * 4, extra, single)
            for k in range(n_layers):
                outs[k][j] = stage[k].astype(jnp.bfloat16)

    loop(0, shards, one)


def serve(got, tables, over):
    n_layers, rows_dev, emb = tables.shape
    shards = got.shape[0]
    bf = jnp.bfloat16
    shapes = [jax.ShapeDtypeStruct((shards, BASE, n_layers * emb), bf)] + [jax.ShapeDtypeStruct((shards, over, emb), bf)] * n_layers
    return pl.pallas_call(
        functools.partial(serve_kernel, n_layers, over),
        in_specs=[pl.BlockSpec(memory_space=pltpu.SMEM), pl.BlockSpec(memory_space=pl.ANY)],
        out_specs=[pl.BlockSpec(memory_space=pltpu.VMEM)] * (1 + n_layers),
        out_shape=shapes,
        scratch_shapes=[pltpu.VMEM((n_layers, rows_dev, emb), bf), pltpu.VMEM((n_layers, rows_dev, emb), jnp.float32),
                        pltpu.VMEM((n_layers, over, emb), jnp.float32), pltpu.SemaphoreType.DMA((n_layers,))],
        compiler_params=pltpu.CompilerParams(vmem_limit_bytes=60_000_000),
        name="serve_rows",
    )(got, tables)


STEPS = 24


def finish_kernel(got, base, tail, total, table, down, proj, up, gate, base_v, tail_v, acc, sem):
    step = pl.program_id(0)
    shards = got.shape[0]
    n_layers, _, emb = acc.shape
    first = pltpu.make_async_copy(base, base_v, sem.at[0])
    second = pltpu.make_async_copy(tail, tail_v, sem.at[1])
    done = pltpu.make_async_copy(acc, table, sem.at[2])
    n = total.shape[0] - 1
    lanes = [slice(k * emb, (k + 1) * emb) for k in range(n_layers)]

    @pl.when(step == 0)
    def _():
        first.start()
        second.start()
        whole = acc.shape[1] // BLK * BLK
        for k in range(n_layers):
            def clear(i, k=k):
                acc[k, pl.ds(pl.multiple_of(i * BLK, BLK), BLK)] = jnp.zeros((BLK, emb), jnp.float32)

            loop(0, whole // BLK, clear)
            acc[k, whole:] = jnp.zeros((acc.shape[1] - whole, emb), jnp.float32)
        first.wait()

    @pl.when(step < STEPS // 2)
    def _():
        for c in range(n):
            down[0, c * BLK:(c + 1) * BLK] = total[c]
        proj[0] = total[n]

    @pl.when(step >= STEPS // 2)
    def _():
        for c in range(n):
            up[0, :, c * BLK:(c + 1) * BLK] = total[c]
        gate[0] = total[n]

    def one(j):
        def rows8(g):
            at = [line(got[j, INFO + g * 8 + i]) for i in range(8)]
            for i in range(8):
                for k in range(n_layers):
                    acc[k, at[i]] = acc[k, at[i]] + base_v[j, line(g * 8 + i), lanes[k]]

        loop(0, BASE // 8, rows8)

    def two(j):
        start, extra = got[j, 1], got[j, 2]

        def some(first_row, n):
            at = [line(got[j, INFO + BASE + start + first_row + i]) for i in range(n)]
            for i in range(n):
                for k in range(n_layers):
                    acc[k, at[i]] = acc[k, at[i]] + tail_v[k, j, line(start + first_row + i)]

        def four(g):
            some(g * 4, 4)

        def single(i):
            some(i, 1)

        loop(0, extra // 4, four)
        loop(extra // 4 * 4, extra, single)

    part = shards // 8

    @pl.when(step < 8)
    def _():
        loop(step * part, (step + 1) * part, one)

    @pl.when(step == 8)
    def _():
        second.wait()

    @pl.when((step >= 8) & (step < 16))
    def _():
        loop((step - 8) * part, (step - 7) * part, two)

    @pl.when(step == 17)
    def _():
        done.start()

    @pl.when(step == STEPS - 1)
    def _():
        done.wait()


def finish(got, base, tail, total, layers, rows_dev, dim, hid, emb):
    f32 = jnp.float32
    shards, over = got.shape[0], TAIL
    wide = base.shape[1]
    nr, nc = (hid + emb) // BLK, dim // BLK
    half = layers * nc
    hbm = pl.BlockSpec(memory_space=pl.ANY)
    S = jax.ShapeDtypeStruct

    def of(s):
        t = lax.rem(s, half)
        return t // nc, lax.rem(t, nc)

    def tall(s):
        i, j = of(jnp.minimum(s, half - 1))
        return i, 0, j

    def flat(s):
        i, j = of(jnp.maximum(s, half) - half)
        return i, j, 0

    def block(s):
        i, j = of(s)
        return (2 * i + s // half) * nc + j, 0, 0

    return pl.pallas_call(
        finish_kernel,
        grid=(2 * half,),
        in_specs=[pl.BlockSpec(memory_space=pltpu.SMEM), hbm, hbm, pl.BlockSpec((nr, BLK, BLK), block)],
        out_specs=[hbm, pl.BlockSpec((1, hid, BLK), tall), pl.BlockSpec((1, emb, BLK), tall),
                   pl.BlockSpec((1, BLK, hid), flat), pl.BlockSpec((1, BLK, emb), flat)],
        out_shape=[S((layers, rows_dev, emb), f32), S((layers, hid, dim), f32), S((layers, emb, dim), f32),
                   S((layers, dim, hid), f32), S((layers, dim, emb), f32)],
        scratch_shapes=[pltpu.VMEM((shards, BASE, wide), f32), pltpu.VMEM((layers, shards, over, emb), f32),
                        pltpu.VMEM((layers, rows_dev, emb), f32), pltpu.SemaphoreType.DMA((3,))],
        compiler_params=pltpu.CompilerParams(vmem_limit_bytes=66_000_000),
        name="finish",
    )(got, base.reshape(shards, BASE, wide), tail.reshape(layers, shards, over, emb), total)


WORK = (1, 2, 1, 0, 0)


def tails_kernel(*refs):
    n = len(ORDERS)
    refs = list(refs)

    def take(count):
        return [refs.pop(0) for _ in range(count)]

    (x_in, w_up, w_down, w_gate), tails, outs, rests, (wug, wd), keep = take(4), take(n), take(6), take(n), take(2), take(6)
    (wsem, dsem, ssem, rsem), bufs = take(4), refs
    f32, bf = jnp.float32, jnp.bfloat16
    me = lax.axis_index("emb")
    hid, dim = w_up.shape[2], w_up.shape[1]
    uv, hv, av, mv, zv, gv = keep
    spot = {name: bit(me // w) for name, w in WEIGHT.items()}
    other = {name: me + w - 2 * w * spot[name] for name, w in WEIGHT.items()}
    barrier = pltpu.get_barrier_semaphore()
    for name in AXES:
        pl.semaphore_signal(barrier, inc=1, device_id=(other[name],), device_id_type=MESH)
    cp = pltpu.make_async_copy
    ways = ((w_up, wug.at[:, pl.ds(0, hid)]), (w_down, wd), (w_gate, wug.at[:, pl.ds(hid, w_gate.shape[2])]))
    loads = [cp(src.at[0], dst, wsem.at[i]) for i, (src, dst) in enumerate(ways)]
    for c in loads:
        c.start()
    pl.semaphore_wait(barrier, len(AXES))

    def rows(i):
        return pl.ds(pl.multiple_of(i * TILE, TILE), TILE)

    def put(i):
        return [cp(src.at[rows(i)], dst.at[rows(i)], dsem.at[j, i]) for j, (src, dst) in enumerate(zip(keep, outs))]

    def tile(i):
        r = rows(i)
        x = x_in[r].astype(f32)
        u = (x * lax.rsqrt(jnp.mean(x * x, **ROW) + EPS)).astype(bf)
        uv[r] = u
        for c0 in range(0, hid, FCH):
            c = slice(c0, c0 + FCH)
            h = dot32(u, wug[:, c], NN).astype(bf)
            hv[r, c] = h
            av[r, c] = gelu_f(h.astype(f32)).astype(bf)
        z = dot32(u, wug[:, hid:], NN).astype(bf)
        zv[r] = z
        gv[r] = gelu_f(z.astype(f32)).astype(bf)
        for c0 in range(0, dim, FCH):
            c = slice(c0, c0 + FCH)
            mv[r, c] = dot32(av[r], wd[:, c], NN).astype(bf)
        for c in put(i):
            c.start()

    cur, names = list(tails), [list(AXES) for _ in range(n)]
    first = 0
    for s, count in enumerate(WORK):
        copies, kept = [], []
        for k in range(n):
            name = ORDERS[k][s]
            at = names[k].index(name)
            side = lambda v: tuple(v if i == at else slice(None) for i in range(len(names[k])))
            copies.append(pltpu.make_async_remote_copy(
                src_ref=cur[k].at[side(1 - spot[name])], dst_ref=bufs[s].at[k], send_sem=ssem.at[k, s], recv_sem=rsem.at[k, s],
                device_id=(other[name],), device_id_type=MESH))
            kept.append(side(spot[name]))
            names[k].remove(name)
        for c in copies:
            c.start()
        if s == 0:
            for c in loads:
                c.wait()
        if count:
            loop(first, first + count, tile)
        first += count
        for k in range(n):
            copies[k].wait()
            dst = bufs[len(WORK) + s].at[k] if s + 1 < len(WORK) else rests[k]
            dst[...] = cur[k][kept[k]] + bufs[s][k]
            cur[k] = dst
    for i in range(first):
        for c in put(i):
            c.wait()


def run_tails(x_in, w_up, w_down, w_gate, tails):
    n = len(tails)
    rows, emb = tails[0].shape[1:]
    toks, dim = x_in.shape
    hid = w_up.shape[2]
    bf = jnp.bfloat16
    S, V, D = jax.ShapeDtypeStruct, pltpu.VMEM, pltpu.SemaphoreType.DMA
    hbm, vm = pl.BlockSpec(memory_space=pl.ANY), pl.BlockSpec(memory_space=pltpu.VMEM)
    cube = (2,) * len(AXES)
    keep = [(toks, dim), (toks, hid), (toks, hid), (toks, dim), (toks, emb), (toks, emb)]
    steps = [V((n,) + cube[s + 1:] + (rows, emb), bf) for s in range(len(AXES))]
    sems = [D((3,)), D((len(keep), toks // TILE)), D((n, len(AXES))), D((n, len(AXES)))]
    return pl.pallas_call(
        tails_kernel,
        in_specs=[vm] + [hbm] * 3 + [vm] * n,
        out_specs=[hbm] * len(keep) + [vm] * n,
        out_shape=[S(s, bf) for s in keep] + [S((rows, emb), bf)] * n,
        scratch_shapes=[V((dim, hid + emb), bf), V((hid, dim), bf)] + [V(s, bf) for s in keep] + sems + steps + steps[:-1],
        compiler_params=pltpu.CompilerParams(collective_id=1, has_side_effects=True, vmem_limit_bytes=66_000_000),
        cost_estimate=pl.CostEstimate(flops=10**11, bytes_accessed=10**8, transcendentals=0),
        name="tails",
    )(x_in, w_up, w_down, w_gate, *[t.reshape(cube + (rows, emb)) for t in tails])


def fast_step(got, pick, pick_t, x_in, d_out, ple_tables, w_up, w_down, w_gate, w_proj):
    layers, rows_dev, emb = ple_tables.shape
    shards = got.shape[0]
    served = serve(got, ple_tables, TAIL)
    base = swap(served[0].reshape(shards * BASE, layers * emb))
    u, h, a, m, z, g, *rests = run_tails(x_in, w_up, w_down, w_gate, served[1:])
    x_out, us, as_, ss, os_, dhs, dzs, _, send_b, send_t = run_model(
        (x_in, m, h, z, g), base, rests, pick, pick_t, d_out, w_up, w_down, w_gate, w_proj)
    base = swap(send_b)
    total, tail = reduce_grads(u, a, us, as_, ss, os_, dhs, dzs, send_t)
    table, down, proj, up, gate = finish(got, base, tail, total, layers, rows_dev, w_up.shape[1], w_up.shape[2], emb)
    return x_out, table, up, down, gate, proj


def padded_step(shards, tok_ids, x_in, d_out, ple_tables, w_up, w_down, w_gate, w_proj):
    layers = ple_tables.shape[0]
    rows_dev = ple_tables.shape[1]
    cap_rows = tok_ids.shape[0] // CAP_DIV
    owner_dev = tok_ids // rows_dev
    local_row = tok_ids - owner_dev * rows_dev
    owner_hot = (col(owner_dev) == row(numbers(shards))).astype(jnp.int32)
    slot_rank = jnp.sum((jnp.cumsum(owner_hot, axis=0) - owner_hot) * owner_hot, axis=1)
    dest_slot = owner_dev * cap_rows + slot_rank
    req_send = jnp.zeros((shards * cap_rows,), jnp.int32).at[dest_slot].set(local_row)
    req_recv = swap(req_send)
    x_cur = x_in
    saved_list = []
    rows_list = []
    for layer_idx in range(layers):
        served = jnp.take(ple_tables[layer_idx], req_recv, axis=0)
        returned = swap(served)
        emb_rows = jnp.take(returned, dest_slot, axis=0)
        x_cur, saved = layer_fwd(x_cur, w_up[layer_idx], w_down[layer_idx], w_gate[layer_idx], w_proj[layer_idx], emb_rows)
        saved_list.append(saved)
        rows_list.append(emb_rows)
    d_x = d_out.astype(jnp.float32)
    kept = [None] * layers
    tables_by_layer = [None] * layers
    for layer_idx in reversed(range(layers)):
        d_x, kept[layer_idx], (g, ds) = layer_bwd(d_x, saved_list[layer_idx], rows_list[layer_idx], w_up[layer_idx], w_down[layer_idx], w_gate[layer_idx], w_proj[layer_idx], layer_idx == 0)
        d_rows = g.astype(jnp.float32) * ds.astype(jnp.float32)
        grad_send = jnp.zeros((shards * cap_rows, d_rows.shape[1]), jnp.float32).at[dest_slot].set(d_rows)
        grad_recv = swap(grad_send)
        tables_by_layer[layer_idx] = jax.ops.segment_sum(grad_recv, req_recv, num_segments=rows_dev)
    u, a, s, o, dh, dz = ([k[i] for k in kept] for i in range(6))
    total = reduce_grads(u[0], a[0], jnp.stack(u[1:]), jnp.stack(a[1:]), jnp.stack(s), jnp.stack(o), jnp.stack(dh), jnp.stack(dz), jnp.zeros((TAIL, dz[0].shape[1] * layers), jnp.float32))[0]
    dim, hid, emb = w_up.shape[1], w_up.shape[2], w_gate.shape[2]
    nr, nc = (hid + emb) // BLK, dim // BLK
    total = total.reshape(layers, 2, nr * nc, BLK, BLK)
    tall = total[:, 0].reshape(layers, nc, nr, BLK, BLK).transpose(0, 2, 3, 1, 4).reshape(layers, hid + emb, dim)
    wide = total[:, 1].reshape(layers, nc, nr, BLK, BLK).transpose(0, 1, 3, 2, 4).reshape(layers, dim, hid + emb)
    outs = (x_cur, jnp.stack(tables_by_layer), wide[:, :, :hid], tall[:, :hid], wide[:, :, hid:], tall[:, hid:])
    return tuple(with_layout_constraint(o, Layout(major_to_minor=tuple(range(o.ndim)))) for o in outs)


def solution(mesh):
    shards = mesh.shape["emb"]

    def device_step(tok_ids, *rest):
        tables = rest[2]
        pick, pick_t, got = spread(tok_ids, shards, tables.shape[1])
        fits = jnp.max(got[:, 3]) <= TAIL
        return lax.cond(fits, lambda: fast_step(got, pick, pick_t, *rest), lambda: tuple(padded_step(shards, tok_ids, *rest)))

    return jax.shard_map(
        device_step,
        mesh=mesh,
        in_specs=(P("emb"), P("emb", None), P("emb", None), P(None, "emb", None), P(), P(), P(), P()),
        out_specs=(P("emb", None), P(None, "emb", None), P(), P(), P(), P()),
        check_vma=False,
    )
```

```python
import functools

import jax
import jax.numpy as jnp
from jax import lax
from jax.experimental import pallas as pl
from jax.experimental.layout import Layout, with_layout_constraint
from jax.experimental.pallas import tpu as pltpu
from jax.sharding import PartitionSpec as P


EPS = 1e-6
CAP_DIV = 4


def gelu_tanh(pre_act):
    return jax.nn.gelu(pre_act, approximate=True)


def gelu_back(pre_act, grad_out):
    _, pull_back = jax.vjp(gelu_tanh, pre_act.astype(jnp.float32))
    return pull_back(grad_out.astype(jnp.float32))[0]


def dot32(a, b, dims):
    return lax.dot_general(a, b, (dims, ((), ())), preferred_element_type=jnp.float32)


def layer_fwd(x_cur, up_mat, down_mat, gate_mat, proj_mat, emb_rows):
    x_wide = x_cur.astype(jnp.float32)
    inv_rms = lax.rsqrt(jnp.mean(x_wide * x_wide, **ROW) + EPS)
    normed = (x_wide * inv_rms).astype(jnp.bfloat16)
    hidden = jnp.dot(normed, up_mat, preferred_element_type=jnp.float32).astype(jnp.bfloat16)
    act_out = gelu_tanh(hidden.astype(jnp.float32)).astype(jnp.bfloat16)
    mlp_out = jnp.dot(act_out, down_mat, preferred_element_type=jnp.float32).astype(jnp.bfloat16)
    gate_pre = jnp.dot(normed, gate_mat, preferred_element_type=jnp.float32).astype(jnp.bfloat16)
    gate_act = gelu_tanh(gate_pre.astype(jnp.float32)).astype(jnp.bfloat16)
    mix_rows = (gate_act.astype(jnp.float32) * emb_rows.astype(jnp.float32)).astype(jnp.bfloat16)
    ple_out = jnp.dot(mix_rows, proj_mat, preferred_element_type=jnp.float32).astype(jnp.bfloat16)
    x_next = (x_wide + mlp_out.astype(jnp.float32) + ple_out.astype(jnp.float32)).astype(jnp.bfloat16)
    return x_next, (x_cur, inv_rms, normed, hidden, act_out, gate_pre, gate_act, mix_rows)


def layer_bwd(d_x, saved, emb_rows, up_mat, down_mat, gate_mat, proj_mat, last):
    x_cur, inv_rms, normed, hidden, act_out, gate_pre, gate_act, mix_rows = saved
    x_wide = x_cur.astype(jnp.float32)
    g_out = d_x.astype(jnp.bfloat16)
    d_act = dot32(g_out, down_mat, NT).astype(jnp.bfloat16)
    d_hidden = gelu_back(hidden, d_act).astype(jnp.bfloat16)
    d_mix = dot32(g_out, proj_mat, NT).astype(jnp.bfloat16)
    d_gate_act = (emb_rows.astype(jnp.float32) * d_mix.astype(jnp.float32)).astype(jnp.bfloat16)
    d_gate_pre = gelu_back(gate_pre, d_gate_act).astype(jnp.bfloat16)
    d_x_new = None
    if not last:
        d_norm = dot32(d_hidden, up_mat, NT) + dot32(d_gate_pre, gate_mat, NT)
        d_x_new = d_x + inv_rms * d_norm - inv_rms ** 3 * x_wide * jnp.mean(d_norm * x_wide, **ROW)
    return d_x_new, (normed, act_out, mix_rows, g_out, d_hidden, d_gate_pre), (gate_act, d_mix)


BASE = 32
TAIL = 128
AXES = ("far", "near", "y", "x", "core")
WEIGHT = {name: 1 << i for i, name in enumerate(reversed(AXES))}
ORDERS = (("core", "x", "y", "near", "far"), ("core", "y", "near", "x", "far"), ("core", "near", "x", "y", "far"))
DOUBLING = [tuple(reversed(order)) for order in ORDERS]
PARTS = ((0, 48), (48, 40), (88, 40))
MESH = pl.DeviceIdType.MESH
DEPTH = 2
FIRST = range(DEPTH)
LAG = 2
NN, NT, TN = ((1,), (0,)), ((1,), (1,)), ((0,), (0,))
ROW = {"axis": -1, "keepdims": True}
HALF, QUART, EIGHTH = 128, 64, 32
COST = pl.CostEstimate(flops=10**11, bytes_accessed=10**8, transcendentals=0)
VMEM_LIMIT = 66_000_000


def bit(v):
    return lax.rem(v, 2)


def loop(first, last, body):
    def step(i, carry):
        body(i)
        return carry

    lax.fori_loop(first, last, step, 0)


def swap(a):
    return lax.all_to_all(a, "emb", 0, 0, tiled=True)


def line(i):
    return pl.ds(i, 1)


def col(v):
    return v[:, None]


def row(v):
    return v[None, :]


def numbers(n):
    return jnp.arange(n, dtype=jnp.int32)


BLK = 256
NB = 16
NS = 8


def reduce_kernel(sizes, *refs):
    n_layers, per, n = sizes
    u_0, a_0, us, as_, ss, os_, dhs, dzs, send_t, out, tails = refs[:11]
    (v_as, v_o, v_u, v_d, blk1, blk2, blk3, rc1, rc2, rc3, rf1, rf2, rs1, rs2, ri1, ri2, rm1, rm2, fin1, fin2,
     ri3, rm3, rx3, rf3, rs3, fin3, ssem, rsem, lsem, osem, tv, tsem, trsem, tlsem) = refs[11:]
    me = lax.axis_index("emb")
    spot = {name: bit(me // w) for name, w in WEIGHT.items()}
    other = {name: me + w - 2 * w * spot[name] for name, w in WEIGHT.items()}
    core, x, y, zb, near = (spot[name] for name in ("core", "x", "y", "far", "near"))
    p_core, p_x, p_y, p_side = (other[name] for name in ("core", "x", "y", "near"))
    mid = near != zb
    end = near == zb
    p_mid = me + WEIGHT["near"] * (near - zb)

    barrier = pltpu.get_barrier_semaphore()
    for dev in other.values():
        pl.semaphore_signal(barrier, inc=1, device_id=(dev,), device_id_type=MESH)

    @pl.when(mid)
    def _():
        pl.semaphore_signal(barrier, inc=1, device_id=(p_mid,), device_id_type=MESH)
        pl.semaphore_wait(barrier, 6)

    @pl.when(end)
    def _():
        pl.semaphore_wait(barrier, 5)

    def loads(ell):
        layer = n_layers - 1 - ell
        u, a = (us.at[layer - 1], as_.at[layer - 1]) if layer else (u_0, a_0)
        s, o, dh, dz = (t.at[layer] for t in (ss, os_, dhs, dzs))
        slot = ell % 2
        hid = a_0.shape[1]
        left, right = pl.ds(0, hid), pl.ds(hid, BLK)
        ways = ((a, v_as.at[slot, :, left]), (s, v_as.at[slot, :, right]), (o, v_o.at[slot]), (u, v_u.at[slot]),
                (dh, v_d.at[slot, :, left]), (dz, v_d.at[slot, :, right]))
        return [pltpu.make_async_copy(src, dst, osem.at[slot, i]) for i, (src, dst) in enumerate(ways)]

    def tail_copy(part, s, p):
        order = DOUBLING[part]
        at = {name: bit(p // (1 << t)) for t, name in enumerate(order[:s])}
        ref = tails.at[tuple(at.get(name, spot[name]) for name in AXES) + (pl.ds(*PARTS[part]),)]
        i = lax.rem(p, LAG + LAG)
        return pltpu.make_async_remote_copy(src_ref=ref, dst_ref=ref, send_sem=tsem.at[part, s, i], recv_sem=trsem.at[part, s, i],
                                            device_id=(other[order[s]],), device_id_type=MESH)

    t_first = [4]
    for s in range(len(AXES)):
        t_first.append(t_first[-1] + (1 << s) + 2)
    t_own = pltpu.make_async_copy(send_t, tv, tlsem.at[0]), pltpu.make_async_copy(tv, tails.at[tuple(spot[name] for name in AXES)], tlsem.at[0])
    for c in t_own:
        c.start()
        c.wait()
    for ell in (0, 1):
        for c in loads(ell):
            c.start()
    for c in loads(0):
        c.wait()

    span = n // n_layers
    rest = {0: 2, 1: 4}
    early, close = 4, 10

    def active(k, kind):
        return k < n - early if kind == 2 else (lax.rem(k, 5) != rest[kind]) | (k >= n - close)

    def unit(k, kind):
        t = lax.rem(k, span)
        if kind == 2:
            return span * 4 // 5 + jnp.where(k >= n - span, early // 2, 0) + t // 2
        p = lax.rem(t, 5)
        return jnp.where(k >= n - close, t - close + 4, 4 * (t // 5) + p - (p > rest[kind]).astype(jnp.int32))

    def where_out(k, kind):
        base = {0: 0, 1: per, 2: per * bit(k)}[kind]
        return (n_layers - 1 - k // span) * 2 * per + base + unit(k, kind)

    def block(slot, w, wide):
        if wide:
            rb, cb = w // 13, lax.rem(w, 13)
            lhs, rhs = v_u, v_d
        else:
            rb, cb = lax.rem(w, 13), w // 13
            lhs, rhs = v_as, v_o
        lv = lhs[slot, :, pl.ds(pl.multiple_of(rb * BLK, BLK), BLK)]
        rv = rhs[slot, :, pl.ds(pl.multiple_of(cb * BLK, BLK), BLK)]
        return dot32(lv, rv, TN)

    h0 = core * HALF
    flows = []

    def add_flow(off, src, dst, dev, send_if=None, recv_if=None):
        flows.append((len(flows), off, src, dst, dev, send_if, recv_if))
        return flows[-1]

    def rows(start, size):
        return pl.ds(pl.multiple_of(start, EIGHTH), size)

    def desc(f, k):
        idx, _, src, dst, dev, _, _ = f
        d = dev(k) if callable(dev) else dev
        return pltpu.make_async_remote_copy(
            src_ref=src(k), dst_ref=dst(k), send_sem=ssem.at[idx, lax.rem(k, NB)], recv_sem=rsem.at[idx, lax.rem(k, NB)],
            device_id=(d,), device_id_type=MESH)

    def ok(k, cond):
        v = (k >= 0) & (k < n)
        return v if cond is None else v & (cond(k) if callable(cond) else cond)

    acts = []

    def clock():
        now = [-1]

        def at(more=LAG):
            now[0] += more
            return now[0]

        return at

    def xyz(kind, blk, rc, rf, rs, ri, rm, fin, f, s, p_f, p_s):
        at = clock()
        q0, q1 = h0 + f * QUART, h0 + (1 - f) * QUART
        e0, e1 = q0 + s * EIGHTH, q0 + (1 - s) * EIGHTH
        b = lambda k: lax.rem(k, NB)
        m = lambda k: lax.rem(k, NS)
        o = lambda k: where_out(k, kind)
        go = lambda k: active(k, kind)
        on = lambda side: (lambda k: side & active(k, kind))
        f_core = add_flow(at(), lambda k: blk.at[b(k), rows(HALF - h0, HALF)], lambda k: rc.at[m(k)], p_core, go, go)
        f_first = add_flow(at(), lambda k: blk.at[b(k), rows(q1, QUART)], lambda k: rf.at[m(k)], p_f, go, go)
        f_second = add_flow(at(), lambda k: blk.at[b(k), rows(e1, EIGHTH)], lambda k: rs.at[m(k)], p_s, go, go)
        f_in = add_flow(at(), lambda k: blk.at[b(k), rows(e0, EIGHTH)], lambda k: ri.at[m(k)], p_side, on(end), on(mid))
        f_mid = add_flow(at(), lambda k: blk.at[b(k), rows(e0, EIGHTH)], lambda k: rm.at[m(k)], p_mid, on(mid), on(mid))
        f_out = add_flow(at(), lambda k: fin.at[b(k)], lambda k: fin.at[b(k)], p_side, on(mid), on(end))
        g_s = add_flow(at(), lambda k: fin.at[b(k)], lambda k: out.at[o(k), rows(e0, EIGHTH)], p_s, go, go)
        g_f = add_flow(at(), lambda k: out.at[o(k), rows(q0, QUART)], lambda k: out.at[o(k), rows(q0, QUART)], p_f, go, go)
        g_c = add_flow(at(), lambda k: out.at[o(k), rows(h0, HALF)], lambda k: out.at[o(k), rows(h0, HALF)], p_core, go, go)

        def plus(dst0, size, src):
            def add(k):
                r = rows(dst0, size)
                blk[b(k), r] = blk[b(k), r] + src[m(k)]

            return add

        def final(k):
            fin[b(k)] = blk[b(k), rows(e0, EIGHTH)] + rm[m(k)]

        acts.append((f_core, plus(h0, HALF, rc)))
        acts.append((f_first, plus(q0, QUART, rf)))
        acts.append((f_second, plus(e0, EIGHTH, rs)))
        acts.append((f_in, plus(e0, EIGHTH, ri)))
        acts.append((f_mid, final))
        acts.extend((g, None) for g in (f_out, g_s, g_f, g_c))
        locals_.append((g_s[1], lambda k: pltpu.make_async_copy(fin.at[b(k)], out.at[o(k), rows(e0, EIGHTH)], lsem.at[kind, m(k)]), go))

    def zfirst(kind, blk, rc, ri, rm, rx, rf, rs, fin):
        at = clock()
        odd = lambda k: bit(k) == 1
        at_end = lambda k: bit(k // 2) == 1
        go = lambda k: active(k, kind)
        here = lambda k: go(k) & jnp.where(at_end(k), end, mid)
        on = lambda side: (lambda k: side & go(k))
        q0, q1 = h0 + zb * QUART, h0 + (1 - zb) * QUART
        b = lambda k: lax.rem(k, NB)
        m = lambda k: lax.rem(k, NS)
        o = lambda k: where_out(k, kind)
        f = lambda k: jnp.where(odd(k), y, x)
        e0 = lambda k: q0 + f(k) * EIGHTH
        e1 = lambda k: q0 + (1 - f(k)) * EIGHTH
        p_f = lambda k: jnp.where(odd(k), p_y, p_x)
        p_s = lambda k: jnp.where(odd(k), p_x, p_y)
        e_root = lambda side: (lambda k: side & go(k) & at_end(k))
        m_root = lambda side: (lambda k: side & go(k) & jnp.logical_not(at_end(k)))
        f_core = add_flow(at(), lambda k: blk.at[b(k), rows(HALF - h0, HALF)], lambda k: rc.at[m(k)], p_core, go, go)
        f_in = add_flow(at(), lambda k: blk.at[b(k), rows(h0, HALF)], lambda k: ri.at[b(k)], p_side, m_root(end), m_root(mid))
        f_in2 = add_flow(at(0), lambda k: blk.at[b(k), rows(q1, QUART)], lambda k: ri.at[b(k), pl.ds(0, QUART)], p_side, e_root(end), e_root(mid))
        f_mid = add_flow(at(), lambda k: blk.at[b(k), rows(q1, QUART)], lambda k: rm.at[m(k)], p_mid, on(mid), on(mid))
        f_x = add_flow(at(), lambda k: blk.at[b(k), rows(q0, QUART)], lambda k: rx.at[m(k)], p_side, e_root(mid), e_root(end))
        f_first = add_flow(at(), lambda k: blk.at[b(k), rows(e1(k), EIGHTH)], lambda k: rf.at[m(k)], p_f, here, here)
        f_second = add_flow(at(), lambda k: blk.at[b(k), rows(e0(k), EIGHTH)], lambda k: rs.at[m(k)], p_s, here, here)
        g_f = add_flow(at(), lambda k: fin.at[m(k)], lambda k: out.at[o(k), rows(e0(k), EIGHTH)], p_f, here, here)
        g_x = add_flow(at(), lambda k: out.at[o(k), rows(q0, QUART)], lambda k: out.at[o(k), rows(q0, QUART)], p_side, e_root(end), e_root(mid))
        g_m = add_flow(at(), lambda k: out.at[o(k), rows(q0, QUART)], lambda k: out.at[o(k), rows(q0, QUART)], p_mid, on(mid), on(mid))
        g_o = add_flow(at(), lambda k: out.at[o(k), rows(h0, HALF)], lambda k: out.at[o(k), rows(h0, HALF)], p_side, m_root(mid), m_root(end))
        g_o2 = add_flow(at(0), lambda k: out.at[o(k), rows(q1, QUART)], lambda k: out.at[o(k), rows(q1, QUART)], p_side, e_root(mid), e_root(end))
        g_c = add_flow(at(), lambda k: out.at[o(k), rows(h0, HALF)], lambda k: out.at[o(k), rows(h0, HALF)], p_core, go, go)

        def plus(start, size, src):
            def add(k):
                r = rows(start(k), size)
                blk[b(k), r] = blk[b(k), r] + src(k)

            return add

        def final(k):
            fin[m(k)] = blk[b(k), rows(e0(k), EIGHTH)] + rs[m(k)]

        acts.append((f_core, plus(lambda k: h0, HALF, lambda k: rc[m(k)])))
        acts.append((f_in, plus(lambda k: h0, HALF, lambda k: ri[b(k)])))
        acts.append((f_in2, plus(lambda k: q1, QUART, lambda k: ri[b(k), :QUART])))
        acts.append((f_mid, plus(lambda k: q0, QUART, lambda k: rm[m(k)])))
        acts.append((f_x, plus(lambda k: q0, QUART, lambda k: rx[m(k)])))
        acts.append((f_first, plus(e0, EIGHTH, lambda k: rf[m(k)])))
        acts.append((f_second, final))
        acts.extend((g, None) for g in (g_f, g_x, g_m, g_o, g_o2, g_c))
        locals_.append((g_f[1], lambda k: pltpu.make_async_copy(fin.at[m(k)], out.at[o(k), rows(e0(k), EIGHTH)], lsem.at[kind, m(k)]), here))

    locals_ = []
    xyz(0, blk1, rc1, rf1, rs1, ri1, rm1, fin1, x, y, p_x, p_y)
    xyz(1, blk2, rc2, rf2, rs2, ri2, rm2, fin2, y, x, p_y, p_x)
    zfirst(2, blk3, rc3, ri3, rm3, rx3, rf3, rs3, fin3)

    def round_(r):
        for f in flows:
            _, off, _, _, _, give, _ = f
            k = r - off - LAG - LAG

            @pl.when(ok(k, give))
            def _(f=f, k=k):
                desc(f, k).wait_send()
        for off, mk, cond in locals_:
            k = r - off - LAG

            @pl.when(ok(k, cond))
            def _(mk=mk, k=k):
                mk(k).wait()
        for f, fn in acts:
            _, off, _, _, _, _, take = f
            k = r - off - LAG

            @pl.when(ok(k, take))
            def _(f=f, fn=fn, k=k):
                desc(f, k).wait_recv()
                if fn is not None:
                    fn(k)
        for s in range(len(AXES)):
            p = r - t_first[s]

            @pl.when((p >= 2) & (p < (1 << s) + 2))
            def _(s=s, p=p):
                for part in range(len(PARTS)):
                    tail_copy(part, s, p - 2).wait()

            @pl.when((p >= 0) & (p < (1 << s)))
            def _(s=s, p=p):
                for part in range(len(PARTS)):
                    tail_copy(part, s, p).start()
        for ell in range(1, n_layers):
            @pl.when(r == span * ell)
            def _(ell=ell):
                for c in loads(ell):
                    c.wait()
        for f in flows:
            _, off, _, _, _, give, _ = f
            k = r - off

            @pl.when(ok(k, give))
            def _(f=f, k=k):
                desc(f, k).start()
        for off, mk, cond in locals_:
            k = r - off

            @pl.when(ok(k, cond))
            def _(mk=mk, k=k):
                mk(k).start()

        slot = bit(r // span)
        s = lax.rem(r, NB)
        odd = bit(r) == 1

        @pl.when((r < n) & active(r, 0))
        def _():
            blk1[s] = block(slot, unit(r, 0), False)

        @pl.when((r < n) & active(r, 1))
        def _():
            blk2[s] = block(slot, unit(r, 1), True)

        @pl.when((r < n) & active(r, 2) & odd)
        def _():
            blk3[s] = block(slot, unit(r, 2), True)

        @pl.when((r < n) & active(r, 2) & jnp.logical_not(odd))
        def _():
            blk3[s] = block(slot, unit(r, 2), False)

        for ell in range(2, n_layers):
            @pl.when(r == span * (ell - 1) - 1)
            def _(ell=ell):
                for c in loads(ell):
                    c.start()

    loop(0, n + 22, round_)


def reduce_grads(u_0, a_0, us, as_, ss, os_, dhs, dzs, send_t):
    n_layers, toks, wide = ss.shape[0], u_0.shape[0], a_0.shape[1] + ss.shape[2]
    dim = u_0.shape[1]
    over, emb = send_t.shape[0], ss.shape[2]
    per = (wide // BLK) * (dim // BLK)
    n = per * 10 // 13 * n_layers
    f32, bf = jnp.float32, jnp.bfloat16
    V = pltpu.VMEM

    def many(count, slots, rows):
        return [V((slots, rows, BLK), f32)] * count

    big, small = (DEPTH, toks, wide), (DEPTH, toks, dim)
    scratch = [V(big, bf), V(small, bf), V(small, bf), V(big, bf)]
    scratch += many(3, NB, BLK) + many(3, NS, HALF) + many(DEPTH, NS, QUART) + many(6, NS, EIGHTH) + many(DEPTH, NB, EIGHTH)
    scratch += many(1, NB, HALF) + many(DEPTH, NS, QUART) + many(3, NS, EIGHTH)
    D = pltpu.SemaphoreType.DMA
    scratch += [D((31, NB)), D((31, NB)), D((3, NS)), D((DEPTH, 6))]
    scratch += [V((over, emb), f32)] + [D((len(PARTS), len(AXES), LAG + LAG))] * DEPTH + [D((1,))]
    flat = (u_0, a_0, us, as_, ss, os_, dhs, dzs, send_t)
    return pl.pallas_call(
        functools.partial(reduce_kernel, (n_layers, per, n)),
        out_shape=[jax.ShapeDtypeStruct((2 * per * n_layers, BLK, BLK), f32),
                   jax.ShapeDtypeStruct((2,) * len(AXES) + (over, emb), f32)],
        in_specs=[pl.BlockSpec(memory_space=pl.ANY)] * len(flat),
        out_specs=[pl.BlockSpec(memory_space=pl.ANY)] * 2,
        scratch_shapes=scratch,
        compiler_params=pltpu.CompilerParams(collective_id=0, has_side_effects=True, vmem_limit_bytes=VMEM_LIMIT),
        cost_estimate=COST,
        name="reduce_grads",
    )(*flat)


TILE = 256
FCH = 512
GK = 0.7978845608028654
GC = 0.044715


def gelu_f(h):
    return (0.5 * h) * (1.0 + jnp.tanh(h * (GK + (GK * GC) * (h * h))))


def gelu_g(h, g):
    h2 = h * h
    t = jnp.tanh(h * (GK + (GK * GC) * h2))
    return g * (0.5 * (1.0 + t) + (0.5 * h) * (1.0 - t * t) * (GK + (3.0 * GK * GC) * h2))


def model_kernel(*refs):
    (x0, m0, h0, z0, g0, base, t0, t1, t2, pick, pick_t, d_out, w_up, w_down, w_gate, w_proj,
     x_out, us, as_, ss, os_, dhs, dzs, hs, base_in, tails_in, send_b, send_t,
     wug, wd, wp, wp0, xs, cs, hbuf, abuf, ubuf, obuf, pbuf, sbuf, zs, es, gs, invs, dus, dsv, sb, st,
     wsem, usem, hsem, asem, osem, isem, jsem, psem, ssem, zsem, vsem, bsem, tsem, rsem, trsem) = refs
    f32, bf = jnp.float32, jnp.bfloat16
    slots = base.shape[0]
    n_tiles = xs.shape[1] // TILE
    top = es.shape[0] - 1
    ends = range(n_tiles - DEPTH, n_tiles)
    hid = hbuf.shape[2]
    emb = wp0.shape[0]
    dim = wp0.shape[1]

    def rows(i):
        return pl.ds(pl.multiple_of(i * TILE, TILE), TILE)

    def mm(a, b):
        return dot32(a, b, NN)

    def mt(a, b):
        return dot32(a, b, NT)

    cp = pltpu.make_async_copy
    me = lax.axis_index("emb")
    devices = slots // BASE
    peers = range(1, devices)
    barrier = pltpu.get_barrier_semaphore()
    for d in peers:
        pl.semaphore_signal(barrier, inc=1, device_id=(lax.rem(me + d, devices),), device_id_type=MESH)

    def parcel(slot, d):
        dev = lax.rem(me + d, devices)
        return pltpu.make_async_remote_copy(
            src_ref=sb.at[slot, pl.ds(pl.multiple_of(dev * BASE, BASE), BASE)], dst_ref=base_in.at[1 - slot, me],
            send_sem=bsem.at[slot, d], recv_sem=rsem.at[slot, d], device_id=(dev,), device_id_type=MESH)

    spots = {name: bit(me // w) for name, w in WEIGHT.items()}

    def tail_copies(layer, s):
        below = layer - 1
        copies = []
        for part, order in enumerate(DOUBLING):
            ref = tails_in.at[(below,) + tuple(slice(None) if name in order[:s] else spots[name] for name in AXES) + (pl.ds(*PARTS[part]),)]
            w = WEIGHT[order[s]]
            copies.append(pltpu.make_async_remote_copy(
                src_ref=ref, dst_ref=ref, send_sem=tsem.at[below, s, part], recv_sem=trsem.at[below, s, part],
                device_id=(me + w - 2 * w * spots[order[s]],), device_id_type=MESH))
        return copies

    def tail_wait(layer, s):
        for c in tail_copies(layer, s):
            c.wait()

    def tail_start(layer, s):
        if s:
            tail_wait(layer, s - 1)
        for c in tail_copies(layer, s):
            c.start()

    plan = {"bwd2": "222.", "bwd1": "2111", "bwd0": ".1.."}
    begun = dict.fromkeys("12", 1)

    def steps_of(name):
        steps = []
        for at, which in enumerate(plan.get(name, "")):
            if which in begun:
                steps.append((at, int(which), begun[which]))
                begun[which] += 1
        return steps

    def at_tile(i, steps):
        for at, which, s in steps:
            @pl.when(i == at)
            def _(which=which, s=s):
                tail_start(which, s)

    def own(slot):
        return cp(sb.at[slot, pl.ds(pl.multiple_of(me * BASE, BASE), BASE)], base_in.at[1 - slot, me], vsem.at[slot])

    def weights(layer, slot):
        ways = ((w_up, wug.at[slot, :, pl.ds(0, hid)]), (w_down, wd.at[slot]), (w_gate, wug.at[slot, :, pl.ds(hid, emb)]), (w_proj, wp.at[slot]))
        return [cp(src.at[layer], dst, wsem.at[slot, i]) for i, (src, dst) in enumerate(ways)]

    first = cp(w_proj.at[0], wp0, wsem.at[0, 4])
    first.start()
    w1, w2 = weights(1, 0), weights(2, 1)
    for c in w1 + w2:
        c.start()

    def slot_of(i):
        return bit(i)

    def in_x(i):
        return cp(x0.at[rows(i)], ubuf.at[slot_of(i)], isem.at[slot_of(i)])

    def in_p(i):
        return cp(pick.at[rows(i)], pbuf.at[slot_of(i)], psem.at[slot_of(i)])

    def in_m(i):
        return cp(m0.at[rows(i)], obuf.at[slot_of(i)], jsem.at[slot_of(i)])

    def put(src, dst, layer, sem):
        return lambda i: cp(src.at[slot_of(i)], dst.at[layer, rows(i)] if layer is not None else dst.at[rows(i)], sem.at[slot_of(i)])

    tails = (t0, t1, t2)

    def rows_of(layer, i):
        in_p(i).wait()
        p = pbuf[slot_of(i)]
        return (mm(p[:, :slots], base[:, layer * emb:(layer + 1) * emb]) + mm(p[:, slots:], tails[layer][...])).astype(bf)

    for i in FIRST:
        in_x(i).start()
        in_m(i).start()
        in_p(i).start()
    first.wait()
    put_s = lambda layer: (lambda i: cp(sbuf.at[slot_of(i)], ss.at[layer, rows(i)], ssem.at[slot_of(i)]))

    def finish0(i):
        r, k = rows(i), slot_of(i)

        @pl.when(i >= DEPTH)
        def _():
            put_s(0)(i - DEPTH).wait()

        e = rows_of(0, i)
        es[0, r] = e
        s = (g0[r].astype(f32) * e.astype(f32)).astype(bf)
        sbuf[k] = s
        put_s(0)(i).start()
        q = mm(s, wp0[...]).astype(bf)
        in_x(i).wait()
        in_m(i).wait()
        xs[0, r] = (ubuf[k].astype(f32) + obuf[k].astype(f32) + q.astype(f32)).astype(bf)

        @pl.when(i + DEPTH < n_tiles)
        def _():
            in_x(i + DEPTH).start()
            in_m(i + DEPTH).start()
            in_p(i + DEPTH).start()

    loop(0, n_tiles, finish0)
    for i in ends:
        put_s(0)(i).wait()

    def in_d(i):
        return cp(d_out.at[rows(i)], ubuf.at[slot_of(i)], isem.at[slot_of(i)])

    def put_t(layer):
        below = layer - 1
        dst = tails_in.at[(below,) + tuple(spots[name] for name in AXES)] if layer else send_t
        return cp(st, dst, jsem.at[0])

    def rows_back(layer, slot):
        below = layer - 1
        proj = wp0 if layer == 0 else wp.at[slot]
        if layer == top:
            for i in FIRST:
                in_d(i).start()

        def tile(i):
            r = rows(i)
            if layer == top:
                in_d(i).wait()
                cs[r] = ubuf[slot_of(i)].astype(f32)

                @pl.when(i + DEPTH < n_tiles)
                def _():
                    in_d(i + DEPTH).start()
            dsv[r] = mt(cs[r].astype(bf), proj[...]).astype(bf)

        loop(0, n_tiles, tile)
        g = g0 if layer == 0 else gs.at[below]
        d = g[...].astype(f32) * dsv[...].astype(f32)
        high = d.astype(bf)
        low = (d - high.astype(f32)).astype(bf)
        spot = layer % 2
        if layer == 0:
            for d in peers:
                parcel(spot, d).wait_send()
            own(spot).wait()
        for c0 in range(0, slots, BLK):
            p = pick_t[c0:c0 + BLK]
            sb[spot, c0:c0 + BLK] = mm(p, high) + mm(p, low)
        p = pick_t[slots:]
        st[...] = mm(p, high) + mm(p, low)
        put_t(layer).start()
        if layer == 0:
            cp(sb.at[spot], send_b, vsem.at[spot]).start()
        else:
            own(spot).start()
            if layer == top:
                pl.semaphore_wait(barrier, devices - 1)
            put_t(layer).wait()
            tail_start(layer, 0)
            if layer == top:
                for d in peers:
                    parcel(spot, d).start()

    def fwd(layer, slot, loaded):
        below = layer - 1
        outs = [put(ubuf, us, below, usem), put(hbuf, hs, below, hsem), put_s(layer),
                lambda i: cp(abuf.at[slot_of(i), :, pl.ds(0, hid)], as_.at[below, rows(i)], asem.at[slot_of(i)])]
        if layer == top:
            outs.append(put(obuf, x_out, None, osem))
        for c in loaded:
            c.wait()
        for i in FIRST:
            in_p(i).start()

        def gates(i):
            r = rows(i)
            x = xs[below, r].astype(f32)
            inv = lax.rsqrt(jnp.mean(x * x, **ROW) + EPS)
            invs[below, r] = jnp.broadcast_to(inv, (TILE, invs.shape[2]))
            z = mm((x * inv).astype(bf), wug[slot, :, hid:]).astype(bf)
            zs[below, r] = z
            gs[below, r] = gelu_f(z.astype(f32)).astype(bf)

        loop(0, n_tiles, gates)
        if layer == top:
            rows_back(layer, slot)
        steps = steps_of(f"fwd{layer}")

        def tile(i):
            r, k = rows(i), slot_of(i)

            @pl.when(i >= DEPTH)
            def _():
                for o in outs:
                    o(i - DEPTH).wait()

            at_tile(i, steps)
            x = xs[below, r].astype(f32)
            u = (x * invs[below, r][:, :1]).astype(bf)
            ubuf[k] = u
            for c0 in range(0, hid, FCH):
                h = mm(u, wug[slot, :, c0:c0 + FCH]).astype(bf)
                hbuf[k, :, c0:c0 + FCH] = h
                abuf[k, :, c0:c0 + FCH] = gelu_f(h.astype(f32)).astype(bf)
            g = gs[below, r]
            e = rows_of(layer, i)
            es[layer, r] = e
            s = (g.astype(f32) * e.astype(f32)).astype(bf)
            sbuf[k] = s
            for c0 in range(0, dim, FCH):
                c1 = c0 + FCH
                q = mm(s, wp[slot, :, c0:c1]).astype(bf)
                m = mm(abuf[k, :, :hid], wd[slot, :, c0:c1]).astype(bf)
                new = (xs[below, r, c0:c1].astype(f32) + m.astype(f32) + q.astype(f32)).astype(bf)
                if layer == top:
                    obuf[k, :, c0:c1] = new
                else:
                    xs[layer, r, c0:c1] = new
            for o in outs:
                o(i).start()

            @pl.when(i + DEPTH < n_tiles)
            def _():
                in_p(i + DEPTH).start()

        loop(0, n_tiles, tile)
        for i in ends:
            for o in outs:
                o(i).wait()

    def in_h(layer, i):
        below = layer - 1
        return cp(h0.at[rows(i)] if layer == 0 else hs.at[below, rows(i)], hbuf.at[slot_of(i)], hsem.at[slot_of(i)])

    def bwd(layer, slot):
        below = layer - 1
        outs = [lambda i: cp(abuf.at[slot_of(i), :, pl.ds(0, hid)], dhs.at[layer, rows(i)], asem.at[slot_of(i)]),
                lambda i: cp(abuf.at[slot_of(i), :, pl.ds(hid, emb)], dzs.at[layer, rows(i)], zsem.at[slot_of(i)]),
                put(obuf, os_, layer, osem)]
        steps = steps_of(f"bwd{layer}")
        if layer == top:
            for i in FIRST:
                in_h(layer, i).start()
        else:
            rows_back(layer, slot)

        def tile(i):
            r, k = rows(i), slot_of(i)

            @pl.when(i >= DEPTH)
            def _():
                for o in outs:
                    o(i - DEPTH).wait()

            at_tile(i, steps)
            if layer == 1:
                @pl.when(i == n_tiles - 1)
                def _():
                    for d in peers:
                        parcel(layer, d).start()
            o = cs[r].astype(bf)
            obuf[k] = o
            ds = dsv[r]
            z = (z0[r] if layer == 0 else zs[below, r]).astype(f32)
            dg = (es[layer, r].astype(f32) * ds.astype(f32)).astype(bf)
            abuf[k, :, hid:] = gelu_g(z, dg.astype(f32)).astype(bf)
            in_h(layer, i).wait()
            for c0 in range(0, hid, FCH):
                da = mt(o, wd[slot, c0:c0 + FCH]).astype(bf)
                abuf[k, :, c0:c0 + FCH] = gelu_g(hbuf[k, :, c0:c0 + FCH].astype(f32), da.astype(f32)).astype(bf)
            if layer > 0:
                dot = jnp.zeros((TILE, 1), f32)
                for c0 in range(0, dim, FCH):
                    du = mt(abuf[k], wug[slot, c0:c0 + FCH])
                    dus[:, c0:c0 + FCH] = du
                    dot = dot + jnp.sum(du * xs[below, r, c0:c0 + FCH].astype(f32), **ROW)
                inv = invs[below, r][:, :1]
                back = (inv * inv * inv) * (dot * (1.0 / dim))
                for c0 in range(0, dim, FCH):
                    c1 = c0 + FCH
                    cs[r, c0:c1] = cs[r, c0:c1] + inv * dus[:, c0:c1] - back * xs[below, r, c0:c1].astype(f32)
            for ot in outs:
                ot(i).start()

            @pl.when(i + DEPTH < n_tiles)
            def _():
                in_h(layer, i + DEPTH).start()

        loop(0, n_tiles, tile)
        if layer > 0:
            for i in FIRST:
                in_h(below, i).start()
        for i in ends:
            for o in outs:
                o(i).wait()

    fwd(1, 0, w1)
    fwd(2, 1, w2)
    bwd(2, 1)
    last = cp(w_down.at[0], wd.at[1], wsem.at[1, 1])
    last.start()
    bwd(1, 0)
    last.wait()
    bwd(0, 1)
    put_t(0).wait()
    for layer in (1, 2):
        tail_wait(layer, len(AXES) - 1)
    cp(sb.at[0], send_b, vsem.at[0]).wait()
    own(1).wait()
    for d in peers:
        parcel(0, d).wait_recv()
        parcel(1, d).wait()


def run_model(pre, base, tails, pick, pick_t, d_out, w_up, w_down, w_gate, w_proj):
    x0, m0, h0, z0, g0 = pre
    layers, dim, hid = w_up.shape
    emb = w_gate.shape[2]
    toks = x0.shape[0]
    slots, over = base.shape[0], tails[0].shape[0]
    below = layers - 1
    f32, bf = jnp.float32, jnp.bfloat16
    hbm, vm = pl.BlockSpec(memory_space=pl.ANY), pl.BlockSpec(memory_space=pltpu.VMEM)
    S = jax.ShapeDtypeStruct
    V = pltpu.VMEM
    D = pltpu.SemaphoreType.DMA
    return pl.pallas_call(
        model_kernel,
        in_specs=[hbm] * 3 + [vm] * 6 + [hbm] + [vm] + [hbm] * 5,
        out_specs=[hbm] * 12,
        out_shape=[S((toks, dim), bf), S((below, toks, dim), bf), S((below, toks, hid), bf), S((layers, toks, emb), bf),
                   S((layers, toks, dim), bf), S((layers, toks, hid), bf), S((layers, toks, emb), bf), S((below, toks, hid), bf),
                   S((below, slots // BASE, BASE, emb), f32),
                   S((below,) + (2,) * len(AXES) + (over, emb), f32), S((slots, emb), f32), S((over, emb), f32)],
        scratch_shapes=[
            V((DEPTH, dim, hid + emb), bf), V((DEPTH, hid, dim), bf), V((DEPTH, emb, dim), bf), V((emb, dim), bf),
            V((DEPTH, toks, dim), bf), V((toks, dim), f32), V((DEPTH, TILE, hid), bf), V((DEPTH, TILE, hid + emb), bf),
            V((DEPTH, TILE, dim), bf), V((DEPTH, TILE, dim), bf), V((DEPTH, TILE, slots + over), bf), V((DEPTH, TILE, emb), bf),
            V((DEPTH, toks, emb), bf), V((layers, toks, emb), bf), V((DEPTH, toks, emb), bf), V((DEPTH, toks, 128), f32), V((TILE, dim), f32),
            V((toks, emb), bf), V((DEPTH, slots, emb), f32), V((over, emb), f32),
            D((DEPTH, 5))] + [D((DEPTH,))] * 10 + [D((DEPTH, slots // BASE)), D((DEPTH, len(AXES), len(PARTS)))] * DEPTH,
        compiler_params=pltpu.CompilerParams(collective_id=2, has_side_effects=True, vmem_limit_bytes=VMEM_LIMIT),
        name="model",
    )(x0, m0, h0, z0, g0, base, *tails, pick, pick_t, d_out, w_up, w_down, w_gate, w_proj)


def spread(tok_ids, shards, rows_dev):
    toks = tok_ids.shape[0]
    i32, f32, bf = jnp.int32, jnp.float32, jnp.bfloat16
    owner = tok_ids // rows_dev
    local = tok_ids - owner * rows_dev
    row_no = lax.broadcasted_iota(i32, (toks, toks), 0)
    col_no = lax.broadcasted_iota(i32, (toks, toks), 1)
    same = col(tok_ids) == row(tok_ids)

    def first_one(earlier, axis):
        return 1.0 - jnp.max((same & earlier).astype(f32), axis=axis)

    new = first_one(col_no < row_no, 1)
    hot32 = (col(owner) == row(numbers(shards))).astype(f32)
    fresh = hot32 * col(new)
    before = (row_no > col_no).astype(bf)
    ahead = jnp.dot(before, fresh.astype(bf), preferred_element_type=f32)
    rank = jnp.sum(ahead * hot32, axis=1)
    count = jnp.sum(fresh, axis=0)
    extra = jnp.maximum(count - BASE, 0.0)
    lower = lax.broadcasted_iota(i32, (shards, shards), 0) > lax.broadcasted_iota(i32, (shards, shards), 1)
    start = jnp.sum(jnp.where(lower, row(extra), 0.0), axis=1)
    tail = jnp.sum(hot32 * row(start), axis=1)
    place = jnp.where(rank < BASE, owner.astype(f32) * BASE + rank, shards * BASE + tail + rank - BASE)
    spots = place * first_one(row_no < col_no, 0)
    slot = jnp.sum(same.astype(f32) * row(spots), axis=1).astype(i32)
    n_slots = shards * BASE + TAIL
    pick = (col(slot) == lax.broadcasted_iota(i32, (toks, n_slots), 1)).astype(bf)
    pick_t = (row(slot) == lax.broadcasted_iota(i32, (n_slots, toks), 0)).astype(bf)
    parts = (jnp.stack([local // 64, local % 64], axis=1).astype(f32) * col(new)).astype(bf)
    want = jnp.dot(pick_t, parts, preferred_element_type=f32)
    want = (want[:, 0] * 64.0 + want[:, 1]).astype(i32)
    base = want[:shards * BASE].reshape(shards, BASE)
    rest = jnp.broadcast_to(want[shards * BASE:][None, :], (shards, TAIL))
    total = jnp.sum(extra)
    fit = (total <= TAIL).astype(f32)
    info = jnp.stack([count, start * fit, extra * fit, jnp.broadcast_to(total, (shards,))], axis=1).astype(i32)
    pad = jnp.zeros((shards, INFO - 4), i32)
    sent = jnp.concatenate([info, pad, base, rest], axis=1)
    got = swap(sent)
    return pick, pick_t, got


INFO = 128


def serve_kernel(n_layers, over, got, tables, *refs):
    base_out, outs, (tab, wide, stage, sem) = refs[0], refs[1:1 + n_layers], refs[1 + n_layers:]
    shards = got.shape[0]
    emb = wide.shape[2]
    loads = [pltpu.make_async_copy(tables.at[k], tab.at[k], sem.at[k]) for k in range(n_layers)]
    for c in loads:
        c.start()
    for k in range(n_layers):
        loads[k].wait()
        whole = wide.shape[1] // BLK * BLK

        def widen(i, k=k):
            r = pl.ds(pl.multiple_of(i * BLK, BLK), BLK)
            wide[k, r] = tab[k, r].astype(jnp.float32)

        loop(0, whole // BLK, widen)
        wide[k, whole:] = tab[k, whole:].astype(jnp.float32)

    stage[...] = jnp.zeros_like(stage)

    def one(j):
        start, extra = got[j, 1], got[j, 2]

        def rows8(g):
            at = [got[j, INFO + g * 8 + i] for i in range(8)]
            for i in range(8):
                for k in range(n_layers):
                    stage[k, line(g * 8 + i)] = wide[k, line(at[i])]

        used = jnp.minimum(got[j, 0], BASE)
        loop(0, (used + 7) // 8, rows8)
        for k in range(n_layers):
            base_out[j, :, k * emb:(k + 1) * emb] = stage[k, :BASE].astype(jnp.bfloat16)

        @pl.when(extra == 0)
        def _():
            for k in range(n_layers):
                outs[k][j] = jnp.zeros((over, emb), jnp.bfloat16)

        @pl.when(extra > 0)
        def _():
            stage[...] = jnp.zeros_like(stage)

            def four(g):
                at = [got[j, INFO + BASE + start + g * 4 + i] for i in range(4)]
                for i in range(4):
                    for k in range(n_layers):
                        stage[k, line(start + g * 4 + i)] = wide[k, line(at[i])]

            def single(i):
                at = got[j, INFO + BASE + start + i]
                for k in range(n_layers):
                    stage[k, line(start + i)] = wide[k, line(at)]

            loop(0, extra // 4, four)
            loop(extra // 4 * 4, extra, single)
            for k in range(n_layers):
                outs[k][j] = stage[k].astype(jnp.bfloat16)

    loop(0, shards, one)


def serve(got, tables, over):
    n_layers, rows_dev, emb = tables.shape
    shards = got.shape[0]
    bf = jnp.bfloat16
    shapes = [jax.ShapeDtypeStruct((shards, BASE, n_layers * emb), bf)] + [jax.ShapeDtypeStruct((shards, over, emb), bf)] * n_layers
    return pl.pallas_call(
        functools.partial(serve_kernel, n_layers, over),
        in_specs=[pl.BlockSpec(memory_space=pltpu.SMEM), pl.BlockSpec(memory_space=pl.ANY)],
        out_specs=[pl.BlockSpec(memory_space=pltpu.VMEM)] * (1 + n_layers),
        out_shape=shapes,
        scratch_shapes=[pltpu.VMEM((n_layers, rows_dev, emb), bf), pltpu.VMEM((n_layers, rows_dev, emb), jnp.float32),
                        pltpu.VMEM((n_layers, over, emb), jnp.float32), pltpu.SemaphoreType.DMA((n_layers,))],
        compiler_params=pltpu.CompilerParams(vmem_limit_bytes=VMEM_LIMIT),
        name="serve_rows",
    )(got, tables)


STEPS = 24


def finish_kernel(got, base, base_in, tail, tails_in, total, table, down, proj, up, gate, base_v, tail_v, acc, sem):
    step = pl.program_id(0)
    shards = got.shape[0]
    n_layers, _, emb = acc.shape
    first = [pltpu.make_async_copy(base, base_v.at[0], sem.at[0]),
             pltpu.make_async_copy(base_in, base_v.at[pl.ds(1, n_layers - 1)], sem.at[3])]
    second = [pltpu.make_async_copy(tail, tail_v.at[0], sem.at[1]),
              pltpu.make_async_copy(tails_in, tail_v.at[pl.ds(1, n_layers - 1)], sem.at[4])]
    done = pltpu.make_async_copy(acc, table, sem.at[2])
    n = total.shape[0] - 1

    @pl.when(step == 0)
    def _():
        for c in first + second:
            c.start()
        whole = acc.shape[1] // BLK * BLK
        for k in range(n_layers):
            def clear(i, k=k):
                acc[k, pl.ds(pl.multiple_of(i * BLK, BLK), BLK)] = jnp.zeros((BLK, emb), jnp.float32)

            loop(0, whole // BLK, clear)
            acc[k, whole:] = jnp.zeros((acc.shape[1] - whole, emb), jnp.float32)
        for c in first:
            c.wait()

    @pl.when(step < STEPS // 2)
    def _():
        for c in range(n):
            down[0, c * BLK:(c + 1) * BLK] = total[c]
        proj[0] = total[n]

    @pl.when(step >= STEPS // 2)
    def _():
        for c in range(n):
            up[0, :, c * BLK:(c + 1) * BLK] = total[c]
        gate[0] = total[n]

    def one(j):
        def rows8(g):
            at = [line(got[j, INFO + g * 8 + i]) for i in range(8)]
            for i in range(8):
                for k in range(n_layers):
                    acc[k, at[i]] = acc[k, at[i]] + base_v[k, j, line(g * 8 + i)]

        loop(0, (jnp.minimum(got[j, 0], BASE) + 7) // 8, rows8)

    def two(j):
        start, extra = got[j, 1], got[j, 2]

        def some(first_row, n):
            at = [line(got[j, INFO + BASE + start + first_row + i]) for i in range(n)]
            for i in range(n):
                for k in range(n_layers):
                    acc[k, at[i]] = acc[k, at[i]] + tail_v[k, j, line(start + first_row + i)]

        def four(g):
            some(g * 4, 4)

        def single(i):
            some(i, 1)

        loop(0, extra // 4, four)
        loop(extra // 4 * 4, extra, single)

    turn = STEPS // 2
    part = 4

    @pl.when(step < turn)
    def _():
        loop(step * part, jnp.minimum((step + 1) * part, shards), one)

    @pl.when(step == turn)
    def _():
        for c in second:
            c.wait()

    @pl.when(step >= turn)
    def _():
        loop(jnp.minimum((step - turn) * part, shards), jnp.minimum((step - turn + 1) * part, shards), two)

    @pl.when(step == STEPS - 5)
    def _():
        done.start()

    @pl.when(step == STEPS - 1)
    def _():
        done.wait()


def finish(got, base, base_in, tail, tails_in, total, layers, rows_dev, dim, hid, emb):
    f32 = jnp.float32
    shards, over = got.shape[0], TAIL
    nr, nc = (hid + emb) // BLK, dim // BLK
    half = layers * nc
    hbm = pl.BlockSpec(memory_space=pl.ANY)
    S = jax.ShapeDtypeStruct

    def of(s):
        t = lax.rem(s, half)
        return t // nc, lax.rem(t, nc)

    def tall(s):
        i, j = of(jnp.minimum(s, half - 1))
        return i, 0, j

    def flat(s):
        i, j = of(jnp.maximum(s, half) - half)
        return i, j, 0

    def block(s):
        i, j = of(s)
        return (2 * i + s // half) * nc + j, 0, 0

    return pl.pallas_call(
        finish_kernel,
        grid=(2 * half,),
        in_specs=[pl.BlockSpec(memory_space=pltpu.SMEM), hbm, hbm, hbm, hbm, pl.BlockSpec((nr, BLK, BLK), block)],
        out_specs=[hbm, pl.BlockSpec((1, hid, BLK), tall), pl.BlockSpec((1, emb, BLK), tall),
                   pl.BlockSpec((1, BLK, hid), flat), pl.BlockSpec((1, BLK, emb), flat)],
        out_shape=[S((layers, rows_dev, emb), f32), S((layers, hid, dim), f32), S((layers, emb, dim), f32),
                   S((layers, dim, hid), f32), S((layers, dim, emb), f32)],
        scratch_shapes=[pltpu.VMEM((layers, shards, BASE, emb), f32), pltpu.VMEM((layers, shards, over, emb), f32),
                        pltpu.VMEM((layers, rows_dev, emb), f32), pltpu.SemaphoreType.DMA((5,))],
        compiler_params=pltpu.CompilerParams(vmem_limit_bytes=VMEM_LIMIT),
        name="finish",
    )(got, base.reshape(shards, BASE, emb), base_in, tail.reshape(shards, over, emb),
      tails_in.reshape(layers - 1, shards, over, emb), total)


WORK = (1, 2, 1, 0, 0)


def tails_kernel(*refs):
    n = len(ORDERS)
    refs = list(refs)

    def take(count):
        return [refs.pop(0) for _ in range(count)]

    (x_in, w_up, w_down, w_gate), tails, outs, rests, (wug, wd), keep = take(4), take(n), take(6), take(n), take(2), take(6)
    (wsem, dsem, ssem, rsem), bufs = take(4), refs
    f32, bf = jnp.float32, jnp.bfloat16
    me = lax.axis_index("emb")
    hid, dim = w_up.shape[2], w_up.shape[1]
    uv, hv, av, mv, zv, gv = keep
    spot = {name: bit(me // w) for name, w in WEIGHT.items()}
    other = {name: me + w - 2 * w * spot[name] for name, w in WEIGHT.items()}
    barrier = pltpu.get_barrier_semaphore()
    for name in AXES:
        pl.semaphore_signal(barrier, inc=1, device_id=(other[name],), device_id_type=MESH)
    cp = pltpu.make_async_copy
    ways = ((w_up, wug.at[:, pl.ds(0, hid)]), (w_down, wd), (w_gate, wug.at[:, pl.ds(hid, w_gate.shape[2])]))
    loads = [cp(src.at[0], dst, wsem.at[i]) for i, (src, dst) in enumerate(ways)]
    for c in loads:
        c.start()
    pl.semaphore_wait(barrier, len(AXES))

    def rows(i):
        return pl.ds(pl.multiple_of(i * TILE, TILE), TILE)

    def put(i):
        return [cp(src.at[rows(i)], dst.at[rows(i)], dsem.at[j, i]) for j, (src, dst) in enumerate(zip(keep, outs))]

    def tile(i):
        r = rows(i)
        x = x_in[r].astype(f32)
        u = (x * lax.rsqrt(jnp.mean(x * x, **ROW) + EPS)).astype(bf)
        uv[r] = u
        for c0 in range(0, hid, FCH):
            c = slice(c0, c0 + FCH)
            h = dot32(u, wug[:, c], NN).astype(bf)
            hv[r, c] = h
            av[r, c] = gelu_f(h.astype(f32)).astype(bf)
        z = dot32(u, wug[:, hid:], NN).astype(bf)
        zv[r] = z
        gv[r] = gelu_f(z.astype(f32)).astype(bf)
        for c0 in range(0, dim, FCH):
            c = slice(c0, c0 + FCH)
            mv[r, c] = dot32(av[r], wd[:, c], NN).astype(bf)
        for c in put(i):
            c.start()

    cur, names = list(tails), [list(AXES) for _ in range(n)]
    first = 0
    for s, count in enumerate(WORK):
        copies, kept = [], []
        for k in range(n):
            name = ORDERS[k][s]
            at = names[k].index(name)
            side = lambda v: tuple(v if i == at else slice(None) for i in range(len(names[k])))
            copies.append(pltpu.make_async_remote_copy(
                src_ref=cur[k].at[side(1 - spot[name])], dst_ref=bufs[s].at[k], send_sem=ssem.at[k, s], recv_sem=rsem.at[k, s],
                device_id=(other[name],), device_id_type=MESH))
            kept.append(side(spot[name]))
            names[k].remove(name)
        for c in copies:
            c.start()
        if s == 0:
            for c in loads:
                c.wait()
        if count:
            loop(first, first + count, tile)
        first += count
        for k in range(n):
            copies[k].wait()
            dst = bufs[len(WORK) + s].at[k] if s + 1 < len(WORK) else rests[k]
            dst[...] = cur[k][kept[k]] + bufs[s][k]
            cur[k] = dst
    for i in range(first):
        for c in put(i):
            c.wait()


def run_tails(x_in, w_up, w_down, w_gate, tails):
    n = len(tails)
    rows, emb = tails[0].shape[1:]
    toks, dim = x_in.shape
    hid = w_up.shape[2]
    bf = jnp.bfloat16
    S, V, D = jax.ShapeDtypeStruct, pltpu.VMEM, pltpu.SemaphoreType.DMA
    hbm, vm = pl.BlockSpec(memory_space=pl.ANY), pl.BlockSpec(memory_space=pltpu.VMEM)
    cube = (2,) * len(AXES)
    keep = [(toks, dim), (toks, hid), (toks, hid), (toks, dim), (toks, emb), (toks, emb)]
    steps = [V((n,) + cube[s + 1:] + (rows, emb), bf) for s in range(len(AXES))]
    sems = [D((3,)), D((len(keep), toks // TILE)), D((n, len(AXES))), D((n, len(AXES)))]
    return pl.pallas_call(
        tails_kernel,
        in_specs=[vm] + [hbm] * 3 + [vm] * n,
        out_specs=[hbm] * len(keep) + [vm] * n,
        out_shape=[S(s, bf) for s in keep] + [S((rows, emb), bf)] * n,
        scratch_shapes=[V((dim, hid + emb), bf), V((hid, dim), bf)] + [V(s, bf) for s in keep] + sems + steps + steps[:-1],
        compiler_params=pltpu.CompilerParams(collective_id=1, has_side_effects=True, vmem_limit_bytes=VMEM_LIMIT),
        cost_estimate=COST,
        name="tails",
    )(x_in, w_up, w_down, w_gate, *[t.reshape(cube + (rows, emb)) for t in tails])


def fast_step(got, pick, pick_t, x_in, d_out, ple_tables, w_up, w_down, w_gate, w_proj):
    layers, rows_dev, emb = ple_tables.shape
    shards = got.shape[0]
    served = serve(got, ple_tables, TAIL)
    base = swap(served[0].reshape(shards * BASE, layers * emb))
    u, h, a, m, z, g, *rests = run_tails(x_in, w_up, w_down, w_gate, served[1:])
    x_out, us, as_, ss, os_, dhs, dzs, _, base_in, tails_in, send_b, send_t = run_model(
        (x_in, m, h, z, g), base, rests, pick, pick_t, d_out, w_up, w_down, w_gate, w_proj)
    base = swap(send_b)
    total, tail = reduce_grads(u, a, us, as_, ss, os_, dhs, dzs, send_t)
    table, down, proj, up, gate = finish(got, base, base_in, tail, tails_in, total, layers, rows_dev, w_up.shape[1], w_up.shape[2], emb)
    return x_out, table, up, down, gate, proj


def padded_step(shards, tok_ids, x_in, d_out, ple_tables, w_up, w_down, w_gate, w_proj):
    layers = ple_tables.shape[0]
    rows_dev = ple_tables.shape[1]
    cap_rows = tok_ids.shape[0] // CAP_DIV
    owner_dev = tok_ids // rows_dev
    local_row = tok_ids - owner_dev * rows_dev
    owner_hot = (col(owner_dev) == row(numbers(shards))).astype(jnp.int32)
    slot_rank = jnp.sum((jnp.cumsum(owner_hot, axis=0) - owner_hot) * owner_hot, axis=1)
    dest_slot = owner_dev * cap_rows + slot_rank
    req_send = jnp.zeros((shards * cap_rows,), jnp.int32).at[dest_slot].set(local_row)
    req_recv = swap(req_send)
    x_cur = x_in
    saved_list = []
    rows_list = []
    for layer_idx in range(layers):
        served = jnp.take(ple_tables[layer_idx], req_recv, axis=0)
        returned = swap(served)
        emb_rows = jnp.take(returned, dest_slot, axis=0)
        x_cur, saved = layer_fwd(x_cur, w_up[layer_idx], w_down[layer_idx], w_gate[layer_idx], w_proj[layer_idx], emb_rows)
        saved_list.append(saved)
        rows_list.append(emb_rows)
    d_x = d_out.astype(jnp.float32)
    kept = [None] * layers
    tables_by_layer = [None] * layers
    for layer_idx in reversed(range(layers)):
        d_x, kept[layer_idx], (g, ds) = layer_bwd(d_x, saved_list[layer_idx], rows_list[layer_idx], w_up[layer_idx], w_down[layer_idx], w_gate[layer_idx], w_proj[layer_idx], layer_idx == 0)
        d_rows = g.astype(jnp.float32) * ds.astype(jnp.float32)
        grad_send = jnp.zeros((shards * cap_rows, d_rows.shape[1]), jnp.float32).at[dest_slot].set(d_rows)
        grad_recv = swap(grad_send)
        tables_by_layer[layer_idx] = jax.ops.segment_sum(grad_recv, req_recv, num_segments=rows_dev)
    u, a, s, o, dh, dz = zip(*kept)
    total = reduce_grads(u[0], a[0], jnp.stack(u[1:]), jnp.stack(a[1:]), jnp.stack(s), jnp.stack(o), jnp.stack(dh), jnp.stack(dz), jnp.zeros((TAIL, dz[0].shape[1]), jnp.float32))[0]
    (_, dim, hid), (_, _, emb) = w_up.shape, w_gate.shape
    nr, nc = (hid + emb) // BLK, dim // BLK
    total = total.reshape(layers, 2, nr * nc, BLK, BLK)
    tall = total[:, 0].reshape(layers, nc, nr, BLK, BLK).transpose(0, 2, 3, 1, 4).reshape(layers, hid + emb, dim)
    wide = total[:, 1].reshape(layers, nc, nr, BLK, BLK).transpose(0, 1, 3, 2, 4).reshape(layers, dim, hid + emb)
    outs = (x_cur, jnp.stack(tables_by_layer), wide[:, :, :hid], tall[:, :hid], wide[:, :, hid:], tall[:, hid:])
    return tuple(with_layout_constraint(o, Layout(major_to_minor=tuple(range(o.ndim)))) for o in outs)


def solution(mesh):
    shards = mesh.shape["emb"]

    def device_step(tok_ids, *rest):
        tables = rest[2]
        pick, pick_t, got = spread(tok_ids, shards, tables.shape[1])
        fits = jnp.max(got[:, 3]) <= TAIL
        outs = fast_step(got, pick, pick_t, *rest)

        def again(_):
            return jnp.bool_(True), padded_step(shards, tok_ids, *rest)

        return lax.while_loop(lambda state: jnp.logical_not(state[0]), again, (fits, outs))[1]

    return jax.shard_map(
        device_step,
        mesh=mesh,
        in_specs=(P("emb"), P("emb", None), P("emb", None), P(None, "emb", None), P(), P(), P(), P()),
        out_specs=(P("emb", None), P(None, "emb", None), P(), P(), P(), P()),
        check_vma=False,
    )
```

```python
import functools

import jax
import jax.numpy as jnp
from jax import lax
from jax.experimental import pallas as pl
from jax.experimental.layout import Layout, with_layout_constraint
from jax.experimental.pallas import tpu as pltpu
from jax.sharding import PartitionSpec as P


EPS = 1e-6
CAP_DIV = 4


def gelu_tanh(pre_act):
    return jax.nn.gelu(pre_act, approximate=True)


def gelu_back(pre_act, grad_out):
    _, pull_back = jax.vjp(gelu_tanh, pre_act.astype(jnp.float32))
    return pull_back(grad_out.astype(jnp.float32))[0]


def dot32(a, b, dims):
    return lax.dot_general(a, b, (dims, ((), ())), preferred_element_type=jnp.float32)


def layer_fwd(x_cur, up_mat, down_mat, gate_mat, proj_mat, emb_rows):
    x_wide = x_cur.astype(jnp.float32)
    inv_rms = lax.rsqrt(jnp.mean(x_wide * x_wide, **ROW) + EPS)
    normed = (x_wide * inv_rms).astype(jnp.bfloat16)
    hidden = jnp.dot(normed, up_mat, preferred_element_type=jnp.float32).astype(jnp.bfloat16)
    act_out = gelu_tanh(hidden.astype(jnp.float32)).astype(jnp.bfloat16)
    mlp_out = jnp.dot(act_out, down_mat, preferred_element_type=jnp.float32).astype(jnp.bfloat16)
    gate_pre = jnp.dot(normed, gate_mat, preferred_element_type=jnp.float32).astype(jnp.bfloat16)
    gate_act = gelu_tanh(gate_pre.astype(jnp.float32)).astype(jnp.bfloat16)
    mix_rows = (gate_act.astype(jnp.float32) * emb_rows.astype(jnp.float32)).astype(jnp.bfloat16)
    ple_out = jnp.dot(mix_rows, proj_mat, preferred_element_type=jnp.float32).astype(jnp.bfloat16)
    x_next = (x_wide + mlp_out.astype(jnp.float32) + ple_out.astype(jnp.float32)).astype(jnp.bfloat16)
    return x_next, (x_cur, inv_rms, normed, hidden, act_out, gate_pre, gate_act, mix_rows)


def layer_bwd(d_x, saved, emb_rows, up_mat, down_mat, gate_mat, proj_mat, last):
    x_cur, inv_rms, normed, hidden, act_out, gate_pre, gate_act, mix_rows = saved
    x_wide = x_cur.astype(jnp.float32)
    g_out = d_x.astype(jnp.bfloat16)
    d_act = dot32(g_out, down_mat, NT).astype(jnp.bfloat16)
    d_hidden = gelu_back(hidden, d_act).astype(jnp.bfloat16)
    d_mix = dot32(g_out, proj_mat, NT).astype(jnp.bfloat16)
    d_gate_act = (emb_rows.astype(jnp.float32) * d_mix.astype(jnp.float32)).astype(jnp.bfloat16)
    d_gate_pre = gelu_back(gate_pre, d_gate_act).astype(jnp.bfloat16)
    d_x_new = None
    if not last:
        d_norm = dot32(d_hidden, up_mat, NT) + dot32(d_gate_pre, gate_mat, NT)
        d_x_new = d_x + inv_rms * d_norm - inv_rms ** 3 * x_wide * jnp.mean(d_norm * x_wide, **ROW)
    return d_x_new, (normed, act_out, mix_rows, g_out, d_hidden, d_gate_pre), (gate_act, d_mix)


BASE = 32
TAIL = 128
AXES = ("far", "near", "y", "x", "core")
WEIGHT = {name: 1 << i for i, name in enumerate(reversed(AXES))}
ORDERS = (("core", "x", "y", "near", "far"), ("core", "y", "near", "x", "far"), ("core", "near", "x", "y", "far"))
DOUBLING = [tuple(reversed(order)) for order in ORDERS]
PARTS = ((0, 48), (48, 40), (88, 40))
MESH = pl.DeviceIdType.MESH
DEPTH = 2
FIRST = range(DEPTH)
LAG = 2
NN, NT, TN = ((1,), (0,)), ((1,), (1,)), ((0,), (0,))
ROW = {"axis": -1, "keepdims": True}
HALF, QUART, EIGHTH = 128, 64, 32
COST = pl.CostEstimate(flops=10**11, bytes_accessed=10**8, transcendentals=0)
VMEM_LIMIT = 66_000_000


def bit(v):
    return lax.rem(v, 2)


def loop(first, last, body):
    def step(i, carry):
        body(i)
        return carry

    lax.fori_loop(first, last, step, 0)


def swap(a):
    return lax.all_to_all(a, "emb", 0, 0, tiled=True)


def line(i):
    return pl.ds(i, 1)


def col(v):
    return v[:, None]


def row(v):
    return v[None, :]


def numbers(n):
    return jnp.arange(n, dtype=jnp.int32)


BLK = 256
NB = 16
NS = 8


def reduce_kernel(sizes, *refs):
    n_layers, per, n = sizes
    u_0, a_0, us, as_, ss, os_, dhs, dzs, send_t, out, tails = refs[:11]
    (v_as, v_o, v_u, v_d, blk1, blk2, blk3, rc1, rc2, rc3, rf1, rf2, rs1, rs2, ri1, ri2, rm1, rm2, fin1, fin2,
     ri3, rm3, rx3, rf3, rs3, fin3, ssem, rsem, lsem, osem, tv, tsem, trsem, tlsem) = refs[11:]
    me = lax.axis_index("emb")
    spot = {name: bit(me // w) for name, w in WEIGHT.items()}
    other = {name: me + w - 2 * w * spot[name] for name, w in WEIGHT.items()}
    core, x, y, zb, near = (spot[name] for name in ("core", "x", "y", "far", "near"))
    p_core, p_x, p_y, p_side = (other[name] for name in ("core", "x", "y", "near"))
    mid = near != zb
    end = near == zb
    p_mid = me + WEIGHT["near"] * (near - zb)

    def loads(ell):
        layer = n_layers - 1 - ell
        u, a = (us.at[layer - 1], as_.at[layer - 1]) if layer else (u_0, a_0)
        s, o, dh, dz = (t.at[layer] for t in (ss, os_, dhs, dzs))
        slot = ell % 2
        hid = a_0.shape[1]
        left, right = pl.ds(0, hid), pl.ds(hid, BLK)
        ways = ((a, v_as.at[slot, :, left]), (s, v_as.at[slot, :, right]), (o, v_o.at[slot]), (u, v_u.at[slot]),
                (dh, v_d.at[slot, :, left]), (dz, v_d.at[slot, :, right]))
        return [pltpu.make_async_copy(src, dst, osem.at[slot, i]) for i, (src, dst) in enumerate(ways)]

    for ell in (0, 1):
        for c in loads(ell):
            c.start()

    barrier = pltpu.get_barrier_semaphore()
    for dev in other.values():
        pl.semaphore_signal(barrier, inc=1, device_id=(dev,), device_id_type=MESH)

    @pl.when(mid)
    def _():
        pl.semaphore_signal(barrier, inc=1, device_id=(p_mid,), device_id_type=MESH)
        pl.semaphore_wait(barrier, 6)

    @pl.when(end)
    def _():
        pl.semaphore_wait(barrier, 5)

    def tail_copy(part, s, p):
        order = DOUBLING[part]
        at = {name: bit(p // (1 << t)) for t, name in enumerate(order[:s])}
        ref = tails.at[tuple(at.get(name, spot[name]) for name in AXES) + (pl.ds(*PARTS[part]),)]
        i = lax.rem(p, LAG + LAG)
        return pltpu.make_async_remote_copy(src_ref=ref, dst_ref=ref, send_sem=tsem.at[part, s, i], recv_sem=trsem.at[part, s, i],
                                            device_id=(other[order[s]],), device_id_type=MESH)

    t_first = [4]
    for s in range(len(AXES)):
        t_first.append(t_first[-1] + (1 << s) + 2)
    t_own = pltpu.make_async_copy(send_t, tv, tlsem.at[0]), pltpu.make_async_copy(tv, tails.at[tuple(spot[name] for name in AXES)], tlsem.at[0])
    for c in t_own:
        c.start()
        c.wait()
    for c in loads(0):
        c.wait()

    span = n // n_layers
    rest = {0: 2, 1: 4}
    early, close = 4, 10

    def active(k, kind):
        return k < n - early if kind == 2 else (lax.rem(k, 5) != rest[kind]) | (k >= n - close)

    def unit(k, kind):
        t = lax.rem(k, span)
        if kind == 2:
            return span * 4 // 5 + jnp.where(k >= n - span, early // 2, 0) + t // 2
        p = lax.rem(t, 5)
        return jnp.where(k >= n - close, t - close + 4, 4 * (t // 5) + p - (p > rest[kind]).astype(jnp.int32))

    def where_out(k, kind):
        base = {0: 0, 1: per, 2: per * bit(k)}[kind]
        return (n_layers - 1 - k // span) * 2 * per + base + unit(k, kind)

    def block(slot, w, wide):
        if wide:
            rb, cb = w // 13, lax.rem(w, 13)
            lhs, rhs = v_u, v_d
        else:
            rb, cb = lax.rem(w, 13), w // 13
            lhs, rhs = v_as, v_o
        lv = lhs[slot, :, pl.ds(pl.multiple_of(rb * BLK, BLK), BLK)]
        rv = rhs[slot, :, pl.ds(pl.multiple_of(cb * BLK, BLK), BLK)]
        return dot32(lv, rv, TN)

    h0 = core * HALF
    flows = []

    def add_flow(off, src, dst, dev, send_if=None, recv_if=None):
        flows.append((len(flows), off, src, dst, dev, send_if, recv_if))
        return flows[-1]

    def rows(start, size):
        return pl.ds(pl.multiple_of(start, EIGHTH), size)

    def desc(f, k):
        idx, _, src, dst, dev, _, _ = f
        d = dev(k) if callable(dev) else dev
        return pltpu.make_async_remote_copy(
            src_ref=src(k), dst_ref=dst(k), send_sem=ssem.at[idx, lax.rem(k, NB)], recv_sem=rsem.at[idx, lax.rem(k, NB)],
            device_id=(d,), device_id_type=MESH)

    def ok(k, cond):
        v = (k >= 0) & (k < n)
        return v if cond is None else v & (cond(k) if callable(cond) else cond)

    acts = []

    def clock():
        now = [-1]

        def at(more=LAG):
            now[0] += more
            return now[0]

        return at

    def xyz(kind, blk, rc, rf, rs, ri, rm, fin, f, s, p_f, p_s):
        at = clock()
        q0, q1 = h0 + f * QUART, h0 + (1 - f) * QUART
        e0, e1 = q0 + s * EIGHTH, q0 + (1 - s) * EIGHTH
        b = lambda k: lax.rem(k, NB)
        m = lambda k: lax.rem(k, NS)
        o = lambda k: where_out(k, kind)
        go = lambda k: active(k, kind)
        on = lambda side: (lambda k: side & active(k, kind))
        f_core = add_flow(at(), lambda k: blk.at[b(k), rows(HALF - h0, HALF)], lambda k: rc.at[m(k)], p_core, go, go)
        f_first = add_flow(at(), lambda k: blk.at[b(k), rows(q1, QUART)], lambda k: rf.at[m(k)], p_f, go, go)
        f_second = add_flow(at(), lambda k: blk.at[b(k), rows(e1, EIGHTH)], lambda k: rs.at[m(k)], p_s, go, go)
        f_in = add_flow(at(), lambda k: blk.at[b(k), rows(e0, EIGHTH)], lambda k: ri.at[m(k)], p_side, on(end), on(mid))
        f_mid = add_flow(at(), lambda k: blk.at[b(k), rows(e0, EIGHTH)], lambda k: rm.at[m(k)], p_mid, on(mid), on(mid))
        f_out = add_flow(at(), lambda k: fin.at[b(k)], lambda k: fin.at[b(k)], p_side, on(mid), on(end))
        g_s = add_flow(at(), lambda k: fin.at[b(k)], lambda k: out.at[o(k), rows(e0, EIGHTH)], p_s, go, go)
        g_f = add_flow(at(), lambda k: out.at[o(k), rows(q0, QUART)], lambda k: out.at[o(k), rows(q0, QUART)], p_f, go, go)
        g_c = add_flow(at(), lambda k: out.at[o(k), rows(h0, HALF)], lambda k: out.at[o(k), rows(h0, HALF)], p_core, go, go)

        def plus(dst0, size, src):
            def add(k):
                r = rows(dst0, size)
                blk[b(k), r] = blk[b(k), r] + src[m(k)]

            return add

        def final(k):
            fin[b(k)] = blk[b(k), rows(e0, EIGHTH)] + rm[m(k)]

        acts.append((f_core, plus(h0, HALF, rc)))
        acts.append((f_first, plus(q0, QUART, rf)))
        acts.append((f_second, plus(e0, EIGHTH, rs)))
        acts.append((f_in, plus(e0, EIGHTH, ri)))
        acts.append((f_mid, final))
        acts.extend((g, None) for g in (f_out, g_s, g_f, g_c))
        locals_.append((g_s[1], lambda k: pltpu.make_async_copy(fin.at[b(k)], out.at[o(k), rows(e0, EIGHTH)], lsem.at[kind, m(k)]), go))

    def zfirst(kind, blk, rc, ri, rm, rx, rf, rs, fin):
        at = clock()
        odd = lambda k: bit(k) == 1
        at_end = lambda k: bit(k // 2) == 1
        go = lambda k: active(k, kind)
        here = lambda k: go(k) & jnp.where(at_end(k), end, mid)
        on = lambda side: (lambda k: side & go(k))
        q0, q1 = h0 + zb * QUART, h0 + (1 - zb) * QUART
        b = lambda k: lax.rem(k, NB)
        m = lambda k: lax.rem(k, NS)
        o = lambda k: where_out(k, kind)
        f = lambda k: jnp.where(odd(k), y, x)
        e0 = lambda k: q0 + f(k) * EIGHTH
        e1 = lambda k: q0 + (1 - f(k)) * EIGHTH
        p_f = lambda k: jnp.where(odd(k), p_y, p_x)
        p_s = lambda k: jnp.where(odd(k), p_x, p_y)
        e_root = lambda side: (lambda k: side & go(k) & at_end(k))
        m_root = lambda side: (lambda k: side & go(k) & jnp.logical_not(at_end(k)))
        f_core = add_flow(at(), lambda k: blk.at[b(k), rows(HALF - h0, HALF)], lambda k: rc.at[m(k)], p_core, go, go)
        f_in = add_flow(at(), lambda k: blk.at[b(k), rows(h0, HALF)], lambda k: ri.at[b(k)], p_side, m_root(end), m_root(mid))
        f_in2 = add_flow(at(0), lambda k: blk.at[b(k), rows(q1, QUART)], lambda k: ri.at[b(k), pl.ds(0, QUART)], p_side, e_root(end), e_root(mid))
        f_mid = add_flow(at(), lambda k: blk.at[b(k), rows(q1, QUART)], lambda k: rm.at[m(k)], p_mid, on(mid), on(mid))
        f_x = add_flow(at(), lambda k: blk.at[b(k), rows(q0, QUART)], lambda k: rx.at[m(k)], p_side, e_root(mid), e_root(end))
        f_first = add_flow(at(), lambda k: blk.at[b(k), rows(e1(k), EIGHTH)], lambda k: rf.at[m(k)], p_f, here, here)
        f_second = add_flow(at(), lambda k: blk.at[b(k), rows(e0(k), EIGHTH)], lambda k: rs.at[m(k)], p_s, here, here)
        g_f = add_flow(at(), lambda k: fin.at[m(k)], lambda k: out.at[o(k), rows(e0(k), EIGHTH)], p_f, here, here)
        g_x = add_flow(at(), lambda k: out.at[o(k), rows(q0, QUART)], lambda k: out.at[o(k), rows(q0, QUART)], p_side, e_root(end), e_root(mid))
        g_m = add_flow(at(), lambda k: out.at[o(k), rows(q0, QUART)], lambda k: out.at[o(k), rows(q0, QUART)], p_mid, on(mid), on(mid))
        g_o = add_flow(at(), lambda k: out.at[o(k), rows(h0, HALF)], lambda k: out.at[o(k), rows(h0, HALF)], p_side, m_root(mid), m_root(end))
        g_o2 = add_flow(at(0), lambda k: out.at[o(k), rows(q1, QUART)], lambda k: out.at[o(k), rows(q1, QUART)], p_side, e_root(mid), e_root(end))
        g_c = add_flow(at(), lambda k: out.at[o(k), rows(h0, HALF)], lambda k: out.at[o(k), rows(h0, HALF)], p_core, go, go)

        def plus(start, size, src):
            def add(k):
                r = rows(start(k), size)
                blk[b(k), r] = blk[b(k), r] + src(k)

            return add

        def final(k):
            fin[m(k)] = blk[b(k), rows(e0(k), EIGHTH)] + rs[m(k)]

        acts.append((f_core, plus(lambda k: h0, HALF, lambda k: rc[m(k)])))
        acts.append((f_in, plus(lambda k: h0, HALF, lambda k: ri[b(k)])))
        acts.append((f_in2, plus(lambda k: q1, QUART, lambda k: ri[b(k), :QUART])))
        acts.append((f_mid, plus(lambda k: q0, QUART, lambda k: rm[m(k)])))
        acts.append((f_x, plus(lambda k: q0, QUART, lambda k: rx[m(k)])))
        acts.append((f_first, plus(e0, EIGHTH, lambda k: rf[m(k)])))
        acts.append((f_second, final))
        acts.extend((g, None) for g in (g_f, g_x, g_m, g_o, g_o2, g_c))
        locals_.append((g_f[1], lambda k: pltpu.make_async_copy(fin.at[m(k)], out.at[o(k), rows(e0(k), EIGHTH)], lsem.at[kind, m(k)]), here))

    locals_ = []
    xyz(0, blk1, rc1, rf1, rs1, ri1, rm1, fin1, x, y, p_x, p_y)
    xyz(1, blk2, rc2, rf2, rs2, ri2, rm2, fin2, y, x, p_y, p_x)
    zfirst(2, blk3, rc3, ri3, rm3, rx3, rf3, rs3, fin3)

    def round_(r):
        for f in flows:
            _, off, _, _, _, give, _ = f
            k = r - off - LAG - LAG

            @pl.when(ok(k, give))
            def _(f=f, k=k):
                desc(f, k).wait_send()
        for off, mk, cond in locals_:
            k = r - off - LAG

            @pl.when(ok(k, cond))
            def _(mk=mk, k=k):
                mk(k).wait()
        for f, fn in acts:
            _, off, _, _, _, _, take = f
            k = r - off - LAG

            @pl.when(ok(k, take))
            def _(f=f, fn=fn, k=k):
                desc(f, k).wait_recv()
                if fn is not None:
                    fn(k)
        for s in range(len(AXES)):
            p = r - t_first[s]

            @pl.when((p >= 2) & (p < (1 << s) + 2))
            def _(s=s, p=p):
                for part in range(len(PARTS)):
                    tail_copy(part, s, p - 2).wait()

            @pl.when((p >= 0) & (p < (1 << s)))
            def _(s=s, p=p):
                for part in range(len(PARTS)):
                    tail_copy(part, s, p).start()
        for ell in range(1, n_layers):
            @pl.when(r == span * ell)
            def _(ell=ell):
                for c in loads(ell):
                    c.wait()
        for f in flows:
            _, off, _, _, _, give, _ = f
            k = r - off

            @pl.when(ok(k, give))
            def _(f=f, k=k):
                desc(f, k).start()
        for off, mk, cond in locals_:
            k = r - off

            @pl.when(ok(k, cond))
            def _(mk=mk, k=k):
                mk(k).start()

        slot = bit(r // span)
        s = lax.rem(r, NB)
        odd = bit(r) == 1

        @pl.when((r < n) & active(r, 0))
        def _():
            blk1[s] = block(slot, unit(r, 0), False)

        @pl.when((r < n) & active(r, 1))
        def _():
            blk2[s] = block(slot, unit(r, 1), True)

        @pl.when((r < n) & active(r, 2) & odd)
        def _():
            blk3[s] = block(slot, unit(r, 2), True)

        @pl.when((r < n) & active(r, 2) & jnp.logical_not(odd))
        def _():
            blk3[s] = block(slot, unit(r, 2), False)

        for ell in range(2, n_layers):
            @pl.when(r == span * (ell - 1) - 1)
            def _(ell=ell):
                for c in loads(ell):
                    c.start()

    loop(0, n + 22, round_)


def reduce_grads(u_0, a_0, us, as_, ss, os_, dhs, dzs, send_t):
    n_layers, toks, wide = ss.shape[0], u_0.shape[0], a_0.shape[1] + ss.shape[2]
    dim = u_0.shape[1]
    over, emb = send_t.shape[0], ss.shape[2]
    per = (wide // BLK) * (dim // BLK)
    n = per * 10 // 13 * n_layers
    f32, bf = jnp.float32, jnp.bfloat16
    V = pltpu.VMEM

    def many(count, slots, rows):
        return [V((slots, rows, BLK), f32)] * count

    big, small = (DEPTH, toks, wide), (DEPTH, toks, dim)
    scratch = [V(big, bf), V(small, bf), V(small, bf), V(big, bf)]
    scratch += many(3, NB, BLK) + many(3, NS, HALF) + many(DEPTH, NS, QUART) + many(6, NS, EIGHTH) + many(DEPTH, NB, EIGHTH)
    scratch += many(1, NB, HALF) + many(DEPTH, NS, QUART) + many(3, NS, EIGHTH)
    D = pltpu.SemaphoreType.DMA
    scratch += [D((31, NB)), D((31, NB)), D((3, NS)), D((DEPTH, 6))]
    scratch += [V((over, emb), f32)] + [D((len(PARTS), len(AXES), LAG + LAG))] * DEPTH + [D((1,))]
    flat = (u_0, a_0, us, as_, ss, os_, dhs, dzs, send_t)
    return pl.pallas_call(
        functools.partial(reduce_kernel, (n_layers, per, n)),
        out_shape=[jax.ShapeDtypeStruct((2 * per * n_layers, BLK, BLK), f32),
                   jax.ShapeDtypeStruct((2,) * len(AXES) + (over, emb), f32)],
        in_specs=[pl.BlockSpec(memory_space=pl.ANY)] * len(flat),
        out_specs=[pl.BlockSpec(memory_space=pl.ANY)] * 2,
        scratch_shapes=scratch,
        compiler_params=pltpu.CompilerParams(collective_id=0, has_side_effects=True, vmem_limit_bytes=VMEM_LIMIT),
        cost_estimate=COST,
        name="reduce_grads",
    )(*flat)


TILE = 256
FCH = 512
GK = 0.7978845608028654
GC = 0.044715


def gelu_f(h):
    return (0.5 * h) * (1.0 + jnp.tanh(h * (GK + (GK * GC) * (h * h))))


def gelu_g(h, g):
    h2 = h * h
    t = jnp.tanh(h * (GK + (GK * GC) * h2))
    return g * (0.5 * (1.0 + t) + (0.5 * h) * (1.0 - t * t) * (GK + (3.0 * GK * GC) * h2))


def model_kernel(*refs):
    (x0, m0, h0, z0, g0, base, t0, t1, t2, pick, pick_t, d_out, w_up, w_down, w_gate, w_proj,
     x_out, us, as_, ss, os_, dhs, dzs, hs, base_in, tails_in, send_b, send_t,
     wug, wd, wp, wp0, xs, cs, hbuf, abuf, ubuf, obuf, pbuf, sbuf, zs, es, gs, invs, dus, dsv, sb, st,
     wsem, usem, hsem, asem, osem, isem, jsem, psem, ssem, zsem, vsem, bsem, tsem, rsem, trsem) = refs
    f32, bf = jnp.float32, jnp.bfloat16
    slots = base.shape[0]
    n_tiles = xs.shape[1] // TILE
    top = es.shape[0] - 1
    ends = range(n_tiles - DEPTH, n_tiles)
    hid = hbuf.shape[2]
    emb = wp0.shape[0]
    dim = wp0.shape[1]

    def rows(i):
        return pl.ds(pl.multiple_of(i * TILE, TILE), TILE)

    def mm(a, b):
        return dot32(a, b, NN)

    def mt(a, b):
        return dot32(a, b, NT)

    cp = pltpu.make_async_copy
    me = lax.axis_index("emb")
    devices = slots // BASE
    peers = range(1, devices)
    barrier = pltpu.get_barrier_semaphore()
    for d in peers:
        pl.semaphore_signal(barrier, inc=1, device_id=(lax.rem(me + d, devices),), device_id_type=MESH)

    def parcel(slot, d):
        dev = lax.rem(me + d, devices)
        return pltpu.make_async_remote_copy(
            src_ref=sb.at[slot, pl.ds(pl.multiple_of(dev * BASE, BASE), BASE)], dst_ref=base_in.at[1 - slot, me],
            send_sem=bsem.at[slot, d], recv_sem=rsem.at[slot, d], device_id=(dev,), device_id_type=MESH)

    spots = {name: bit(me // w) for name, w in WEIGHT.items()}

    def tail_copies(layer, s):
        below = layer - 1
        copies = []
        for part, order in enumerate(DOUBLING):
            ref = tails_in.at[(below,) + tuple(slice(None) if name in order[:s] else spots[name] for name in AXES) + (pl.ds(*PARTS[part]),)]
            w = WEIGHT[order[s]]
            copies.append(pltpu.make_async_remote_copy(
                src_ref=ref, dst_ref=ref, send_sem=tsem.at[below, s, part], recv_sem=trsem.at[below, s, part],
                device_id=(me + w - 2 * w * spots[order[s]],), device_id_type=MESH))
        return copies

    def tail_wait(layer, s):
        for c in tail_copies(layer, s):
            c.wait()

    def tail_start(layer, s):
        if s:
            tail_wait(layer, s - 1)
        for c in tail_copies(layer, s):
            c.start()

    plan = {"bwd2": "222.", "bwd1": "2111", "bwd0": ".1.."}
    begun = dict.fromkeys("12", 1)

    def steps_of(name):
        steps = []
        for at, which in enumerate(plan.get(name, "")):
            if which in begun:
                steps.append((at, int(which), begun[which]))
                begun[which] += 1
        return steps

    def at_tile(i, steps):
        for at, which, s in steps:
            @pl.when(i == at)
            def _(which=which, s=s):
                tail_start(which, s)

    def own(slot):
        return cp(sb.at[slot, pl.ds(pl.multiple_of(me * BASE, BASE), BASE)], base_in.at[1 - slot, me], vsem.at[slot])

    def weights(layer, slot):
        ways = ((w_up, wug.at[slot, :, pl.ds(0, hid)]), (w_down, wd.at[slot]), (w_gate, wug.at[slot, :, pl.ds(hid, emb)]), (w_proj, wp.at[slot]))
        return [cp(src.at[layer], dst, wsem.at[slot, i]) for i, (src, dst) in enumerate(ways)]

    first = cp(w_proj.at[0], wp0, wsem.at[0, 4])
    first.start()
    w1, w2 = weights(1, 0), weights(2, 1)
    for c in w1 + w2:
        c.start()

    def slot_of(i):
        return bit(i)

    def in_x(i):
        return cp(x0.at[rows(i)], ubuf.at[slot_of(i)], isem.at[slot_of(i)])

    def in_p(i):
        return cp(pick.at[rows(i)], pbuf.at[slot_of(i)], psem.at[slot_of(i)])

    def in_m(i):
        return cp(m0.at[rows(i)], obuf.at[slot_of(i)], jsem.at[slot_of(i)])

    def put(src, dst, layer, sem):
        return lambda i: cp(src.at[slot_of(i)], dst.at[layer, rows(i)] if layer is not None else dst.at[rows(i)], sem.at[slot_of(i)])

    tails = (t0, t1, t2)

    def rows_of(layer, i):
        in_p(i).wait()
        p = pbuf[slot_of(i)]
        return (mm(p[:, :slots], base[:, layer * emb:(layer + 1) * emb]) + mm(p[:, slots:], tails[layer][...])).astype(bf)

    for i in FIRST:
        in_x(i).start()
        in_m(i).start()
        in_p(i).start()
    first.wait()
    put_s = lambda layer: (lambda i: cp(sbuf.at[slot_of(i)], ss.at[layer, rows(i)], ssem.at[slot_of(i)]))

    def finish0(i):
        r, k = rows(i), slot_of(i)

        @pl.when(i >= DEPTH)
        def _():
            put_s(0)(i - DEPTH).wait()

        e = rows_of(0, i)
        es[0, r] = e
        s = (g0[r].astype(f32) * e.astype(f32)).astype(bf)
        sbuf[k] = s
        put_s(0)(i).start()
        q = mm(s, wp0[...]).astype(bf)
        in_x(i).wait()
        in_m(i).wait()
        xs[0, r] = (ubuf[k].astype(f32) + obuf[k].astype(f32) + q.astype(f32)).astype(bf)

        @pl.when(i + DEPTH < n_tiles)
        def _():
            in_x(i + DEPTH).start()
            in_m(i + DEPTH).start()
            in_p(i + DEPTH).start()

    loop(0, n_tiles, finish0)
    for i in ends:
        put_s(0)(i).wait()

    def in_d(i):
        return cp(d_out.at[rows(i)], ubuf.at[slot_of(i)], isem.at[slot_of(i)])

    def put_t(layer):
        below = layer - 1
        dst = tails_in.at[(below,) + tuple(spots[name] for name in AXES)] if layer else send_t
        return cp(st, dst, jsem.at[0])

    def rows_back(layer, slot):
        below = layer - 1
        proj = wp0 if layer == 0 else wp.at[slot]
        if layer == top:
            for i in FIRST:
                in_d(i).start()

        def tile(i):
            r = rows(i)
            if layer == top:
                in_d(i).wait()
                cs[r] = ubuf[slot_of(i)].astype(f32)

                @pl.when(i + DEPTH < n_tiles)
                def _():
                    in_d(i + DEPTH).start()
            dsv[r] = mt(cs[r].astype(bf), proj[...]).astype(bf)

        loop(0, n_tiles, tile)
        g = g0 if layer == 0 else gs.at[below]
        d = g[...].astype(f32) * dsv[...].astype(f32)
        high = d.astype(bf)
        low = (d - high.astype(f32)).astype(bf)
        spot = layer % 2
        if layer == 0:
            for d in peers:
                parcel(spot, d).wait_send()
            own(spot).wait()
        for c0 in range(0, slots, BLK):
            p = pick_t[c0:c0 + BLK]
            sb[spot, c0:c0 + BLK] = mm(p, high) + mm(p, low)
        p = pick_t[slots:]
        st[...] = mm(p, high) + mm(p, low)
        put_t(layer).start()
        if layer == 0:
            cp(sb.at[spot], send_b, vsem.at[spot]).start()
        else:
            own(spot).start()
            if layer == top:
                pl.semaphore_wait(barrier, devices - 1)
            put_t(layer).wait()
            tail_start(layer, 0)
            if layer == top:
                for d in peers:
                    parcel(spot, d).start()

    def fwd(layer, slot, loaded):
        below = layer - 1
        outs = [put(ubuf, us, below, usem), put(hbuf, hs, below, hsem), put_s(layer),
                lambda i: cp(abuf.at[slot_of(i), :, pl.ds(0, hid)], as_.at[below, rows(i)], asem.at[slot_of(i)])]
        if layer == top:
            outs.append(put(obuf, x_out, None, osem))
        for c in loaded:
            c.wait()
        for i in FIRST:
            in_p(i).start()

        def gates(i):
            r = rows(i)
            x = xs[below, r].astype(f32)
            inv = lax.rsqrt(jnp.mean(x * x, **ROW) + EPS)
            invs[below, r] = jnp.broadcast_to(inv, (TILE, invs.shape[2]))
            z = mm((x * inv).astype(bf), wug[slot, :, hid:]).astype(bf)
            zs[below, r] = z
            gs[below, r] = gelu_f(z.astype(f32)).astype(bf)

        loop(0, n_tiles, gates)
        if layer == top:
            rows_back(layer, slot)
        steps = steps_of(f"fwd{layer}")

        def tile(i):
            r, k = rows(i), slot_of(i)

            @pl.when(i >= DEPTH)
            def _():
                for o in outs:
                    o(i - DEPTH).wait()

            at_tile(i, steps)
            x = xs[below, r].astype(f32)
            u = (x * invs[below, r][:, :1]).astype(bf)
            ubuf[k] = u
            for c0 in range(0, hid, FCH):
                h = mm(u, wug[slot, :, c0:c0 + FCH]).astype(bf)
                hbuf[k, :, c0:c0 + FCH] = h
                abuf[k, :, c0:c0 + FCH] = gelu_f(h.astype(f32)).astype(bf)
            g = gs[below, r]
            e = rows_of(layer, i)
            es[layer, r] = e
            s = (g.astype(f32) * e.astype(f32)).astype(bf)
            sbuf[k] = s
            for c0 in range(0, dim, FCH):
                c1 = c0 + FCH
                q = mm(s, wp[slot, :, c0:c1]).astype(bf)
                m = mm(abuf[k, :, :hid], wd[slot, :, c0:c1]).astype(bf)
                new = (xs[below, r, c0:c1].astype(f32) + m.astype(f32) + q.astype(f32)).astype(bf)
                if layer == top:
                    obuf[k, :, c0:c1] = new
                else:
                    xs[layer, r, c0:c1] = new
            for o in outs:
                o(i).start()

            @pl.when(i + DEPTH < n_tiles)
            def _():
                in_p(i + DEPTH).start()

        loop(0, n_tiles, tile)
        for i in ends:
            for o in outs:
                o(i).wait()

    def in_h(layer, i):
        below = layer - 1
        return cp(h0.at[rows(i)] if layer == 0 else hs.at[below, rows(i)], hbuf.at[slot_of(i)], hsem.at[slot_of(i)])

    def bwd(layer, slot):
        below = layer - 1
        outs = [lambda i: cp(abuf.at[slot_of(i), :, pl.ds(0, hid)], dhs.at[layer, rows(i)], asem.at[slot_of(i)]),
                lambda i: cp(abuf.at[slot_of(i), :, pl.ds(hid, emb)], dzs.at[layer, rows(i)], zsem.at[slot_of(i)]),
                put(obuf, os_, layer, osem)]
        steps = steps_of(f"bwd{layer}")
        if layer == top:
            for i in FIRST:
                in_h(layer, i).start()
        else:
            rows_back(layer, slot)

        def tile(i):
            r, k = rows(i), slot_of(i)

            @pl.when(i >= DEPTH)
            def _():
                for o in outs:
                    o(i - DEPTH).wait()

            at_tile(i, steps)
            if layer == 1:
                @pl.when(i == n_tiles - 1)
                def _():
                    for d in peers:
                        parcel(layer, d).start()
            o = cs[r].astype(bf)
            obuf[k] = o
            ds = dsv[r]
            z = (z0[r] if layer == 0 else zs[below, r]).astype(f32)
            dg = (es[layer, r].astype(f32) * ds.astype(f32)).astype(bf)
            abuf[k, :, hid:] = gelu_g(z, dg.astype(f32)).astype(bf)
            in_h(layer, i).wait()
            for c0 in range(0, hid, FCH):
                da = mt(o, wd[slot, c0:c0 + FCH]).astype(bf)
                abuf[k, :, c0:c0 + FCH] = gelu_g(hbuf[k, :, c0:c0 + FCH].astype(f32), da.astype(f32)).astype(bf)
            if layer > 0:
                dot = jnp.zeros((TILE, 1), f32)
                for c0 in range(0, dim, FCH):
                    du = mt(abuf[k], wug[slot, c0:c0 + FCH])
                    dus[:, c0:c0 + FCH] = du
                    dot = dot + jnp.sum(du * xs[below, r, c0:c0 + FCH].astype(f32), **ROW)
                inv = invs[below, r][:, :1]
                back = (inv * inv * inv) * (dot * (1.0 / dim))
                for c0 in range(0, dim, FCH):
                    c1 = c0 + FCH
                    cs[r, c0:c1] = cs[r, c0:c1] + inv * dus[:, c0:c1] - back * xs[below, r, c0:c1].astype(f32)
            for ot in outs:
                ot(i).start()

            @pl.when(i + DEPTH < n_tiles)
            def _():
                in_h(layer, i + DEPTH).start()

        loop(0, n_tiles, tile)
        if layer > 0:
            for i in FIRST:
                in_h(below, i).start()
        for i in ends:
            for o in outs:
                o(i).wait()

    fwd(1, 0, w1)
    fwd(2, 1, w2)
    bwd(2, 1)
    last = cp(w_down.at[0], wd.at[1], wsem.at[1, 1])
    last.start()
    bwd(1, 0)
    last.wait()
    bwd(0, 1)
    put_t(0).wait()
    for layer in (1, 2):
        tail_wait(layer, len(AXES) - 1)
    cp(sb.at[0], send_b, vsem.at[0]).wait()
    own(1).wait()
    for d in peers:
        parcel(0, d).wait_recv()
        parcel(1, d).wait()


def run_model(pre, base, tails, pick, pick_t, d_out, w_up, w_down, w_gate, w_proj):
    x0, m0, h0, z0, g0 = pre
    layers, dim, hid = w_up.shape
    emb = w_gate.shape[2]
    toks = x0.shape[0]
    slots, over = base.shape[0], tails[0].shape[0]
    below = layers - 1
    f32, bf = jnp.float32, jnp.bfloat16
    hbm, vm = pl.BlockSpec(memory_space=pl.ANY), pl.BlockSpec(memory_space=pltpu.VMEM)
    S = jax.ShapeDtypeStruct
    V = pltpu.VMEM
    D = pltpu.SemaphoreType.DMA
    return pl.pallas_call(
        model_kernel,
        in_specs=[hbm] * 3 + [vm] * 6 + [hbm] + [vm] + [hbm] * 5,
        out_specs=[hbm] * 12,
        out_shape=[S((toks, dim), bf), S((below, toks, dim), bf), S((below, toks, hid), bf), S((layers, toks, emb), bf),
                   S((layers, toks, dim), bf), S((layers, toks, hid), bf), S((layers, toks, emb), bf), S((below, toks, hid), bf),
                   S((below, slots // BASE, BASE, emb), f32),
                   S((below,) + (2,) * len(AXES) + (over, emb), f32), S((slots, emb), f32), S((over, emb), f32)],
        scratch_shapes=[
            V((DEPTH, dim, hid + emb), bf), V((DEPTH, hid, dim), bf), V((DEPTH, emb, dim), bf), V((emb, dim), bf),
            V((DEPTH, toks, dim), bf), V((toks, dim), f32), V((DEPTH, TILE, hid), bf), V((DEPTH, TILE, hid + emb), bf),
            V((DEPTH, TILE, dim), bf), V((DEPTH, TILE, dim), bf), V((DEPTH, TILE, slots + over), bf), V((DEPTH, TILE, emb), bf),
            V((DEPTH, toks, emb), bf), V((layers, toks, emb), bf), V((DEPTH, toks, emb), bf), V((DEPTH, toks, 128), f32), V((TILE, dim), f32),
            V((toks, emb), bf), V((DEPTH, slots, emb), f32), V((over, emb), f32),
            D((DEPTH, 5))] + [D((DEPTH,))] * 10 + [D((DEPTH, slots // BASE)), D((DEPTH, len(AXES), len(PARTS)))] * DEPTH,
        compiler_params=pltpu.CompilerParams(collective_id=2, has_side_effects=True, vmem_limit_bytes=VMEM_LIMIT),
        name="model",
    )(x0, m0, h0, z0, g0, base, *tails, pick, pick_t, d_out, w_up, w_down, w_gate, w_proj)


def spread(tok_ids, shards, rows_dev):
    toks = tok_ids.shape[0]
    i32, f32, bf = jnp.int32, jnp.float32, jnp.bfloat16
    owner = tok_ids // rows_dev
    local = tok_ids - owner * rows_dev
    row_no = lax.broadcasted_iota(i32, (toks, toks), 0)
    col_no = lax.broadcasted_iota(i32, (toks, toks), 1)
    same = col(tok_ids) == row(tok_ids)

    def first_one(earlier, axis):
        return 1.0 - jnp.max((same & earlier).astype(f32), axis=axis)

    new = first_one(col_no < row_no, 1)
    hot32 = (col(owner) == row(numbers(shards))).astype(f32)
    fresh = hot32 * col(new)
    before = (row_no > col_no).astype(bf)
    ahead = jnp.dot(before, fresh.astype(bf), preferred_element_type=f32)
    rank = jnp.sum(ahead * hot32, axis=1)
    count = jnp.sum(fresh, axis=0)
    extra = jnp.maximum(count - BASE, 0.0)
    lower = lax.broadcasted_iota(i32, (shards, shards), 0) > lax.broadcasted_iota(i32, (shards, shards), 1)
    start = jnp.sum(jnp.where(lower, row(extra), 0.0), axis=1)
    tail = jnp.sum(hot32 * row(start), axis=1)
    place = jnp.where(rank < BASE, owner.astype(f32) * BASE + rank, shards * BASE + tail + rank - BASE)
    spots = place * first_one(row_no < col_no, 0)
    slot = jnp.sum(same.astype(f32) * row(spots), axis=1).astype(i32)
    n_slots = shards * BASE + TAIL
    pick = (col(slot) == lax.broadcasted_iota(i32, (toks, n_slots), 1)).astype(bf)
    pick_t = (row(slot) == lax.broadcasted_iota(i32, (n_slots, toks), 0)).astype(bf)
    parts = (jnp.stack([local // 64, local % 64], axis=1).astype(f32) * col(new)).astype(bf)
    want = jnp.dot(pick_t, parts, preferred_element_type=f32)
    want = (want[:, 0] * 64.0 + want[:, 1]).astype(i32)
    base = want[:shards * BASE].reshape(shards, BASE)
    rest = jnp.broadcast_to(want[shards * BASE:][None, :], (shards, TAIL))
    total = jnp.sum(extra)
    fit = (total <= TAIL).astype(f32)
    info = jnp.stack([count, start * fit, extra * fit, jnp.broadcast_to(total, (shards,))], axis=1).astype(i32)
    pad = jnp.zeros((shards, INFO - 4), i32)
    sent = jnp.concatenate([info, pad, base, rest], axis=1)
    got = swap(sent)
    return pick, pick_t, got


INFO = 128


def tail_of(got, j):
    return got[j, 1], got[j, 2]


def serve_kernel(n_layers, over, got, tables, *refs):
    base_out, outs, (tab, wide, stage, sem) = refs[0], refs[1:1 + n_layers], refs[1 + n_layers:]
    shards = got.shape[0]
    emb = wide.shape[2]
    loads = [pltpu.make_async_copy(tables.at[k], tab.at[k], sem.at[k]) for k in range(n_layers)]
    for c in loads:
        c.start()
    for k in range(n_layers):
        loads[k].wait()
        whole = wide.shape[1] // BLK * BLK

        def widen(i, k=k):
            r = pl.ds(pl.multiple_of(i * BLK, BLK), BLK)
            wide[k, r] = tab[k, r].astype(jnp.float32)

        loop(0, whole // BLK, widen)
        wide[k, whole:] = tab[k, whole:].astype(jnp.float32)

    stage[...] = jnp.zeros_like(stage)

    def one(j):
        start, extra = tail_of(got, j)

        def rows8(g):
            at = [got[j, INFO + g * 8 + i] for i in range(8)]
            for i in range(8):
                for k in range(n_layers):
                    stage[k, line(g * 8 + i)] = wide[k, line(at[i])]

        used = jnp.minimum(got[j, 0], BASE)
        loop(0, (used + 7) // 8, rows8)
        for k in range(n_layers):
            base_out[j, :, k * emb:(k + 1) * emb] = stage[k, :BASE].astype(jnp.bfloat16)

        @pl.when(extra == 0)
        def _():
            for k in range(n_layers):
                outs[k][j] = jnp.zeros((over, emb), jnp.bfloat16)

        @pl.when(extra > 0)
        def _():
            stage[...] = jnp.zeros_like(stage)

            def four(g):
                at = [got[j, INFO + BASE + start + g * 4 + i] for i in range(4)]
                for i in range(4):
                    for k in range(n_layers):
                        stage[k, line(start + g * 4 + i)] = wide[k, line(at[i])]

            def single(i):
                at = got[j, INFO + BASE + start + i]
                for k in range(n_layers):
                    stage[k, line(start + i)] = wide[k, line(at)]

            loop(0, extra // 4, four)
            loop(extra // 4 * 4, extra, single)
            for k in range(n_layers):
                outs[k][j] = stage[k].astype(jnp.bfloat16)

    loop(0, shards, one)


def serve(got, tables, over):
    n_layers, rows_dev, emb = tables.shape
    shards = got.shape[0]
    bf = jnp.bfloat16
    shapes = [jax.ShapeDtypeStruct((shards, BASE, n_layers * emb), bf)] + [jax.ShapeDtypeStruct((shards, over, emb), bf)] * n_layers
    return pl.pallas_call(
        functools.partial(serve_kernel, n_layers, over),
        in_specs=[pl.BlockSpec(memory_space=pltpu.SMEM), pl.BlockSpec(memory_space=pl.ANY)],
        out_specs=[pl.BlockSpec(memory_space=pltpu.VMEM)] * (1 + n_layers),
        out_shape=shapes,
        scratch_shapes=[pltpu.VMEM((n_layers, rows_dev, emb), bf), pltpu.VMEM((n_layers, rows_dev, emb), jnp.float32),
                        pltpu.VMEM((n_layers, over, emb), jnp.float32), pltpu.SemaphoreType.DMA((n_layers,))],
        compiler_params=pltpu.CompilerParams(vmem_limit_bytes=VMEM_LIMIT),
        name="serve_rows",
    )(got, tables)


RING = 64


def finish_kernel(got, base, base_in, tail, tails_in, x_in, total, table, x_out, down, proj, up, gate, base_v, tail_v, acc, x_v, ring, sem, rsem, wsem):
    shards = got.shape[0]
    n_layers, rows_dev, emb = acc.shape
    n = total.shape[0]
    tall = down.shape[1] // BLK
    nr, half = tall + 1, n // n_layers // 2
    lag = RING // 2
    cp = pltpu.make_async_copy
    first = [cp(base, base_v.at[0], sem.at[0]), cp(base_in, base_v.at[pl.ds(1, n_layers - 1)], sem.at[3])]
    x_load, x_store = cp(x_in, x_v, sem.at[1]), cp(x_v, x_out, sem.at[1])
    done = cp(acc, table, sem.at[2])

    def slot(i):
        return lax.rem(i, RING)

    def load(i):
        return cp(total.at[i], ring.at[slot(i)], rsem.at[slot(i)])

    def block(i):
        return pl.ds(pl.multiple_of(i * BLK, BLK), BLK)

    def put(i, dst):
        return cp(ring.at[slot(i)], dst, wsem.at[slot(i)])

    def store(i):
        layer, t = i // (2 * half), lax.rem(i, half)
        wide = bit(i // half) == 1
        a, b = t // nr, lax.rem(t, nr)
        for here, dst in ((~wide & (b < tall), lambda: down.at[layer, block(b), block(a)]), (~wide & (b == tall), lambda: proj.at[layer, :, block(a)]),
                          (wide & (b < tall), lambda: up.at[layer, block(a), block(b)]), (wide & (b == tall), lambda: gate.at[layer, block(a)])):
            @pl.when(here)
            def _(dst=dst):
                put(i, dst()).start()

    def stored(i):
        put(i, proj.at[0, :, pl.ds(0, BLK)]).wait()

    for c in first:
        c.start()
    x_load.start()

    def begin(i):
        load(i).start()

    loop(0, RING, begin)
    whole = rows_dev // BLK * BLK
    for k in range(n_layers):
        def clear(i, k=k):
            acc[k, block(i)] = jnp.zeros((BLK, emb), jnp.float32)

        loop(0, whole // BLK, clear)
        acc[k, whole:] = jnp.zeros((rows_dev - whole, emb), jnp.float32)

    def one(j):
        def rows8(g):
            at = [line(got[j, INFO + g * 8 + i]) for i in range(8)]
            for i in range(8):
                for k in range(n_layers):
                    acc[k, at[i]] = acc[k, at[i]] + base_v[k, j, line(g * 8 + i)]

        loop(0, (jnp.minimum(got[j, 0], BASE) + 7) // 8, rows8)

    def two(j):
        start, extra = tail_of(got, j)
        blocks = [cp(tail.at[j], tail_v.at[0], sem.at[4]), cp(tails_in.at[:, j], tail_v.at[pl.ds(1, n_layers - 1)], sem.at[5])]

        @pl.when(extra > 0)
        def _():
            for c in blocks:
                c.start()
            for c in blocks:
                c.wait()

        def some(first_row, n):
            at = [line(got[j, INFO + BASE + start + first_row + i]) for i in range(n)]
            for i in range(n):
                for k in range(n_layers):
                    acc[k, at[i]] = acc[k, at[i]] + tail_v[k, line(start + first_row + i)]

        def four(g):
            some(g * 4, 4)

        def single(i):
            some(i, 1)

        loop(0, extra // 4, four)
        loop(extra // 4 * 4, extra, single)

    for c in first:
        c.wait()

    def step(i):
        load(i).wait()
        store(i)
        old = i - lag

        @pl.when(old >= 0)
        def _():
            stored(old)

            @pl.when(old + RING < n)
            def _():
                load(old + RING).start()

        j = i // 4
        now = lax.rem(i, 4) == 0

        @pl.when(now & (j < shards))
        def _():
            one(j)

        @pl.when(now & (j >= shards) & (j < 2 * shards))
        def _():
            two(j - shards)

        @pl.when(i == 8 * shards)
        def _():
            done.start()
            x_load.wait()
            x_store.start()

    loop(0, n, step)

    def end(i):
        stored(i)

    loop(n - lag, n, end)
    done.wait()
    x_store.wait()


def finish(got, base, base_in, tail, tails_in, x_in, total, layers, rows_dev, dim, hid, emb):
    f32 = jnp.float32
    shards = got.shape[0]
    hbm = pl.BlockSpec(memory_space=pl.ANY)
    S, V, D = jax.ShapeDtypeStruct, pltpu.VMEM, pltpu.SemaphoreType.DMA
    return pl.pallas_call(
        finish_kernel,
        in_specs=[pl.BlockSpec(memory_space=pltpu.SMEM)] + [hbm] * 6,
        out_specs=[hbm] * 6,
        out_shape=[S((layers, rows_dev, emb), f32), S(x_in.shape, x_in.dtype), S((layers, hid, dim), f32), S((layers, emb, dim), f32),
                   S((layers, dim, hid), f32), S((layers, dim, emb), f32)],
        scratch_shapes=[V((layers, shards, BASE, emb), f32), V((layers, TAIL, emb), f32), V((layers, rows_dev, emb), f32), V(x_in.shape, x_in.dtype),
                        V((RING, BLK, BLK), f32), D((6,)), D((RING,)), D((RING,))],
        compiler_params=pltpu.CompilerParams(vmem_limit_bytes=VMEM_LIMIT),
        name="finish",
    )(got, base.reshape(shards, BASE, emb), base_in, tail.reshape(shards, TAIL, emb), tails_in.reshape(layers - 1, shards, TAIL, emb), x_in, total)


WORK = (1, 2, 1, 0, 0)


def tails_kernel(*refs):
    n = len(ORDERS)
    refs = list(refs)

    def take(count):
        return [refs.pop(0) for _ in range(count)]

    (x_in, w_up, w_down, w_gate), tails, outs, rests, (wug, wd), keep = take(4), take(n), take(6), take(n), take(2), take(6)
    (wsem, dsem, ssem, rsem), bufs = take(4), refs
    f32, bf = jnp.float32, jnp.bfloat16
    me = lax.axis_index("emb")
    hid, dim = w_up.shape[2], w_up.shape[1]
    uv, hv, av, mv, zv, gv = keep
    spot = {name: bit(me // w) for name, w in WEIGHT.items()}
    other = {name: me + w - 2 * w * spot[name] for name, w in WEIGHT.items()}
    barrier = pltpu.get_barrier_semaphore()
    for name in AXES:
        pl.semaphore_signal(barrier, inc=1, device_id=(other[name],), device_id_type=MESH)
    cp = pltpu.make_async_copy
    ways = ((w_up, wug.at[:, pl.ds(0, hid)]), (w_down, wd), (w_gate, wug.at[:, pl.ds(hid, w_gate.shape[2])]))
    loads = [cp(src.at[0], dst, wsem.at[i]) for i, (src, dst) in enumerate(ways)]
    for c in loads:
        c.start()
    pl.semaphore_wait(barrier, len(AXES))

    def rows(i):
        return pl.ds(pl.multiple_of(i * TILE, TILE), TILE)

    def put(i):
        return [cp(src.at[rows(i)], dst.at[rows(i)], dsem.at[j, i]) for j, (src, dst) in enumerate(zip(keep, outs))]

    def tile(i):
        r = rows(i)
        x = x_in[r].astype(f32)
        u = (x * lax.rsqrt(jnp.mean(x * x, **ROW) + EPS)).astype(bf)
        uv[r] = u
        for c0 in range(0, hid, FCH):
            c = slice(c0, c0 + FCH)
            h = dot32(u, wug[:, c], NN).astype(bf)
            hv[r, c] = h
            av[r, c] = gelu_f(h.astype(f32)).astype(bf)
        z = dot32(u, wug[:, hid:], NN).astype(bf)
        zv[r] = z
        gv[r] = gelu_f(z.astype(f32)).astype(bf)
        for c0 in range(0, dim, FCH):
            c = slice(c0, c0 + FCH)
            mv[r, c] = dot32(av[r], wd[:, c], NN).astype(bf)
        for c in put(i):
            c.start()

    cur, names = list(tails), [list(AXES) for _ in range(n)]
    first = 0
    for s, count in enumerate(WORK):
        copies, kept = [], []
        for k in range(n):
            name = ORDERS[k][s]
            at = names[k].index(name)
            side = lambda v: tuple(v if i == at else slice(None) for i in range(len(names[k])))
            copies.append(pltpu.make_async_remote_copy(
                src_ref=cur[k].at[side(1 - spot[name])], dst_ref=bufs[s].at[k], send_sem=ssem.at[k, s], recv_sem=rsem.at[k, s],
                device_id=(other[name],), device_id_type=MESH))
            kept.append(side(spot[name]))
            names[k].remove(name)
        for c in copies:
            c.start()
        if s == 0:
            for c in loads:
                c.wait()
        if count:
            loop(first, first + count, tile)
        first += count
        for k in range(n):
            copies[k].wait()
            dst = bufs[len(WORK) + s].at[k] if s + 1 < len(WORK) else rests[k]
            dst[...] = cur[k][kept[k]] + bufs[s][k]
            cur[k] = dst
    for i in range(first):
        for c in put(i):
            c.wait()


def run_tails(x_in, w_up, w_down, w_gate, tails):
    n = len(tails)
    rows, emb = tails[0].shape[1:]
    toks, dim = x_in.shape
    hid = w_up.shape[2]
    bf = jnp.bfloat16
    S, V, D = jax.ShapeDtypeStruct, pltpu.VMEM, pltpu.SemaphoreType.DMA
    hbm, vm = pl.BlockSpec(memory_space=pl.ANY), pl.BlockSpec(memory_space=pltpu.VMEM)
    cube = (2,) * len(AXES)
    keep = [(toks, dim), (toks, hid), (toks, hid), (toks, dim), (toks, emb), (toks, emb)]
    steps = [V((n,) + cube[s + 1:] + (rows, emb), bf) for s in range(len(AXES))]
    sems = [D((3,)), D((len(keep), toks // TILE)), D((n, len(AXES))), D((n, len(AXES)))]
    return pl.pallas_call(
        tails_kernel,
        in_specs=[vm] + [hbm] * 3 + [vm] * n,
        out_specs=[hbm] * len(keep) + [vm] * n,
        out_shape=[S(s, bf) for s in keep] + [S((rows, emb), bf)] * n,
        scratch_shapes=[V((dim, hid + emb), bf), V((hid, dim), bf)] + [V(s, bf) for s in keep] + sems + steps + steps[:-1],
        compiler_params=pltpu.CompilerParams(collective_id=1, has_side_effects=True, vmem_limit_bytes=VMEM_LIMIT),
        cost_estimate=COST,
        name="tails",
    )(x_in, w_up, w_down, w_gate, *[t.reshape(cube + (rows, emb)) for t in tails])


def fast_step(got, pick, pick_t, x_in, d_out, ple_tables, w_up, w_down, w_gate, w_proj):
    layers, rows_dev, emb = ple_tables.shape
    shards = got.shape[0]
    served = serve(got, ple_tables, TAIL)
    base = swap(served[0].reshape(shards * BASE, layers * emb))
    u, h, a, m, z, g, *rests = run_tails(x_in, w_up, w_down, w_gate, served[1:])
    x_out, us, as_, ss, os_, dhs, dzs, _, base_in, tails_in, send_b, send_t = run_model(
        (x_in, m, h, z, g), base, rests, pick, pick_t, d_out, w_up, w_down, w_gate, w_proj)
    base = swap(send_b)
    total, tail = reduce_grads(u, a, us, as_, ss, os_, dhs, dzs, send_t)
    table, x_out, down, proj, up, gate = finish(got, base, base_in, tail, tails_in, x_out, total, layers, rows_dev, w_up.shape[1], w_up.shape[2], emb)
    return x_out, table, up, down, gate, proj


def padded_step(shards, tok_ids, x_in, d_out, ple_tables, w_up, w_down, w_gate, w_proj):
    layers = ple_tables.shape[0]
    rows_dev = ple_tables.shape[1]
    cap_rows = tok_ids.shape[0] // CAP_DIV
    owner_dev = tok_ids // rows_dev
    local_row = tok_ids - owner_dev * rows_dev
    owner_hot = (col(owner_dev) == row(numbers(shards))).astype(jnp.int32)
    slot_rank = jnp.sum((jnp.cumsum(owner_hot, axis=0) - owner_hot) * owner_hot, axis=1)
    dest_slot = owner_dev * cap_rows + slot_rank
    req_send = jnp.zeros((shards * cap_rows,), jnp.int32).at[dest_slot].set(local_row)
    req_recv = swap(req_send)
    x_cur = x_in
    saved_list = []
    rows_list = []
    for layer_idx in range(layers):
        served = jnp.take(ple_tables[layer_idx], req_recv, axis=0)
        returned = swap(served)
        emb_rows = jnp.take(returned, dest_slot, axis=0)
        x_cur, saved = layer_fwd(x_cur, w_up[layer_idx], w_down[layer_idx], w_gate[layer_idx], w_proj[layer_idx], emb_rows)
        saved_list.append(saved)
        rows_list.append(emb_rows)
    d_x = d_out.astype(jnp.float32)
    kept = [None] * layers
    tables_by_layer = [None] * layers
    for layer_idx in reversed(range(layers)):
        d_x, kept[layer_idx], (g, ds) = layer_bwd(d_x, saved_list[layer_idx], rows_list[layer_idx], w_up[layer_idx], w_down[layer_idx], w_gate[layer_idx], w_proj[layer_idx], layer_idx == 0)
        d_rows = g.astype(jnp.float32) * ds.astype(jnp.float32)
        grad_send = jnp.zeros((shards * cap_rows, d_rows.shape[1]), jnp.float32).at[dest_slot].set(d_rows)
        grad_recv = swap(grad_send)
        tables_by_layer[layer_idx] = jax.ops.segment_sum(grad_recv, req_recv, num_segments=rows_dev)
    u, a, s, o, dh, dz = zip(*kept)
    total = reduce_grads(u[0], a[0], jnp.stack(u[1:]), jnp.stack(a[1:]), jnp.stack(s), jnp.stack(o), jnp.stack(dh), jnp.stack(dz), jnp.zeros((TAIL, dz[0].shape[1]), jnp.float32))[0]
    (_, dim, hid), (_, _, emb) = w_up.shape, w_gate.shape
    nr, nc = (hid + emb) // BLK, dim // BLK
    total = total.reshape(layers, 2, nr * nc, BLK, BLK)
    tall = total[:, 0].reshape(layers, nc, nr, BLK, BLK).transpose(0, 2, 3, 1, 4).reshape(layers, hid + emb, dim)
    wide = total[:, 1].reshape(layers, nc, nr, BLK, BLK).transpose(0, 1, 3, 2, 4).reshape(layers, dim, hid + emb)
    outs = (x_cur, jnp.stack(tables_by_layer), wide[:, :, :hid], tall[:, :hid], wide[:, :, hid:], tall[:, hid:])
    return tuple(with_layout_constraint(o, Layout(major_to_minor=tuple(range(o.ndim)))) for o in outs)


def solution(mesh):
    shards = mesh.shape["emb"]

    def device_step(tok_ids, *rest):
        tables = rest[2]
        pick, pick_t, got = spread(tok_ids, shards, tables.shape[1])
        fits = jnp.max(got[:, 3]) <= TAIL
        outs = fast_step(got, pick, pick_t, *rest)

        def again(_):
            return jnp.bool_(True), padded_step(shards, tok_ids, *rest)

        return lax.while_loop(lambda state: jnp.logical_not(state[0]), again, (fits, outs))[1]

    return jax.shard_map(
        device_step,
        mesh=mesh,
        in_specs=(P("emb"), P("emb", None), P("emb", None), P(None, "emb", None), P(), P(), P(), P()),
        out_specs=(P("emb", None), P(None, "emb", None), P(), P(), P(), P()),
        check_vma=False,
    )
```
